32 devices in a mesh: ka: 16 (over z, y, core), ga: 2 (over x).
Axes of the slice: x: 2, y: 2, z: 4, core: 2. Of those that a mesh axis runs over, the one named last changes fastest.
Arguments:
- coeffs: bfloat16 [16, 240, 2, 64, 128], P('ka', 'ga'), may hold values from -0.44921875 to 0.44921875
- neighbour: int32 [16, 3], P('ka'), may hold values from 0 to 15, as said below
- shift_id: int32 [16, 3], P('ka'), may hold values from 0 to 7
- block_map: int32 [8, 240], replicated, may hold values from 0 to 239, as said below
Outputs:
- intersection: float32 [16, 3, 2, 64, 64], P('ka', None, None, 'ga')
The draws below stay inside these ranges and needn't reach their ends.
Inputs may be any that keep to these rules, and one draw needn't show every extreme that they name: `neighbour`: the k-points are numbered helically. The three columns of row k hold (k + 1) mod 16, (k + 4) mod 16 and (k + 8) mod 16, in an order drawn for each row. `block_map`: each row is a permutation of the 240 blocks. Block j lies in G-slice j // 120. In every row, each G-slice receives exactly 20 of its blocks from one other G-slice, exactly 10 from each of the remaining other G-slices, and the rest from itself.
All inputs are finite; a program needn't handle non-finite values.
Results may differ from the reference program's by a relative error of at most 0.0003.
Values may be sent and summed in bfloat16 or wider, within the bound.
A program may use at most 128 MiB of HBM per device.

```python
import jax
import jax.numpy as jnp
from jax import lax

NB = 64
NBV = 3
NSHIFT = 8
K_DEV = 1
KPTS = 16
MZ = 4
NBLK = 240
BLK_SL = 120
CAP = 20
N_KA = 16
N_GA = 2


def column_order(one_key):
    return jax.random.permutation(one_key, 3).astype(jnp.int32)


def draw_neighbour(key, part):
    total = K_DEV * N_KA
    points = jnp.arange(total, dtype=jnp.int32)
    z_step = jnp.mod(points + 1, total)
    y_step = jnp.mod(points + MZ, total)
    x_step = jnp.mod(points + total // 2, total)
    stacked = jnp.stack([z_step, y_step, x_step], axis=1).astype(jnp.int32)
    orders = jax.vmap(column_order)(jax.random.split(jax.random.fold_in(key, 17), total))
    return jnp.take_along_axis(stacked, orders, axis=1).astype(jnp.int32)


def row_shuffle(one_key):
    return jax.random.permutation(one_key, BLK_SL).astype(jnp.int32)


def one_map(key):
    keys = jax.random.split(key, 3)
    lighter = CAP // 2
    heavy = jax.random.randint(keys[0], (), 1, N_GA, dtype=jnp.int32)
    rows = jnp.arange(N_GA, dtype=jnp.int32)[:, None]
    cols = jnp.arange(BLK_SL, dtype=jnp.int32)[None, :]
    self_count = BLK_SL - CAP - (N_GA - 2) * lighter
    remain = jnp.maximum(cols - self_count - CAP, 0) // lighter
    other_step = jnp.where(remain + 1 < heavy, remain + 1, remain + 2)
    offset = jnp.where(cols < self_count, 0, jnp.where(cols < self_count + CAP, heavy, other_step))
    labels = jnp.mod(rows + offset, N_GA).astype(jnp.int32)
    shuffles = jax.vmap(row_shuffle)(jax.random.split(keys[1], N_GA))
    labels = jnp.take_along_axis(labels, shuffles, axis=1).reshape(-1)
    grouped = jnp.argsort(labels, stable=True).astype(jnp.int32)
    inner = jax.vmap(row_shuffle)(jax.random.split(keys[2], N_GA))
    sources = (jnp.arange(N_GA, dtype=jnp.int32)[:, None] * BLK_SL + inner).reshape(-1)
    return jnp.zeros((N_GA * BLK_SL,), jnp.int32).at[grouped].set(sources)


def draw_block_map(key, part):
    keys = jax.random.split(key, NSHIFT)
    return jax.vmap(one_map)(keys).astype(jnp.int32)


def place_ends(values, own_key, least, top_value):
    place = [jax.random.randint(jax.random.fold_in(own_key, axis), (), 0, length) for axis, length in enumerate(values.shape)]
    main_axis = values.shape.index(max(values.shape))
    beside = place[:main_axis] + [(place[main_axis] + 1) % values.shape[main_axis]] + place[main_axis + 1:]
    return values.at[tuple(place)].set(least).at[tuple(beside)].set(top_value)


def block_scale(own_key, shape, pieces, smallest, largest):
    factor_of = 1.0
    for position, parts in pieces:
        steps = jax.random.uniform(jax.random.fold_in(jax.random.fold_in(own_key, 6), position), (parts,), jnp.float32, smallest / len(pieces), largest / len(pieces))
        factor_of = factor_of * jnp.repeat(jnp.exp(steps), shape[position] // parts).reshape((-1,) + (1,) * (len(shape) - 1 - position))
    return factor_of


def gaussian(key, extent, deviation, bound, cuts=(), held_as=jnp.bfloat16):
    loudness = block_scale(key, extent, cuts, -0.22, 0.18) if cuts else 1.0
    entries = jax.random.normal(key, extent, jnp.float32) * deviation * loudness
    return jnp.minimum(jnp.maximum(entries, -bound), bound).astype(held_as)


def setup_inputs(seed: int = 0) -> dict:
    arg_keys = jax.random.split(jax.random.key(seed), 5)
    coeffs = gaussian(arg_keys[0], (KPTS, NBLK, 2, NB, 128), 0.0755, 0.44921875, ((0, 16), (1, 2)))
    neighbour = draw_neighbour(jax.random.fold_in(arg_keys[4], 71), 0)
    shift_id = place_ends(jax.random.randint(arg_keys[2], (KPTS, NBV), 0, NSHIFT), jax.random.fold_in(arg_keys[2], 1), 0, NSHIFT - 1).astype(jnp.int32)
    block_map = draw_block_map(jax.random.fold_in(arg_keys[4], 71), 0)
    return dict(coeffs=coeffs, neighbour=neighbour, shift_id=shift_id, block_map=block_map)


def pair_product(left, right):
    return jnp.einsum("jmw,jnw->mn", left, right, precision=lax.Precision.HIGHEST)


def reference(coeffs, neighbour, shift_id, block_map):
    bra_points = (jnp.arange(KPTS * NBV, dtype=jnp.int32) // NBV).astype(jnp.int32)
    ket_points = neighbour.reshape(-1).astype(jnp.int32)
    shifts_flat = shift_id.reshape(-1).astype(jnp.int32)

    def one_pair(inputs):
        bra_point, ket_point, shift_row = inputs
        bra = coeffs[bra_point].astype(jnp.float32)
        ket = jnp.take(coeffs[ket_point], block_map[shift_row], axis=0).astype(jnp.float32)
        real_part = pair_product(bra[:, 0], ket[:, 0]) + pair_product(bra[:, 1], ket[:, 1])
        imag_part = pair_product(bra[:, 0], ket[:, 1]) - pair_product(bra[:, 1], ket[:, 0])
        return jnp.stack([real_part, imag_part])

    result = lax.map(one_pair, (bra_points, ket_points, shifts_flat))
    return result.reshape(KPTS, NBV, 2, NB, NB)
```

```python
import functools

import jax
import jax.numpy as jnp
from jax import lax
from jax.sharding import PartitionSpec as P
from jax.experimental import pallas as pl
from jax.experimental.pallas import tpu as pltpu

CHUNKS = 10
ROLES = 3


def shifted(block, axis, distance):
    devices = range(lax.axis_size(axis))
    route = [((i - distance) % len(devices), i) for i in devices]
    return lax.ppermute(block, axis, route)


def complex_intersection(bra_real, bra_imag, ket_real, ket_imag, form):
    real_part = jnp.einsum(form, bra_real, ket_real, preferred_element_type=jnp.float32)
    real_part = real_part + jnp.einsum(form, bra_imag, ket_imag, preferred_element_type=jnp.float32)
    imag_part = jnp.einsum(form, bra_real, ket_imag, preferred_element_type=jnp.float32)
    imag_part = imag_part - jnp.einsum(form, bra_imag, ket_real, preferred_element_type=jnp.float32)
    return jnp.stack([real_part, imag_part], axis=-3)


def slot_plan(
    home_slice, target_slice, sent_local, place_local, my_slice, slices, capacity, slab_blocks
):
    targets = jnp.arange(slices, dtype=jnp.int32)
    chosen = (home_slice == my_slice)[:, None, :] & (
        target_slice[:, None, :] == targets[None, :, None]
    )
    chosen = chosen & (targets != my_slice)[None, :, None]
    counted = jnp.cumsum(chosen.astype(jnp.int32), axis=2) - 1
    places = jnp.arange(capacity, dtype=jnp.int32)
    matched = (
        chosen[:, :, None, :] & (counted[:, :, None, :] == places[None, None, :, None])
    ).astype(jnp.int32)
    filled = jnp.sum(matched, axis=3)
    sent_block = jnp.sum(matched * sent_local[:, None, None, :], axis=3)
    where_to = jnp.sum(matched * place_local[:, None, None, :], axis=3) + (1 - filled) * slab_blocks
    pair_count = home_slice.shape[0]
    return (
        sent_block.reshape(pair_count, slices * capacity),
        where_to.reshape(pair_count, slices * capacity),
    )


def on_device(coeffs, neighbour, shift_id, block_map):
    k_local = coeffs.shape[0]
    slab_blocks = coeffs.shape[1]
    band_count = coeffs.shape[3]
    lane_width = coeffs.shape[4]
    vector_count = neighbour.shape[1]
    cycle_size = lax.axis_size("ka")
    slices = lax.axis_size("ga")
    my_cycle = lax.axis_index("ka")
    my_slice = lax.axis_index("ga")
    capacity = 2 * max(1, slab_blocks // 12)
    all_blocks = slab_blocks * slices
    pair_count = k_local * vector_count
    k_total = k_local * cycle_size
    row_points = min(16, k_total // 4)
    row_devices = row_points // k_local
    pad_spec = ((0, 0), (0, 1), (0, 0), (0, 0), (0, 0))
    row_point = shifted(coeffs, "ka", -1)
    row_source = jnp.mod(my_cycle + 1, cycle_size)
    plane_kets = shifted(coeffs, "ka", -row_devices)
    plane_source = jnp.mod(my_cycle + row_devices, cycle_size)
    opposite = shifted(coeffs, "ka", cycle_size // 2)
    targets_flat = neighbour.reshape(-1)
    shifts_flat = shift_id.reshape(-1)
    target_device = targets_flat // k_local
    target_lane = targets_flat - target_device * k_local
    ket_index = jnp.where(
        target_device == my_cycle,
        target_lane,
        jnp.where(
            target_device == row_source,
            k_local,
            jnp.where(
                target_device == plane_source,
                k_local + 1 + target_lane,
                2 * k_local + 1 + target_lane,
            ),
        ),
    )
    bra_index = jnp.arange(pair_count, dtype=jnp.int32) // vector_count
    picks = (
        shifts_flat[:, None] == jnp.arange(block_map.shape[0], dtype=jnp.int32)[None, :]
    ).astype(jnp.int32)
    relabel = jnp.sum(picks[:, :, None] * block_map[None, :, :], axis=1)
    dest_global = jnp.broadcast_to(jnp.arange(all_blocks, dtype=jnp.int32)[None, :], relabel.shape)
    source_slice = relabel // slab_blocks
    dest_slice = dest_global // slab_blocks
    source_local = relabel - source_slice * slab_blocks
    dest_local = dest_global - dest_slice * slab_blocks
    kets = jnp.pad(jnp.concatenate([coeffs, row_point, plane_kets, opposite], axis=0), pad_spec)
    own_source = lax.dynamic_slice_in_dim(relabel, my_slice * slab_blocks, slab_blocks, 1)
    self_place = jnp.where(
        own_source // slab_blocks == my_slice, own_source - my_slice * slab_blocks, slab_blocks
    )
    ket_self = kets[ket_index[:, None], self_place]
    ket_self = ket_self.reshape(k_local, vector_count, slab_blocks, 2, band_count, lane_width)
    local_terms = complex_intersection(
        coeffs[:, :, 0],
        coeffs[:, :, 1],
        ket_self[:, :, :, 0],
        ket_self[:, :, :, 1],
        "ksmw,kbsnw->kbmn",
    )
    sent_block, where_to = slot_plan(
        dest_slice, source_slice, dest_local, source_local, my_slice, slices, capacity, slab_blocks
    )
    payload = coeffs[bra_index[:, None], sent_block]
    owner = jnp.broadcast_to(ket_index[:, None], (pair_count, slices))
    blocks = lax.all_to_all(payload, "ga", split_axis=1, concat_axis=1, tiled=True)
    places_in = lax.all_to_all(where_to, "ga", split_axis=1, concat_axis=1, tiled=True)
    owners = lax.all_to_all(owner, "ga", split_axis=1, concat_axis=1, tiled=True)
    partner = kets[owners[:, 0][:, None], places_in]
    remote = complex_intersection(
        blocks[:, :, 0], blocks[:, :, 1], partner[:, :, 0], partner[:, :, 1], "ismw,isnw->imn"
    )
    summed_part = local_terms + remote.reshape(k_local, vector_count, 2, band_count, band_count)
    total = lax.psum(summed_part, "ga")
    row_count = band_count // slices
    return lax.dynamic_slice_in_dim(total, my_slice * row_count, row_count, 3)


def index_tables(block_map, my_slice, slab, capacity):
    shifts, blocks = block_map.shape
    exact = jnp.bfloat16
    base = (my_slice * slab).astype(jnp.float32)

    def lane_product(left, right, axis):
        return lax.dot_general(
            left.astype(exact), right.astype(exact), (((1,), (axis,)), ((), ())),
            preferred_element_type=jnp.float32,
        )

    def ones(mask):
        return jnp.where(mask, 1.0, 0.0)

    def place_rows(table):
        return lax.broadcasted_iota(jnp.int32, table.shape, 0)

    forward = block_map.astype(jnp.float32)
    counted = lax.broadcasted_iota(jnp.int32, (shifts, blocks), 1).astype(jnp.float32)
    block_rows = lax.broadcasted_iota(jnp.int32, (blocks, blocks), 0)
    inverse = jnp.zeros((shifts, blocks), jnp.float32)
    for r in range(shifts):
        row = lane_product(counted, ones(block_map[r : r + 1, :] == block_rows), 1)
        inverse = jnp.where(place_rows(row) == r, row, inverse)
    before = ones(
        lax.broadcasted_iota(jnp.int32, (slab, slab), 0)
        < lax.broadcasted_iota(jnp.int32, (slab, slab), 1)
    )
    padded = -(-capacity // 8) * 8
    slots = lax.broadcasted_iota(jnp.int32, (padded, slab), 0).astype(jnp.float32)
    indexes, sends = [], []
    for table in (forward, inverse):
        low, high = table[:, :slab], table[:, slab:]
        mine = jnp.where(my_slice == 0, low, high) - base
        other = jnp.where(my_slice == 0, high, low) - base
        inside = (mine >= 0) & (mine < slab)
        rank = jnp.minimum(lane_product(1.0 - ones(inside), before, 0), capacity - 1.0)
        at = jnp.where(inside, mine, slab + rank).astype(jnp.int32)
        indexes.append(jnp.clip(at, 0, slab + capacity - 1))
        wanted = ones((other >= 0) & (other < slab))
        rank = lane_product(wanted, before, 0)
        rank = jnp.where(wanted > 0, rank, -1.0)
        send = jnp.zeros((shifts, padded), jnp.float32)
        for r in range(shifts):
            row = lane_product(other, ones(rank[r : r + 1, :] == slots), 1)
            send = jnp.where(place_rows(row) == r, row, send)
        sends.append(jnp.clip(send.astype(jnp.int32), 0, slab - 1))
    return indexes, sends, padded


def meet_kernel(
    points, slab, capacity, near_ref, shift_ref, map_ref, own_hbm, out_ref,
    own, first, second, third, extra, packs, landed, meta_out, meta_in, tables,
    sums, results, slots, meta, table_at,
    local_sems, meta_sems, send_sems, first_sems, second_sems, third_sems, extra_sems,
    swap_send, swap_recv, result_send, result_recv, go,
):
    levels = points // (points // 4)
    row = points // levels
    me = lax.axis_index("ka")
    my_slice = lax.axis_index("ga")
    partner = 1 - my_slice
    z, column = me // row, me % row
    low = (column == 0) | (column == row - 1)
    role = jnp.where(low, z, levels - 1 - z)
    is_outer, is_hub, is_inner, is_far = role == 0, role == 1, role == 2, role == 3

    def member(r):
        return jnp.where(low, r, levels - 1 - r) * row + column

    outer, hub, inner, far = member(0), member(1), member(2), member(3)
    twin = me + 1 - 2 * (column % 2)
    lower_half = z < 2
    bands, lanes = own.shape[2], own.shape[3]
    size = slab // CHUNKS
    shifts = map_ref.shape[0]

    barrier = pltpu.get_barrier_semaphore()
    mesh = pl.DeviceIdType.MESH

    def greet(r, carry):
        peer = (me + r) % points
        for g in range(2):
            pl.semaphore_signal(barrier, inc=1, device_id={"ka": peer, "ga": g}, device_id_type=mesh)
        return carry

    lax.fori_loop(1, points, greet, 0)
    pl.semaphore_signal(barrier, inc=1, device_id={"ga": partner}, device_id_type=mesh)
    pl.semaphore_wait(barrier, 2 * points - 1)

    def remote(source, target, send, recv, peer):
        return pltpu.make_async_remote_copy(
            src_ref=source, dst_ref=target, send_sem=send, recv_sem=recv,
            device_id=peer, device_id_type=mesh,
        )

    def chunk(c):
        return pl.ds(c * size, size)

    def own_part(c, target, n, sems, peer):
        return remote(own_hbm.at[chunk(c)], target.at[chunk(c)], send_sems.at[n], sems.at[c], {"ka": peer})

    def send_own(target, n, sems, peer, start=0, stop=CHUNKS):
        for c in range(start, stop):
            own_part(c, target, n, sems, peer).start()

    def sent_own(n, chunks):
        part = own_hbm.at[pl.ds(0, chunks * size)]
        return remote(part, own.at[pl.ds(0, chunks * size)], send_sems.at[n], first_sems.at[0], {"ka": twin})

    keep = pltpu.make_async_copy(own_hbm, own.at[pl.ds(0, slab)], local_sems.at[0])

    @pl.when(is_outer)
    def _():
        send_own(first, 0, first_sems, hub, 0, CHUNKS - 1)
        send_own(first, 1, first_sems, hub, CHUNKS - 1, CHUNKS)

    @pl.when(is_inner)
    def _():
        send_own(second, 0, second_sems, hub, 0, CHUNKS - 1)
        send_own(second, 1, second_sems, hub, CHUNKS - 1, CHUNKS)

    corner_low = me == row
    corner_high = me == 2 * row - 1
    gated_extra = me == row + 2
    extra_down = (me == row) | (me == 2)
    extra_up = (me == 2 * row + 1) | (me == 2 * row + 3) | (me == 3 * row + 1)
    extra_source = extra_down | extra_up | corner_high | gated_extra
    extra_site = (
        (me == row - 1) | (me == 1) | (me == row + 1)
        | (me == 2 * row + 2) | (me == 3 * row) | (me == 3 * row + 2)
    )
    extra_peer = jnp.where(corner_high, row, jnp.where(extra_up, me + 1, me - 1))

    @pl.when(extra_down | extra_up | corner_high)
    def _():
        send_own(extra, 3, extra_sems, extra_peer)

    @pl.when(is_outer | is_hub)
    def _():
        send_own(first, 2, first_sems, twin)

    keep.start()

    def role_shift(step):
        target = (me + step) % points
        total = jnp.int32(0)
        for b in range(ROLES):
            total = total + jnp.where(near_ref[0, b] == target, shift_ref[0, b], 0)
        return total

    lane = lax.broadcasted_iota(jnp.int32, meta_out.shape, 1)
    facts = jnp.where(
        lane == 0, role_shift(1), jnp.where(lane == 1, role_shift(row), role_shift(points // 2))
    )
    meta_out[...] = facts
    meta_in[me] = facts

    indexes, sends, padded = index_tables(map_ref[...], my_slice, slab, capacity)
    tables[...] = jnp.zeros_like(tables)
    for d in range(2):
        tables[pl.ds(d * shifts, shifts), pl.ds(0, slab)] = indexes[d]
        tables[pl.ds((2 + d) * shifts, shifts), pl.ds(0, padded)] = sends[d]

    def tell(r, carry):
        remote(meta_out, meta_in.at[me], meta_sems.at[0], meta_sems.at[1], {"ka": (me + r) % points}).start()
        return carry

    lax.fori_loop(1, points, tell, 0)
    told = meta_in.at[pl.ds(0, points - 1)]
    all_told = remote(told, told, meta_sems.at[0], meta_sems.at[1], {"ka": twin})
    tables_in = pltpu.make_async_copy(tables, table_at, local_sems.at[1])
    tables_in.start()
    all_told.wait_recv()
    meta_copy = pltpu.make_async_copy(meta_in, meta, local_sems.at[2])
    meta_copy.start()
    all_told.wait_send()
    meta_copy.wait()
    tables_in.wait()
    keep.wait()

    def shift_of(point, kind):
        return meta[point, 0, kind]

    NEXT, ROW, HALF = 0, 1, 2

    def swap(n):
        part = pl.ds(n * capacity, capacity)
        return remote(packs.at[part], landed.at[part], swap_send.at[n], swap_recv.at[n], {"ga": partner})

    def take(n, target, place):
        swap(n).wait_recv()

        def move(r, carry):
            target[slab + place * capacity + r] = landed[n * capacity + r]
            return carry

        lax.fori_loop(0, capacity, move, 0, unroll=4)

    def pack(n, source, inverse, shift):
        line = (2 + inverse) * shifts + shift

        def gather(r, carry):
            packs[n * capacity + r] = source[table_at[line, r]]
            return carry

        lax.fori_loop(0, capacity, gather, 0, unroll=4)

    def offer(n, source, inverse, shift):
        pack(n, source, inverse, shift)
        swap(n).start()

    def pick(ref, at):
        return ref[at].reshape(2 * bands, lanes)

    def accumulate(e, c, still, moving, place, inverse, shift):
        line = inverse * shifts + shift

        def at(n):
            value = table_at[line, n]
            return value + jnp.where(value >= slab, place * capacity, 0)

        total = sums[e]
        for u in range(0, size, 2):
            n = c * size + u
            total = total + lax.dot_general(
                jnp.concatenate([pick(still, n), pick(still, n + 1)], axis=1),
                jnp.concatenate([pick(moving, at(n)), pick(moving, at(n + 1))], axis=1),
                (((1,), (1,)), ((), ())),
                preferred_element_type=jnp.float32,
            )
        sums[e] = total

    def whole(e, still, moving, place, inverse, shift):
        def step(c, carry):
            accumulate(e, c, still, moving, place, inverse, shift)
            return carry

        lax.fori_loop(0, CHUNKS, step, 0)

    def result_copies(e, kind, bra):
        pairs = []
        half = bands // 2
        for g in range(2):
            source = results.at[e, pl.ds(g * half, half)]
            target = slots.at[kind, my_slice]
            arrived = result_recv.at[kind * 2 + my_slice]
            at_home = (bra == me) & (my_slice == g)
            near = pltpu.make_async_copy(source, target, arrived)
            away = remote(source, target, result_send.at[e * 2 + g], arrived, {"ka": bra, "ga": g})
            pairs.append((at_home, near, away))
        return pairs

    def deliver(e, kind, bra, inverse):
        total = sums[e]
        total = jnp.where(inverse == 1, total.T, total)
        upper, under = total[:bands], pltpu.roll(total[bands:], bands, 1)
        left = lax.broadcasted_iota(jnp.int32, upper.shape, 1) < bands
        results[e] = upper + jnp.where(left, under, -under)
        for at_home, near, away in result_copies(e, kind, bra):
            pl.when(at_home)(near.start)
            pl.when(~at_home)(away.start)

    def delivered(e, kind, bra):
        for at_home, _, away in result_copies(e, kind, bra):
            pl.when(~at_home)(away.wait_send)

    def arrived(buffer, sems, c):
        part = buffer.at[chunk(c)]
        remote(part, part, send_sems.at[0], sems.at[c], {"ka": twin}).wait_recv()

    sums[...] = jnp.zeros_like(sums)
    flip = jnp.where(low, 0, 1)
    extra_inverse = jnp.where(lower_half, 1, 0)
    extra_bra = jnp.where(lower_half, me, me - 1)
    EXTRA = 6
    OWN_EXTRA = 4
    OUTER_SLOT, INNER_SLOT, CORNER_SLOT = 5, 6, 7

    hub_edges = (
        (first, own, 0, flip, jnp.where(low, outer, hub), ROW),
        (second, own, 1, 1 - flip, jnp.where(low, hub, inner), ROW),
        (third, own, 2, 1, hub, HALF),
        (third, own, 3, 0, far, HALF),
        (third, first, 0, flip, jnp.where(low, far, outer), ROW),
        (third, second, 0, 1 - flip, jnp.where(low, inner, far), ROW),
    )

    @pl.when(extra_site)
    def _():
        offer(OWN_EXTRA, own, extra_inverse, shift_of(extra_bra, NEXT))

    def extra_edge():
        take(OWN_EXTRA, own, OWN_EXTRA)
        shift = shift_of(extra_bra, NEXT)

        def step(c, carry):
            arrived(extra, extra_sems, c)
            accumulate(EXTRA, c, extra, own, OWN_EXTRA, extra_inverse, shift)
            return carry

        lax.fori_loop(0, CHUNKS, step, 0)
        deliver(EXTRA, NEXT, extra_bra, extra_inverse)

    def corner_copy(c):
        return remote(first.at[chunk(c)], extra.at[chunk(c)], send_sems.at[5], extra_sems.at[c], {"ka": 2 * row - 1})

    @pl.when(is_hub)
    def _():
        for e in range(4):
            _, _, _, inverse, bra, kind = hub_edges[e]
            offer(e, own, inverse, shift_of(bra, kind))

        def relay(c, carry):
            arrived(second, second_sems, c)
            remote(second.at[chunk(c)], first.at[chunk(c)], send_sems.at[4], first_sems.at[c], {"ka": outer}).start()
            arrived(first, first_sems, c)
            pl.when(corner_low)(corner_copy(c).start)
            return carry

        lax.fori_loop(0, CHUNKS, relay, 0)

        @pl.when(corner_high)
        def _():
            sent_own(3, CHUNKS).wait_send()
            pl.semaphore_signal(go, inc=1, device_id={"ka": twin}, device_id_type=mesh)

        for n, e in ((OUTER_SLOT, 4), (INNER_SLOT, 5)):
            _, source, _, inverse, bra, kind = hub_edges[e]
            offer(n, source, inverse, shift_of(bra, kind))

        @pl.when(corner_low)
        def _():
            offer(CORNER_SLOT, second, 0, shift_of(2 * row - 1, NEXT))

        for e in range(2):
            still, moving, place, inverse, bra, kind = hub_edges[e]
            take(e, own, e)
            whole(e, still, moving, place, inverse, shift_of(bra, kind))
            deliver(e, kind, bra, inverse)

        @pl.when(extra_site)
        def _():
            extra_edge()

        @pl.when(corner_high)
        def _():
            def gain(c, carry):
                arrived(extra, extra_sems, c)
                return carry

            lax.fori_loop(0, CHUNKS, gain, 0)
            offer(CORNER_SLOT, extra, 0, shift_of(4 * row - 1, NEXT))

        for e in (2, 3):
            take(e, own, e)
        take(OUTER_SLOT, first, 0)
        take(INNER_SLOT, second, 0)

        @pl.when(corner_low)
        def _():
            take(CORNER_SLOT, second, 1)

            def step(c, carry):
                arrived(extra, extra_sems, c)
                accumulate(EXTRA, c, extra, second, 1, 0, shift_of(2 * row - 1, NEXT))
                return carry

            lax.fori_loop(0, CHUNKS, step, 0)
            deliver(EXTRA, NEXT, 2 * row - 1, 0)

        @pl.when(corner_high)
        def _():
            take(CORNER_SLOT, extra, 0)

        def late(c, carry):
            arrived(third, third_sems, c)
            for e in range(2, 6):
                still, moving, place, inverse, bra, kind = hub_edges[e]
                accumulate(e, c, still, moving, place, inverse, shift_of(bra, kind))

            @pl.when(corner_high)
            def _():
                accumulate(EXTRA, c, third, extra, 0, 0, shift_of(4 * row - 1, NEXT))

            return carry

        lax.fori_loop(0, CHUNKS, late, 0)
        for e in range(2, 6):
            _, _, _, inverse, bra, kind = hub_edges[e]
            deliver(e, kind, bra, inverse)

        @pl.when(corner_high)
        def _():
            deliver(EXTRA, NEXT, 4 * row - 1, 0)

        for e in range(6):
            _, _, _, _, bra, kind = hub_edges[e]
            delivered(e, kind, bra)

        @pl.when(corner_low)
        def _():
            delivered(EXTRA, NEXT, 2 * row - 1)
            swap(CORNER_SLOT).wait_send()
            sent_own(5, CHUNKS).wait_send()

        @pl.when(corner_high)
        def _():
            delivered(EXTRA, NEXT, 4 * row - 1)
            swap(CORNER_SLOT).wait_send()

        for e in range(4):
            swap(e).wait_send()
        swap(OUTER_SLOT).wait_send()
        swap(INNER_SLOT).wait_send()
        sent_own(4, CHUNKS).wait_send()

    @pl.when(is_outer)
    def _():
        for e, inverse, bra in ((0, 1, outer), (1, 0, inner)):
            offer(e, own, inverse, shift_of(bra, HALF))
        sent_own(0, CHUNKS - 1).wait_send()
        pl.semaphore_signal(go, inc=1, device_id={"ka": twin}, device_id_type=mesh)
        for e in range(2):
            take(e, own, e)

        def step(c, carry):
            arrived(first, first_sems, c)
            for e, inverse, bra in ((0, 1, outer), (1, 0, inner)):
                accumulate(e, c, first, own, e, inverse, shift_of(bra, HALF))
            return carry

        lax.fori_loop(0, CHUNKS, step, 0)
        for e, inverse, bra in ((0, 1, outer), (1, 0, inner)):
            deliver(e, HALF, bra, inverse)
        pl.when(extra_site)(extra_edge)
        for e, inverse, bra in ((0, 1, outer), (1, 0, inner)):
            delivered(e, HALF, bra)
            swap(e).wait_send()

    twin_inverse = jnp.where(column % 2 == 1, 0, 1)
    twin_bra = me - column % 2

    @pl.when(is_inner | is_far)
    def _():
        shift = shift_of(twin_bra, NEXT)
        offer(0, own, twin_inverse, shift)
        take(0, own, 0)

        def step(c, carry):
            arrived(first, first_sems, c)
            accumulate(0, c, first, own, 0, twin_inverse, shift)
            return carry

        lax.fori_loop(0, CHUNKS, step, 0)
        deliver(0, NEXT, twin_bra, twin_inverse)

        @pl.when(is_far | gated_extra)
        def _():
            pl.semaphore_wait(go, 1)

        @pl.when(is_far)
        def _():
            send_own(third, 0, third_sems, hub, 0, CHUNKS - 1)
            send_own(third, 1, third_sems, hub, CHUNKS - 1, CHUNKS)

        @pl.when(gated_extra)
        def _():
            send_own(extra, 3, extra_sems, extra_peer)

        pl.when(extra_site)(extra_edge)
        delivered(0, NEXT, twin_bra)
        swap(0).wait_send()
        sent_own(0, CHUNKS - 1).wait_send()

    @pl.when(extra_site)
    def _():
        delivered(EXTRA, NEXT, extra_bra)
        swap(OWN_EXTRA).wait_send()

    @pl.when(~is_hub)
    def _():
        sent_own(1, 1).wait_send()

    @pl.when(is_outer | is_hub)
    def _():
        sent_own(2, CHUNKS).wait_send()

    @pl.when(extra_source)
    def _():
        @pl.when(~corner_high)
        def _():
            sent_own(3, CHUNKS).wait_send()

    for kind in range(ROLES):
        for g in range(2):
            slot = slots.at[kind, g]
            pltpu.make_async_copy(slot, slot, result_recv.at[kind * 2 + g]).wait()
        both = slots[kind, 0] + slots[kind, 1]
        out_ref[kind, 0] = both[:, :bands]
        out_ref[kind, 1] = both[:, bands:]


def meet(neighbour, shift_id, block_map, own, points, capacity):
    slab, bands, lanes = own.shape[0], own.shape[2], own.shape[3]
    block = own.shape[1:]
    shifts = block_map.shape[0]
    half = bands // 2
    dma = pltpu.SemaphoreType.DMA

    def blocks(count):
        return pltpu.VMEM((count,) + block, own.dtype)

    return pl.pallas_call(
        functools.partial(meet_kernel, points, slab, capacity),
        out_shape=jax.ShapeDtypeStruct((ROLES, 2, half, bands), jnp.float32),
        in_specs=[
            pl.BlockSpec(memory_space=pltpu.SMEM),
            pl.BlockSpec(memory_space=pltpu.SMEM),
            pl.BlockSpec(memory_space=pltpu.VMEM),
            pl.BlockSpec(memory_space=pl.ANY),
        ],
        out_specs=pl.BlockSpec(memory_space=pltpu.VMEM),
        scratch_shapes=[
            blocks(slab + 5 * capacity),
            blocks(slab + capacity),
            blocks(slab + 2 * capacity),
            blocks(slab),
            blocks(slab + capacity),
            blocks(8 * capacity),
            blocks(8 * capacity),
            pltpu.VMEM((1, lanes), jnp.int32),
            pltpu.VMEM((points, 1, lanes), jnp.int32),
            pltpu.VMEM((4 * shifts, lanes), jnp.int32),
            pltpu.VMEM((7, 2 * bands, 2 * bands), jnp.float32),
            pltpu.VMEM((7, bands, 2 * bands), jnp.float32),
            pltpu.VMEM((ROLES, 2, half, 2 * bands), jnp.float32),
            pltpu.SMEM((points, 1, lanes), jnp.int32),
            pltpu.SMEM((4 * shifts, lanes), jnp.int32),
            dma((3,)), dma((2,)), dma((6,)),
            dma((CHUNKS,)), dma((CHUNKS,)), dma((CHUNKS,)), dma((CHUNKS,)),
            dma((8,)), dma((8,)), dma((14,)), dma((2 * ROLES,)),
            pltpu.SemaphoreType.REGULAR,
        ],
        compiler_params=pltpu.CompilerParams(
            collective_id=0, has_side_effects=True, vmem_limit_bytes=60 * 2**20
        ),
        name="meet",
    )(neighbour, shift_id, block_map, own)


def on_four_levels(coeffs, neighbour, shift_id, block_map):
    own = coeffs[0]
    points = lax.axis_size("ka")
    row = points // 4
    me = lax.axis_index("ka")
    capacity = 2 * max(1, own.shape[0] // 12)
    sums = meet(neighbour, shift_id, block_map, own, points, capacity)
    target = neighbour[0][:, None, None, None]
    out = jnp.where(
        target == jnp.mod(me + 1, points),
        sums[0],
        jnp.where(target == jnp.mod(me + row, points), sums[1], sums[2]),
    )
    return out[None]


def solution(mesh):
    in_specs = (P("ka", "ga", None, None, None), P("ka", None), P("ka", None), P())
    out_specs = P("ka", None, None, "ga", None)
    levels = mesh.shape["ka"] // 4
    square = mesh.shape["ga"] == 2 and mesh.shape["ka"] == 4 * levels and levels == 4

    def run(coeffs, neighbour, shift_id, block_map):
        one_each = coeffs.shape[0] == mesh.shape["ka"] and neighbour.shape[1] == ROLES
        per_slice = coeffs.shape[1] // mesh.shape["ga"]
        lanes = coeffs.shape[4]
        fits = per_slice % (2 * CHUNKS) == 0 and per_slice <= lanes and 2 * coeffs.shape[3] == lanes
        body = on_four_levels if square and one_each and fits else on_device
        return jax.shard_map(
            body, mesh=mesh, in_specs=in_specs, out_specs=out_specs, check_vma=False
        )(coeffs, neighbour, shift_id, block_map)

    return run
```

```python
import functools

import jax
import jax.numpy as jnp
from jax import lax
from jax.sharding import PartitionSpec as P
from jax.experimental import pallas as pl
from jax.experimental.pallas import tpu as pltpu

CHUNKS = 10
ROLES = 3


def shifted(block, axis, distance):
    devices = range(lax.axis_size(axis))
    route = [((i - distance) % len(devices), i) for i in devices]
    return lax.ppermute(block, axis, route)


def complex_intersection(bra_real, bra_imag, ket_real, ket_imag, form):
    real_part = jnp.einsum(form, bra_real, ket_real, preferred_element_type=jnp.float32)
    real_part = real_part + jnp.einsum(form, bra_imag, ket_imag, preferred_element_type=jnp.float32)
    imag_part = jnp.einsum(form, bra_real, ket_imag, preferred_element_type=jnp.float32)
    imag_part = imag_part - jnp.einsum(form, bra_imag, ket_real, preferred_element_type=jnp.float32)
    return jnp.stack([real_part, imag_part], axis=-3)


def slot_plan(
    home_slice, target_slice, sent_local, place_local, my_slice, slices, capacity, slab_blocks
):
    targets = jnp.arange(slices, dtype=jnp.int32)
    chosen = (home_slice == my_slice)[:, None, :] & (
        target_slice[:, None, :] == targets[None, :, None]
    )
    chosen = chosen & (targets != my_slice)[None, :, None]
    counted = jnp.cumsum(chosen.astype(jnp.int32), axis=2) - 1
    places = jnp.arange(capacity, dtype=jnp.int32)
    matched = (
        chosen[:, :, None, :] & (counted[:, :, None, :] == places[None, None, :, None])
    ).astype(jnp.int32)
    filled = jnp.sum(matched, axis=3)
    sent_block = jnp.sum(matched * sent_local[:, None, None, :], axis=3)
    where_to = jnp.sum(matched * place_local[:, None, None, :], axis=3) + (1 - filled) * slab_blocks
    pair_count = home_slice.shape[0]
    return (
        sent_block.reshape(pair_count, slices * capacity),
        where_to.reshape(pair_count, slices * capacity),
    )


def on_device(coeffs, neighbour, shift_id, block_map):
    k_local = coeffs.shape[0]
    slab_blocks = coeffs.shape[1]
    band_count = coeffs.shape[3]
    lane_width = coeffs.shape[4]
    vector_count = neighbour.shape[1]
    cycle_size = lax.axis_size("ka")
    slices = lax.axis_size("ga")
    my_cycle = lax.axis_index("ka")
    my_slice = lax.axis_index("ga")
    capacity = 2 * max(1, slab_blocks // 12)
    all_blocks = slab_blocks * slices
    pair_count = k_local * vector_count
    k_total = k_local * cycle_size
    row_points = min(16, k_total // 4)
    row_devices = row_points // k_local
    pad_spec = ((0, 0), (0, 1), (0, 0), (0, 0), (0, 0))
    row_point = shifted(coeffs, "ka", -1)
    row_source = jnp.mod(my_cycle + 1, cycle_size)
    plane_kets = shifted(coeffs, "ka", -row_devices)
    plane_source = jnp.mod(my_cycle + row_devices, cycle_size)
    opposite = shifted(coeffs, "ka", cycle_size // 2)
    targets_flat = neighbour.reshape(-1)
    shifts_flat = shift_id.reshape(-1)
    target_device = targets_flat // k_local
    target_lane = targets_flat - target_device * k_local
    ket_index = jnp.where(
        target_device == my_cycle,
        target_lane,
        jnp.where(
            target_device == row_source,
            k_local,
            jnp.where(
                target_device == plane_source,
                k_local + 1 + target_lane,
                2 * k_local + 1 + target_lane,
            ),
        ),
    )
    bra_index = jnp.arange(pair_count, dtype=jnp.int32) // vector_count
    picks = (
        shifts_flat[:, None] == jnp.arange(block_map.shape[0], dtype=jnp.int32)[None, :]
    ).astype(jnp.int32)
    relabel = jnp.sum(picks[:, :, None] * block_map[None, :, :], axis=1)
    dest_global = jnp.broadcast_to(jnp.arange(all_blocks, dtype=jnp.int32)[None, :], relabel.shape)
    source_slice = relabel // slab_blocks
    dest_slice = dest_global // slab_blocks
    source_local = relabel - source_slice * slab_blocks
    dest_local = dest_global - dest_slice * slab_blocks
    kets = jnp.pad(jnp.concatenate([coeffs, row_point, plane_kets, opposite], axis=0), pad_spec)
    own_source = lax.dynamic_slice_in_dim(relabel, my_slice * slab_blocks, slab_blocks, 1)
    self_place = jnp.where(
        own_source // slab_blocks == my_slice, own_source - my_slice * slab_blocks, slab_blocks
    )
    ket_self = kets[ket_index[:, None], self_place]
    ket_self = ket_self.reshape(k_local, vector_count, slab_blocks, 2, band_count, lane_width)
    local_terms = complex_intersection(
        coeffs[:, :, 0],
        coeffs[:, :, 1],
        ket_self[:, :, :, 0],
        ket_self[:, :, :, 1],
        "ksmw,kbsnw->kbmn",
    )
    sent_block, where_to = slot_plan(
        dest_slice, source_slice, dest_local, source_local, my_slice, slices, capacity, slab_blocks
    )
    payload = coeffs[bra_index[:, None], sent_block]
    owner = jnp.broadcast_to(ket_index[:, None], (pair_count, slices))
    blocks = lax.all_to_all(payload, "ga", split_axis=1, concat_axis=1, tiled=True)
    places_in = lax.all_to_all(where_to, "ga", split_axis=1, concat_axis=1, tiled=True)
    owners = lax.all_to_all(owner, "ga", split_axis=1, concat_axis=1, tiled=True)
    partner = kets[owners[:, 0][:, None], places_in]
    remote = complex_intersection(
        blocks[:, :, 0], blocks[:, :, 1], partner[:, :, 0], partner[:, :, 1], "ismw,isnw->imn"
    )
    summed_part = local_terms + remote.reshape(k_local, vector_count, 2, band_count, band_count)
    total = lax.psum(summed_part, "ga")
    row_count = band_count // slices
    return lax.dynamic_slice_in_dim(total, my_slice * row_count, row_count, 3)


def index_tables(block_map, my_slice, slab, capacity):
    shifts, blocks = block_map.shape
    exact = jnp.bfloat16
    base = (my_slice * slab).astype(jnp.float32)

    def lane_product(left, right, axis):
        return lax.dot_general(
            left.astype(exact), right.astype(exact), (((1,), (axis,)), ((), ())),
            preferred_element_type=jnp.float32,
        )

    def ones(mask):
        return jnp.where(mask, 1.0, 0.0)

    def place_rows(table):
        return lax.broadcasted_iota(jnp.int32, table.shape, 0)

    forward = block_map.astype(jnp.float32)
    counted = lax.broadcasted_iota(jnp.int32, (shifts, blocks), 1).astype(jnp.float32)
    block_rows = lax.broadcasted_iota(jnp.int32, (blocks, blocks), 0)
    inverse = jnp.zeros((shifts, blocks), jnp.float32)
    for r in range(shifts):
        row = lane_product(counted, ones(block_map[r : r + 1, :] == block_rows), 1)
        inverse = jnp.where(place_rows(row) == r, row, inverse)
    before = ones(
        lax.broadcasted_iota(jnp.int32, (slab, slab), 0)
        < lax.broadcasted_iota(jnp.int32, (slab, slab), 1)
    )
    padded = -(-capacity // 8) * 8
    slots = lax.broadcasted_iota(jnp.int32, (padded, slab), 0).astype(jnp.float32)
    indexes, sends = [], []
    for table in (forward, inverse):
        low, high = table[:, :slab], table[:, slab:]
        mine = jnp.where(my_slice == 0, low, high) - base
        other = jnp.where(my_slice == 0, high, low) - base
        inside = (mine >= 0) & (mine < slab)
        rank = jnp.minimum(lane_product(1.0 - ones(inside), before, 0), capacity - 1.0)
        at = jnp.where(inside, mine, slab + rank).astype(jnp.int32)
        indexes.append(jnp.clip(at, 0, slab + capacity - 1))
        wanted = ones((other >= 0) & (other < slab))
        rank = lane_product(wanted, before, 0)
        rank = jnp.where(wanted > 0, rank, -1.0)
        send = jnp.zeros((shifts, padded), jnp.float32)
        for r in range(shifts):
            row = lane_product(other, ones(rank[r : r + 1, :] == slots), 1)
            send = jnp.where(place_rows(row) == r, row, send)
        sends.append(jnp.clip(send.astype(jnp.int32), 0, slab - 1))
    return indexes, sends, padded


def meet_kernel(
    points, slab, capacity, near_ref, shift_ref, map_ref, own_hbm, out_ref,
    own, first, second, third, extra, packs, landed, meta_out, meta_in, tables,
    sums, results, slots, meta, table_at,
    local_sems, meta_sems, send_sems, first_sems, second_sems, third_sems, extra_sems,
    swap_send, swap_recv, result_send, result_recv, go,
):
    levels = points // (points // 4)
    row = points // levels
    me = lax.axis_index("ka")
    my_slice = lax.axis_index("ga")
    partner = 1 - my_slice
    z, column = me // row, me % row
    low = (column == 0) | (column == row - 1)
    role = jnp.where(low, z, levels - 1 - z)
    is_outer, is_hub, is_inner, is_far = role == 0, role == 1, role == 2, role == 3

    def member(r):
        return jnp.where(low, r, levels - 1 - r) * row + column

    outer, hub, inner, far = member(0), member(1), member(2), member(3)
    twin = me + 1 - 2 * (column % 2)
    lower_half = z < 2
    bands, lanes = own.shape[2], own.shape[3]
    size = slab // CHUNKS
    shifts = map_ref.shape[0]

    barrier = pltpu.get_barrier_semaphore()
    mesh = pl.DeviceIdType.MESH

    def greet(r, carry):
        peer = (me + r) % points
        for g in range(2):
            pl.semaphore_signal(barrier, inc=1, device_id={"ka": peer, "ga": g}, device_id_type=mesh)
        return carry

    def role_shift(step):
        target = (me + step) % points
        total = jnp.int32(0)
        for b in range(ROLES):
            total = total + jnp.where(near_ref[0, b] == target, shift_ref[0, b], 0)
        return total

    keep = pltpu.make_async_copy(own_hbm, own.at[pl.ds(0, slab)], local_sems.at[0])
    keep.start()
    lane = lax.broadcasted_iota(jnp.int32, meta_out.shape, 1)
    facts = jnp.where(
        lane == 0, role_shift(1), jnp.where(lane == 1, role_shift(row), role_shift(points // 2))
    )
    meta_out[...] = facts
    meta_in[me] = facts

    lax.fori_loop(1, points, greet, 0)
    pl.semaphore_signal(barrier, inc=1, device_id={"ga": partner}, device_id_type=mesh)
    pl.semaphore_wait(barrier, 2 * points - 1)

    def remote(source, target, send, recv, peer):
        return pltpu.make_async_remote_copy(
            src_ref=source, dst_ref=target, send_sem=send, recv_sem=recv,
            device_id=peer, device_id_type=mesh,
        )

    def chunk(c):
        return pl.ds(c * size, size)

    def own_part(c, target, n, sems, peer):
        return remote(own_hbm.at[chunk(c)], target.at[chunk(c)], send_sems.at[n], sems.at[c], {"ka": peer})

    def send_own(target, n, sems, peer):
        for c in range(CHUNKS):
            own_part(c, target, n, sems, peer).start()

    def sent_own(n):
        return remote(own_hbm, own.at[pl.ds(0, slab)], send_sems.at[n], first_sems.at[0], {"ka": twin})

    def tell(r, carry):
        remote(meta_out, meta_in.at[me], meta_sems.at[0], meta_sems.at[1], {"ka": (me + r) % points}).start()
        return carry

    lax.fori_loop(1, points, tell, 0)

    @pl.when(is_outer)
    def _():
        send_own(first, 0, first_sems, hub)

    @pl.when(is_inner)
    def _():
        send_own(second, 0, second_sems, hub)

    corner_low = me == row
    corner_high = me == 2 * row - 1
    gated_extra = me == row + 2
    extra_down = me == 2
    extra_up = (me == 2 * row + 1) | (me == 2 * row + 3) | (me == 3 * row + 1)
    extra_source = extra_down | extra_up | corner_low | gated_extra
    extra_site = (
        (me == row - 1) | (me == 1) | (me == row + 1)
        | (me == 2 * row + 2) | (me == 3 * row) | (me == 3 * row + 2)
    )
    extra_peer = jnp.where(corner_high, row, jnp.where(extra_up, me + 1, me - 1))

    @pl.when(extra_down | extra_up | corner_high)
    def _():
        send_own(extra, 3, extra_sems, extra_peer)

    @pl.when(is_outer | is_hub)
    def _():
        send_own(first, 2, first_sems, twin)

    indexes, sends, padded = index_tables(map_ref[...], my_slice, slab, capacity)
    tables[...] = jnp.zeros_like(tables)
    for d in range(2):
        tables[pl.ds(d * shifts, shifts), pl.ds(0, slab)] = indexes[d]
        tables[pl.ds((2 + d) * shifts, shifts), pl.ds(0, padded)] = sends[d]

    told = meta_in.at[pl.ds(0, points - 1)]
    all_told = remote(told, told, meta_sems.at[0], meta_sems.at[1], {"ka": twin})
    tables_in = pltpu.make_async_copy(tables, table_at, local_sems.at[1])
    tables_in.start()
    all_told.wait_recv()
    meta_copy = pltpu.make_async_copy(meta_in, meta, local_sems.at[2])
    meta_copy.start()
    all_told.wait_send()
    meta_copy.wait()
    tables_in.wait()
    keep.wait()

    def shift_of(point, kind):
        return meta[point, 0, kind]

    NEXT, ROW, HALF = 0, 1, 2

    def swap(n):
        part = pl.ds(n * capacity, capacity)
        return remote(packs.at[part], landed.at[part], swap_send.at[n], swap_recv.at[n], {"ga": partner})

    def take(n, target, place):
        swap(n).wait_recv()

        def move(r, carry):
            target[slab + place * capacity + r] = landed[n * capacity + r]
            return carry

        lax.fori_loop(0, capacity, move, 0, unroll=4)

    def pack(n, source, inverse, shift):
        line = (2 + inverse) * shifts + shift

        def gather(r, carry):
            packs[n * capacity + r] = source[table_at[line, r]]
            return carry

        lax.fori_loop(0, capacity, gather, 0, unroll=4)

    def offer(n, source, inverse, shift):
        pack(n, source, inverse, shift)
        swap(n).start()

    def pick(ref, at):
        return ref[at].reshape(2 * bands, lanes)

    def accumulate(e, c, still, moving, place, inverse, shift):
        line = inverse * shifts + shift

        def at(n):
            value = table_at[line, n]
            return value + jnp.where(value >= slab, place * capacity, 0)

        total = sums[e]
        for u in range(0, size, 2):
            n = c * size + u
            total = total + lax.dot_general(
                jnp.concatenate([pick(still, n), pick(still, n + 1)], axis=1),
                jnp.concatenate([pick(moving, at(n)), pick(moving, at(n + 1))], axis=1),
                (((1,), (1,)), ((), ())),
                preferred_element_type=jnp.float32,
            )
        sums[e] = total

    def whole(e, still, moving, place, inverse, shift):
        def step(c, carry):
            accumulate(e, c, still, moving, place, inverse, shift)
            return carry

        lax.fori_loop(0, CHUNKS, step, 0)

    def result_copies(e, kind, bra):
        pairs = []
        half = bands // 2
        for g in range(2):
            source = results.at[e, pl.ds(g * half, half)]
            target = slots.at[kind, my_slice]
            arrived = result_recv.at[kind * 2 + my_slice]
            at_home = (bra == me) & (my_slice == g)
            near = pltpu.make_async_copy(source, target, arrived)
            away = remote(source, target, result_send.at[e * 2 + g], arrived, {"ka": bra, "ga": g})
            pairs.append((at_home, near, away))
        return pairs

    def deliver(e, kind, bra, inverse):
        total = sums[e]
        total = jnp.where(inverse == 1, total.T, total)
        upper, under = total[:bands], pltpu.roll(total[bands:], bands, 1)
        left = lax.broadcasted_iota(jnp.int32, upper.shape, 1) < bands
        results[e] = upper + jnp.where(left, under, -under)
        for at_home, near, away in result_copies(e, kind, bra):
            pl.when(at_home)(near.start)
            pl.when(~at_home)(away.start)

    def delivered(e, kind, bra):
        for at_home, _, away in result_copies(e, kind, bra):
            pl.when(~at_home)(away.wait_send)

    def arrived(buffer, sems, c):
        part = buffer.at[chunk(c)]
        remote(part, part, send_sems.at[0], sems.at[c], {"ka": twin}).wait_recv()

    sums[...] = jnp.zeros_like(sums)
    flip = jnp.where(low, 0, 1)
    extra_inverse = jnp.where(lower_half, 1, 0)
    extra_bra = jnp.where(lower_half, me, me - 1)
    EXTRA = 6
    OWN_EXTRA = 4
    OUTER_SLOT, INNER_SLOT, CORNER_SLOT = 5, 6, 7

    hub_edges = (
        (first, own, 0, flip, jnp.where(low, outer, hub), ROW),
        (second, own, 1, 1 - flip, jnp.where(low, hub, inner), ROW),
        (third, own, 2, 1, hub, HALF),
        (third, own, 3, 0, far, HALF),
        (third, first, 0, flip, jnp.where(low, far, outer), ROW),
        (third, second, 0, 1 - flip, jnp.where(low, inner, far), ROW),
    )

    @pl.when(extra_site)
    def _():
        offer(OWN_EXTRA, own, extra_inverse, shift_of(extra_bra, NEXT))

    def extra_edge():
        take(OWN_EXTRA, own, OWN_EXTRA)
        shift = shift_of(extra_bra, NEXT)

        def step(c, carry):
            arrived(extra, extra_sems, c)
            accumulate(EXTRA, c, extra, own, OWN_EXTRA, extra_inverse, shift)
            return carry

        lax.fori_loop(0, CHUNKS, step, 0)
        deliver(EXTRA, NEXT, extra_bra, extra_inverse)

    def corner_copy(c):
        return remote(first.at[chunk(c)], extra.at[chunk(c)], send_sems.at[5], extra_sems.at[c], {"ka": 2 * row - 1})

    @pl.when(is_hub)
    def _():
        for e in range(4):
            _, _, _, inverse, bra, kind = hub_edges[e]
            offer(e, own, inverse, shift_of(bra, kind))

        def relay(c, carry):
            arrived(second, second_sems, c)
            remote(second.at[chunk(c)], first.at[chunk(c)], send_sems.at[4], first_sems.at[c], {"ka": outer}).start()
            arrived(first, first_sems, c)
            pl.when(corner_low)(corner_copy(c).start)
            return carry

        lax.fori_loop(0, CHUNKS, relay, 0)

        @pl.when(corner_low)
        def _():
            send_own(extra, 3, extra_sems, extra_peer)

        @pl.when(corner_high)
        def _():
            sent_own(3).wait_send()
            pl.semaphore_signal(go, inc=1, device_id={"ka": twin}, device_id_type=mesh)

        for n, e in ((OUTER_SLOT, 4), (INNER_SLOT, 5)):
            _, source, _, inverse, bra, kind = hub_edges[e]
            offer(n, source, inverse, shift_of(bra, kind))

        @pl.when(corner_low)
        def _():
            offer(CORNER_SLOT, second, 0, shift_of(2 * row - 1, NEXT))

        for e in range(2):
            still, moving, place, inverse, bra, kind = hub_edges[e]
            take(e, own, e)
            whole(e, still, moving, place, inverse, shift_of(bra, kind))
            deliver(e, kind, bra, inverse)

        @pl.when(extra_site)
        def _():
            extra_edge()

        @pl.when(corner_high)
        def _():
            def gain(c, carry):
                arrived(extra, extra_sems, c)
                return carry

            lax.fori_loop(0, CHUNKS, gain, 0)
            offer(CORNER_SLOT, extra, 0, shift_of(4 * row - 1, NEXT))

        for e in (2, 3):
            take(e, own, e)
        take(OUTER_SLOT, first, 0)
        take(INNER_SLOT, second, 0)

        @pl.when(corner_low)
        def _():
            take(CORNER_SLOT, second, 1)

            def step(c, carry):
                arrived(extra, extra_sems, c)
                accumulate(EXTRA, c, extra, second, 1, 0, shift_of(2 * row - 1, NEXT))
                return carry

            lax.fori_loop(0, CHUNKS, step, 0)
            deliver(EXTRA, NEXT, 2 * row - 1, 0)

        @pl.when(corner_high)
        def _():
            take(CORNER_SLOT, extra, 0)

        def late(c, carry):
            arrived(third, third_sems, c)
            for e in range(2, 6):
                still, moving, place, inverse, bra, kind = hub_edges[e]
                accumulate(e, c, still, moving, place, inverse, shift_of(bra, kind))

            @pl.when(corner_high)
            def _():
                accumulate(EXTRA, c, third, extra, 0, 0, shift_of(4 * row - 1, NEXT))

            return carry

        lax.fori_loop(0, CHUNKS, late, 0)
        for e in range(2, 6):
            _, _, _, inverse, bra, kind = hub_edges[e]
            deliver(e, kind, bra, inverse)

        @pl.when(corner_high)
        def _():
            deliver(EXTRA, NEXT, 4 * row - 1, 0)

        for e in range(6):
            _, _, _, _, bra, kind = hub_edges[e]
            delivered(e, kind, bra)

        @pl.when(corner_low)
        def _():
            delivered(EXTRA, NEXT, 2 * row - 1)
            swap(CORNER_SLOT).wait_send()
            sent_own(5).wait_send()

        @pl.when(corner_high)
        def _():
            delivered(EXTRA, NEXT, 4 * row - 1)
            swap(CORNER_SLOT).wait_send()

        for e in range(4):
            swap(e).wait_send()
        swap(OUTER_SLOT).wait_send()
        swap(INNER_SLOT).wait_send()
        sent_own(4).wait_send()

    @pl.when(is_outer)
    def _():
        for e, inverse, bra in ((0, 1, outer), (1, 0, inner)):
            offer(e, own, inverse, shift_of(bra, HALF))
        sent_own(0).wait_send()
        pl.semaphore_signal(go, inc=1, device_id={"ka": twin}, device_id_type=mesh)
        for e in range(2):
            take(e, own, e)

        def step(c, carry):
            arrived(first, first_sems, c)
            for e, inverse, bra in ((0, 1, outer), (1, 0, inner)):
                accumulate(e, c, first, own, e, inverse, shift_of(bra, HALF))
            return carry

        lax.fori_loop(0, CHUNKS, step, 0)
        for e, inverse, bra in ((0, 1, outer), (1, 0, inner)):
            deliver(e, HALF, bra, inverse)
        pl.when(extra_site)(extra_edge)
        for e, inverse, bra in ((0, 1, outer), (1, 0, inner)):
            delivered(e, HALF, bra)
            swap(e).wait_send()

    twin_inverse = jnp.where(column % 2 == 1, 0, 1)
    twin_bra = me - column % 2

    @pl.when(is_inner | is_far)
    def _():
        shift = shift_of(twin_bra, NEXT)
        offer(0, own, twin_inverse, shift)
        take(0, own, 0)

        def step(c, carry):
            arrived(first, first_sems, c)
            accumulate(0, c, first, own, 0, twin_inverse, shift)
            return carry

        lax.fori_loop(0, CHUNKS, step, 0)
        deliver(0, NEXT, twin_bra, twin_inverse)

        @pl.when(is_inner)
        def _():
            sent_own(0).wait_send()
            pl.semaphore_signal(go, inc=1, device_id={"ka": far}, device_id_type=mesh)

        @pl.when(gated_extra)
        def _():
            pl.semaphore_wait(go, 1)

        @pl.when(is_far)
        def _():
            pl.semaphore_wait(go, 2)
            send_own(third, 0, third_sems, hub)

        @pl.when(gated_extra)
        def _():
            send_own(extra, 3, extra_sems, extra_peer)

        pl.when(extra_site)(extra_edge)
        delivered(0, NEXT, twin_bra)
        swap(0).wait_send()
        pl.when(is_far)(sent_own(0).wait_send)

    @pl.when(extra_site)
    def _():
        delivered(EXTRA, NEXT, extra_bra)
        swap(OWN_EXTRA).wait_send()

    @pl.when(is_outer | is_hub)
    def _():
        sent_own(2).wait_send()

    @pl.when(extra_source)
    def _():
        sent_own(3).wait_send()

    for kind in range(ROLES):
        for g in range(2):
            slot = slots.at[kind, g]
            pltpu.make_async_copy(slot, slot, result_recv.at[kind * 2 + g]).wait()
        both = slots[kind, 0] + slots[kind, 1]
        out_ref[kind, 0] = both[:, :bands]
        out_ref[kind, 1] = both[:, bands:]


def meet(neighbour, shift_id, block_map, own, points, capacity):
    slab, bands, lanes = own.shape[0], own.shape[2], own.shape[3]
    block = own.shape[1:]
    shifts = block_map.shape[0]
    half = bands // 2
    dma = pltpu.SemaphoreType.DMA

    def blocks(count):
        return pltpu.VMEM((count,) + block, own.dtype)

    return pl.pallas_call(
        functools.partial(meet_kernel, points, slab, capacity),
        out_shape=jax.ShapeDtypeStruct((ROLES, 2, half, bands), jnp.float32),
        in_specs=[
            pl.BlockSpec(memory_space=pltpu.SMEM),
            pl.BlockSpec(memory_space=pltpu.SMEM),
            pl.BlockSpec(memory_space=pltpu.VMEM),
            pl.BlockSpec(memory_space=pl.ANY),
        ],
        out_specs=pl.BlockSpec(memory_space=pltpu.VMEM),
        scratch_shapes=[
            blocks(slab + 5 * capacity),
            blocks(slab + capacity),
            blocks(slab + 2 * capacity),
            blocks(slab),
            blocks(slab + capacity),
            blocks(8 * capacity),
            blocks(8 * capacity),
            pltpu.VMEM((1, lanes), jnp.int32),
            pltpu.VMEM((points, 1, lanes), jnp.int32),
            pltpu.VMEM((4 * shifts, lanes), jnp.int32),
            pltpu.VMEM((7, 2 * bands, 2 * bands), jnp.float32),
            pltpu.VMEM((7, bands, 2 * bands), jnp.float32),
            pltpu.VMEM((ROLES, 2, half, 2 * bands), jnp.float32),
            pltpu.SMEM((points, 1, lanes), jnp.int32),
            pltpu.SMEM((4 * shifts, lanes), jnp.int32),
            dma((3,)), dma((2,)), dma((6,)),
            dma((CHUNKS,)), dma((CHUNKS,)), dma((CHUNKS,)), dma((CHUNKS,)),
            dma((8,)), dma((8,)), dma((14,)), dma((2 * ROLES,)),
            pltpu.SemaphoreType.REGULAR,
        ],
        compiler_params=pltpu.CompilerParams(
            collective_id=0, has_side_effects=True, vmem_limit_bytes=60 * 2**20
        ),
        name="meet",
    )(neighbour, shift_id, block_map, own)


def on_four_levels(coeffs, neighbour, shift_id, block_map):
    own = coeffs[0]
    points = lax.axis_size("ka")
    row = points // 4
    me = lax.axis_index("ka")
    capacity = 2 * max(1, own.shape[0] // 12)
    sums = meet(neighbour, shift_id, block_map, own, points, capacity)
    target = neighbour[0][:, None, None, None]
    out = jnp.where(
        target == jnp.mod(me + 1, points),
        sums[0],
        jnp.where(target == jnp.mod(me + row, points), sums[1], sums[2]),
    )
    return out[None]


def solution(mesh):
    in_specs = (P("ka", "ga", None, None, None), P("ka", None), P("ka", None), P())
    out_specs = P("ka", None, None, "ga", None)
    levels = mesh.shape["ka"] // 4
    square = mesh.shape["ga"] == 2 and mesh.shape["ka"] == 4 * levels and levels == 4

    def run(coeffs, neighbour, shift_id, block_map):
        one_each = coeffs.shape[0] == mesh.shape["ka"] and neighbour.shape[1] == ROLES
        per_slice = coeffs.shape[1] // mesh.shape["ga"]
        lanes = coeffs.shape[4]
        fits = per_slice % (2 * CHUNKS) == 0 and per_slice <= lanes and 2 * coeffs.shape[3] == lanes
        body = on_four_levels if square and one_each and fits else on_device
        return jax.shard_map(
            body, mesh=mesh, in_specs=in_specs, out_specs=out_specs, check_vma=False
        )(coeffs, neighbour, shift_id, block_map)

    return run
```

```python
import functools

import jax
import jax.numpy as jnp
from jax import lax
from jax.sharding import PartitionSpec as P
from jax.experimental import pallas as pl
from jax.experimental.pallas import tpu as pltpu

CHUNKS = 20
EARLY = 3
LUMP = 4
ROLES = 3


def shifted(block, axis, distance):
    devices = range(lax.axis_size(axis))
    route = [((i - distance) % len(devices), i) for i in devices]
    return lax.ppermute(block, axis, route)


def complex_intersection(bra_real, bra_imag, ket_real, ket_imag, form):
    real_part = jnp.einsum(form, bra_real, ket_real, preferred_element_type=jnp.float32)
    real_part = real_part + jnp.einsum(form, bra_imag, ket_imag, preferred_element_type=jnp.float32)
    imag_part = jnp.einsum(form, bra_real, ket_imag, preferred_element_type=jnp.float32)
    imag_part = imag_part - jnp.einsum(form, bra_imag, ket_real, preferred_element_type=jnp.float32)
    return jnp.stack([real_part, imag_part], axis=-3)


def slot_plan(
    home_slice, target_slice, sent_local, place_local, my_slice, slices, capacity, slab_blocks
):
    targets = jnp.arange(slices, dtype=jnp.int32)
    chosen = (home_slice == my_slice)[:, None, :] & (
        target_slice[:, None, :] == targets[None, :, None]
    )
    chosen = chosen & (targets != my_slice)[None, :, None]
    counted = jnp.cumsum(chosen.astype(jnp.int32), axis=2) - 1
    places = jnp.arange(capacity, dtype=jnp.int32)
    matched = (
        chosen[:, :, None, :] & (counted[:, :, None, :] == places[None, None, :, None])
    ).astype(jnp.int32)
    filled = jnp.sum(matched, axis=3)
    sent_block = jnp.sum(matched * sent_local[:, None, None, :], axis=3)
    where_to = jnp.sum(matched * place_local[:, None, None, :], axis=3) + (1 - filled) * slab_blocks
    pair_count = home_slice.shape[0]
    return (
        sent_block.reshape(pair_count, slices * capacity),
        where_to.reshape(pair_count, slices * capacity),
    )


def on_device(coeffs, neighbour, shift_id, block_map):
    k_local = coeffs.shape[0]
    slab_blocks = coeffs.shape[1]
    band_count = coeffs.shape[3]
    lane_width = coeffs.shape[4]
    vector_count = neighbour.shape[1]
    cycle_size = lax.axis_size("ka")
    slices = lax.axis_size("ga")
    my_cycle = lax.axis_index("ka")
    my_slice = lax.axis_index("ga")
    capacity = 2 * max(1, slab_blocks // 12)
    all_blocks = slab_blocks * slices
    pair_count = k_local * vector_count
    k_total = k_local * cycle_size
    row_points = min(16, k_total // 4)
    row_devices = row_points // k_local
    pad_spec = ((0, 0), (0, 1), (0, 0), (0, 0), (0, 0))
    row_point = shifted(coeffs, "ka", -1)
    row_source = jnp.mod(my_cycle + 1, cycle_size)
    plane_kets = shifted(coeffs, "ka", -row_devices)
    plane_source = jnp.mod(my_cycle + row_devices, cycle_size)
    opposite = shifted(coeffs, "ka", cycle_size // 2)
    targets_flat = neighbour.reshape(-1)
    shifts_flat = shift_id.reshape(-1)
    target_device = targets_flat // k_local
    target_lane = targets_flat - target_device * k_local
    ket_index = jnp.where(
        target_device == my_cycle,
        target_lane,
        jnp.where(
            target_device == row_source,
            k_local,
            jnp.where(
                target_device == plane_source,
                k_local + 1 + target_lane,
                2 * k_local + 1 + target_lane,
            ),
        ),
    )
    bra_index = jnp.arange(pair_count, dtype=jnp.int32) // vector_count
    picks = (
        shifts_flat[:, None] == jnp.arange(block_map.shape[0], dtype=jnp.int32)[None, :]
    ).astype(jnp.int32)
    relabel = jnp.sum(picks[:, :, None] * block_map[None, :, :], axis=1)
    dest_global = jnp.broadcast_to(jnp.arange(all_blocks, dtype=jnp.int32)[None, :], relabel.shape)
    source_slice = relabel // slab_blocks
    dest_slice = dest_global // slab_blocks
    source_local = relabel - source_slice * slab_blocks
    dest_local = dest_global - dest_slice * slab_blocks
    kets = jnp.pad(jnp.concatenate([coeffs, row_point, plane_kets, opposite], axis=0), pad_spec)
    own_source = lax.dynamic_slice_in_dim(relabel, my_slice * slab_blocks, slab_blocks, 1)
    self_place = jnp.where(
        own_source // slab_blocks == my_slice, own_source - my_slice * slab_blocks, slab_blocks
    )
    ket_self = kets[ket_index[:, None], self_place]
    ket_self = ket_self.reshape(k_local, vector_count, slab_blocks, 2, band_count, lane_width)
    local_terms = complex_intersection(
        coeffs[:, :, 0],
        coeffs[:, :, 1],
        ket_self[:, :, :, 0],
        ket_self[:, :, :, 1],
        "ksmw,kbsnw->kbmn",
    )
    sent_block, where_to = slot_plan(
        dest_slice, source_slice, dest_local, source_local, my_slice, slices, capacity, slab_blocks
    )
    payload = coeffs[bra_index[:, None], sent_block]
    owner = jnp.broadcast_to(ket_index[:, None], (pair_count, slices))
    blocks = lax.all_to_all(payload, "ga", split_axis=1, concat_axis=1, tiled=True)
    places_in = lax.all_to_all(where_to, "ga", split_axis=1, concat_axis=1, tiled=True)
    owners = lax.all_to_all(owner, "ga", split_axis=1, concat_axis=1, tiled=True)
    partner = kets[owners[:, 0][:, None], places_in]
    remote = complex_intersection(
        blocks[:, :, 0], blocks[:, :, 1], partner[:, :, 0], partner[:, :, 1], "ismw,isnw->imn"
    )
    summed_part = local_terms + remote.reshape(k_local, vector_count, 2, band_count, band_count)
    total = lax.psum(summed_part, "ga")
    row_count = band_count // slices
    return lax.dynamic_slice_in_dim(total, my_slice * row_count, row_count, 3)


def index_tables(block_map, my_slice, slab, capacity):
    shifts, blocks = block_map.shape
    exact = jnp.bfloat16
    base = (my_slice * slab).astype(jnp.float32)

    def lane_product(left, right, axis):
        return lax.dot_general(
            left.astype(exact), right.astype(exact), (((1,), (axis,)), ((), ())),
            preferred_element_type=jnp.float32,
        )

    def ones(mask):
        return jnp.where(mask, 1.0, 0.0)

    def place_rows(table):
        return lax.broadcasted_iota(jnp.int32, table.shape, 0)

    forward = block_map.astype(jnp.float32)
    counted = lax.broadcasted_iota(jnp.int32, (shifts, blocks), 1).astype(jnp.float32)
    block_rows = lax.broadcasted_iota(jnp.int32, (blocks, blocks), 0)
    inverse = jnp.zeros((shifts, blocks), jnp.float32)
    for r in range(shifts):
        row = lane_product(counted, ones(block_map[r : r + 1, :] == block_rows), 1)
        inverse = jnp.where(place_rows(row) == r, row, inverse)
    before = ones(
        lax.broadcasted_iota(jnp.int32, (slab, slab), 0)
        < lax.broadcasted_iota(jnp.int32, (slab, slab), 1)
    )
    padded = -(-capacity // 8) * 8
    slots = lax.broadcasted_iota(jnp.int32, (padded, slab), 0).astype(jnp.float32)
    indexes, sends = [], []
    for table in (forward, inverse):
        low, high = table[:, :slab], table[:, slab:]
        mine = jnp.where(my_slice == 0, low, high) - base
        other = jnp.where(my_slice == 0, high, low) - base
        inside = (mine >= 0) & (mine < slab)
        rank = jnp.minimum(lane_product(1.0 - ones(inside), before, 0), capacity - 1.0)
        at = jnp.where(inside, mine, slab + rank).astype(jnp.int32)
        indexes.append(jnp.clip(at, 0, slab + capacity - 1))
        wanted = ones((other >= 0) & (other < slab))
        rank = lane_product(wanted, before, 0)
        rank = jnp.where(wanted > 0, rank, -1.0)
        send = jnp.zeros((shifts, padded), jnp.float32)
        for r in range(shifts):
            row = lane_product(other, ones(rank[r : r + 1, :] == slots), 1)
            send = jnp.where(place_rows(row) == r, row, send)
        sends.append(jnp.clip(send.astype(jnp.int32), 0, slab - 1))
    return indexes, sends, padded


def meet_kernel(
    points, slab, capacity, near_hbm, shift_hbm, map_hbm, own_hbm, out_ref,
    near_ref, shift_ref, map_ref, own, first, second, third, extra, packs, landed, meta_out, meta_in, tables,
    sums, results, slots, meta, table_at,
    local_sems, meta_sems, send_sems, first_sems, second_sems, third_sems, extra_sems,
    swap_send, swap_recv, result_send, result_recv, go,
):
    levels = points // (points // 4)
    row = points // levels
    me = lax.axis_index("ka")
    my_slice = lax.axis_index("ga")
    partner = 1 - my_slice
    z, column = me // row, me % row
    low = (column == 0) | (column == row - 1)
    role = jnp.where(low, z, levels - 1 - z)
    is_outer, is_hub, is_inner, is_far = role == 0, role == 1, role == 2, role == 3

    def member(r):
        return jnp.where(low, r, levels - 1 - r) * row + column

    outer, hub, inner, far = member(0), member(1), member(2), member(3)
    below, above = hub - row, hub + row
    twin = me + 1 - 2 * (column % 2)
    lower_half = z < 2
    bands, lanes = own.shape[2], own.shape[3]
    size = slab // CHUNKS
    shifts = map_hbm.shape[0]

    barrier = pltpu.get_barrier_semaphore()
    mesh = pl.DeviceIdType.MESH

    def greet(r, carry):
        peer = (me + r) % points
        for g in range(2):
            pl.semaphore_signal(barrier, inc=1, device_id={"ka": peer, "ga": g}, device_id_type=mesh)
        return carry

    lax.fori_loop(1, points, greet, 0)
    pl.semaphore_signal(barrier, inc=1, device_id={"ga": partner}, device_id_type=mesh)
    near_in = pltpu.make_async_copy(near_hbm, near_ref, local_sems.at[3])
    shift_in = pltpu.make_async_copy(shift_hbm, shift_ref, local_sems.at[4])
    map_in = pltpu.make_async_copy(map_hbm, map_ref, local_sems.at[5])
    keep = pltpu.make_async_copy(own_hbm, own.at[pl.ds(0, slab)], local_sems.at[0])
    for copy in (near_in, shift_in, map_in, keep):
        copy.start()
    near_in.wait()
    shift_in.wait()

    def role_shift(step):
        target = (me + step) % points
        total = jnp.int32(0)
        for b in range(ROLES):
            total = total + jnp.where(near_ref[0, b] == target, shift_ref[0, b], 0)
        return total

    lane = lax.broadcasted_iota(jnp.int32, meta_out.shape, 1)
    facts = jnp.where(
        lane == 0, role_shift(1), jnp.where(lane == 1, role_shift(row), role_shift(points // 2))
    )
    meta_out[...] = facts
    meta_in[me] = facts
    pl.semaphore_wait(barrier, 2 * points - 1)

    def remote(source, target, send, recv, peer):
        return pltpu.make_async_remote_copy(
            src_ref=source, dst_ref=target, send_sem=send, recv_sem=recv,
            device_id=peer, device_id_type=mesh,
        )

    def chunk(c):
        return pl.ds(c * size, size)

    def own_part(c, target, n, sems, peer):
        return remote(own_hbm.at[chunk(c)], target.at[chunk(c)], send_sems.at[n], sems.at[c], {"ka": peer})

    def send_own(target, n, sems, peer, start=0, stop=CHUNKS):
        for c in range(start, stop):
            own_part(c, target, n, sems, peer).start()

    def sent_own(n, chunks=CHUNKS):
        part = pl.ds(0, chunks * size)
        return remote(own_hbm.at[part], own.at[part], send_sems.at[n], first_sems.at[0], {"ka": twin})

    def tell(r, carry):
        remote(meta_out, meta_in.at[me], meta_sems.at[0], meta_sems.at[1], {"ka": (me + r) % points}).start()
        return carry

    lax.fori_loop(1, points, tell, 0)


    @pl.when(me == below)
    def _():
        send_own(first, 0, first_sems, hub, 0, CHUNKS - 1)
        send_own(first, 1, first_sems, hub, CHUNKS - 1, CHUNKS)

    @pl.when(me == above)
    def _():
        send_own(second, 0, second_sems, hub, 0, CHUNKS - 1)
        send_own(second, 1, second_sems, hub, CHUNKS - 1, CHUNKS)

    corner_low = me == row
    corner_high = me == 2 * row - 1
    gated_extra = me == row + 2
    extra_down = me == 2
    extra_up = (me == 2 * row + 1) | (me == 2 * row + 3) | (me == 3 * row + 1)
    extra_source = extra_down | extra_up | corner_low | gated_extra
    extra_site = (
        (me == row - 1) | (me == 1) | (me == row + 1)
        | (me == 2 * row + 2) | (me == 3 * row) | (me == 3 * row + 2)
    )
    extra_peer = jnp.where(corner_high, row, jnp.where(extra_up, me + 1, me - 1))

    @pl.when(extra_down | extra_up | corner_high)
    def _():
        send_own(extra, 3, extra_sems, extra_peer)

    @pl.when(corner_low)
    def _():
        send_own(extra, 3, extra_sems, extra_peer, 0, EARLY)

    @pl.when(is_outer | is_hub)
    def _():
        send_own(first, 2, first_sems, twin)

    map_in.wait()
    indexes, sends, padded = index_tables(map_ref[...], my_slice, slab, capacity)
    tables[...] = jnp.zeros_like(tables)
    for d in range(2):
        tables[pl.ds(d * shifts, shifts), pl.ds(0, slab)] = indexes[d]
        tables[pl.ds((2 + d) * shifts, shifts), pl.ds(0, padded)] = sends[d]

    told = meta_in.at[pl.ds(0, points - 1)]
    all_told = remote(told, told, meta_sems.at[0], meta_sems.at[1], {"ka": twin})
    tables_in = pltpu.make_async_copy(tables, table_at, local_sems.at[1])
    tables_in.start()
    all_told.wait_recv()
    meta_copy = pltpu.make_async_copy(meta_in, meta, local_sems.at[2])
    meta_copy.start()
    all_told.wait_send()
    meta_copy.wait()
    tables_in.wait()
    keep.wait()

    def shift_of(point, kind):
        return meta[point, 0, kind]

    NEXT, ROW, HALF = 0, 1, 2

    def swap(n):
        part = pl.ds(n * capacity, capacity)
        return remote(packs.at[part], landed.at[part], swap_send.at[n], swap_recv.at[n], {"ga": partner})

    def take(n, target, place):
        swap(n).wait_recv()

        def move(r, carry):
            target[slab + place * capacity + r] = landed[n * capacity + r]
            return carry

        lax.fori_loop(0, capacity, move, 0, unroll=4)

    def pack(n, source, inverse, shift):
        line = (2 + inverse) * shifts + shift

        def gather(r, carry):
            packs[n * capacity + r] = source[table_at[line, r]]
            return carry

        lax.fori_loop(0, capacity, gather, 0, unroll=4)

    def offer(n, source, inverse, shift):
        pack(n, source, inverse, shift)
        swap(n).start()

    def pick(ref, at):
        return ref[at].reshape(2 * bands, lanes)

    def accumulate(e, c, still, moving, place, inverse, shift, turn=False, count=size):
        line = inverse * shifts + shift

        def at(n):
            value = table_at[line, n]
            return value + jnp.where(value >= slab, place * capacity, 0)

        total = sums[e]
        for u in range(0, count, 2):
            n = c * count + u
            left = jnp.concatenate([pick(still, n), pick(still, n + 1)], axis=1)
            right = jnp.concatenate([pick(moving, at(n)), pick(moving, at(n + 1))], axis=1)
            total = total + lax.dot_general(
                right if turn else left,
                left if turn else right,
                (((1,), (1,)), ((), ())),
                preferred_element_type=jnp.float32,
            )
        sums[e] = total

    def whole(e, still, moving, place, inverse, shift):
        def step(c, carry):
            accumulate(e, c, still, moving, place, inverse, shift, inverse == 1, LUMP * size)
            return carry

        lax.fori_loop(0, CHUNKS // LUMP, step, 0)

    def result_copies(e, kind, bra):
        pairs = []
        half = bands // 2
        for g in range(2):
            source = results.at[e, pl.ds(g * half, half)]
            target = slots.at[kind, my_slice]
            arrived = result_recv.at[kind * 2 + my_slice]
            at_home = (bra == me) & (my_slice == g)
            near = pltpu.make_async_copy(source, target, arrived)
            away = remote(source, target, result_send.at[e * 2 + g], arrived, {"ka": bra, "ga": g})
            pairs.append((at_home, near, away))
        return pairs

    def deliver(e, kind, bra, inverse=None):
        total = sums[e]
        if inverse is not None:
            total = jnp.where(inverse == 1, total.T, total)
        upper, under = total[:bands], pltpu.roll(total[bands:], bands, 1)
        left = lax.broadcasted_iota(jnp.int32, upper.shape, 1) < bands
        results[e] = upper + jnp.where(left, under, -under)
        for at_home, near, away in result_copies(e, kind, bra):
            pl.when(at_home)(near.start)
            pl.when(~at_home)(away.start)

    def delivered(e, kind, bra):
        for at_home, _, away in result_copies(e, kind, bra):
            pl.when(~at_home)(away.wait_send)

    def arrived(buffer, sems, c):
        part = buffer.at[chunk(c)]
        remote(part, part, send_sems.at[0], sems.at[c], {"ka": twin}).wait_recv()

    sums[...] = jnp.zeros_like(sums)
    extra_inverse = jnp.where(lower_half, 1, 0)
    extra_bra = jnp.where(lower_half, me, me - 1)
    EXTRA = 6
    OWN_EXTRA = 4
    BELOW_SLOT, ABOVE_SLOT, CORNER_SLOT = 5, 6, 7

    hub_edges = (
        (first, own, 0, 0, below, ROW),
        (second, own, 1, 1, hub, ROW),
        (third, own, 2, 1, hub, HALF),
        (third, own, 3, 0, far, HALF),
        (third, first, 0, 0, far, ROW),
        (third, second, 0, 1, above, ROW),
    )

    @pl.when(extra_site)
    def _():
        offer(OWN_EXTRA, own, extra_inverse, shift_of(extra_bra, NEXT))

    def extra_edge():
        take(OWN_EXTRA, own, OWN_EXTRA)
        shift = shift_of(extra_bra, NEXT)

        def step(c, carry):
            arrived(extra, extra_sems, c)
            accumulate(EXTRA, c, extra, own, OWN_EXTRA, extra_inverse, shift)
            return carry

        lax.fori_loop(0, CHUNKS, step, 0)
        deliver(EXTRA, NEXT, extra_bra, extra_inverse)

    def corner_copy(c):
        return remote(first.at[chunk(c)], extra.at[chunk(c)], send_sems.at[5], extra_sems.at[c], {"ka": 2 * row - 1})

    @pl.when(is_hub)
    def _():
        for e in range(4):
            _, _, _, inverse, bra, kind = hub_edges[e]
            offer(e, own, inverse, shift_of(bra, kind))

        def relayed(source, c):
            return remote(source.at[chunk(c)], first.at[chunk(c)], send_sems.at[4], first_sems.at[c], {"ka": outer})

        def relay(c, carry):
            arrived(second, second_sems, c)
            pl.when(low)(relayed(second, c).start)
            arrived(first, first_sems, c)
            pl.when(~low)(relayed(first, c).start)
            pl.when(corner_low)(corner_copy(c).start)
            return carry

        lax.fori_loop(0, CHUNKS, relay, 0)

        @pl.when(corner_low)
        def _():
            send_own(extra, 3, extra_sems, extra_peer, EARLY, CHUNKS)

        @pl.when(corner_high)
        def _():
            sent_own(3).wait_send()
            pl.semaphore_signal(go, inc=1, device_id={"ka": twin}, device_id_type=mesh)

        for n, e in ((BELOW_SLOT, 4), (ABOVE_SLOT, 5)):
            _, source, _, inverse, bra, kind = hub_edges[e]
            offer(n, source, inverse, shift_of(bra, kind))

        @pl.when(corner_low)
        def _():
            offer(CORNER_SLOT, second, 0, shift_of(2 * row - 1, NEXT))

        for e in range(2):
            still, moving, place, inverse, bra, kind = hub_edges[e]
            take(e, own, e)
            whole(e, still, moving, place, inverse, shift_of(bra, kind))
            deliver(e, kind, bra)

        @pl.when(extra_site)
        def _():
            extra_edge()

        @pl.when(corner_high)
        def _():
            def gain(c, carry):
                arrived(extra, extra_sems, c)
                return carry

            lax.fori_loop(0, CHUNKS, gain, 0)
            offer(CORNER_SLOT, extra, 0, shift_of(4 * row - 1, NEXT))

        for e in (2, 3):
            take(e, own, e)
        take(BELOW_SLOT, first, 0)
        take(ABOVE_SLOT, second, 0)

        @pl.when(corner_low)
        def _():
            take(CORNER_SLOT, second, 1)

            def step(c, carry):
                arrived(extra, extra_sems, c)
                accumulate(EXTRA, c, extra, second, 1, 0, shift_of(2 * row - 1, NEXT))
                return carry

            lax.fori_loop(0, CHUNKS, step, 0)
            deliver(EXTRA, NEXT, 2 * row - 1)

        @pl.when(corner_high)
        def _():
            take(CORNER_SLOT, extra, 0)

        def late_edge(e, c):
            still, moving, place, inverse, bra, kind = hub_edges[e]
            accumulate(e, c, still, moving, place, inverse, shift_of(bra, kind), inverse == 1)

        def late_corner(c):
            accumulate(EXTRA, c, third, extra, 0, 0, shift_of(4 * row - 1, NEXT))

        def late(c, carry):
            arrived(third, third_sems, c)
            for e in range(2, 6):
                late_edge(e, c)

            @pl.when(corner_high)
            def _():
                late_corner(c)

            return carry

        lax.fori_loop(0, CHUNKS - 1, late, 0)
        arrived(third, third_sems, CHUNKS - 1)

        @pl.when(corner_high)
        def _():
            late_corner(CHUNKS - 1)
            deliver(EXTRA, NEXT, 4 * row - 1)

        for e in (3, 4, 5, 2):
            late_edge(e, CHUNKS - 1)
            deliver(e, hub_edges[e][5], hub_edges[e][4])

        for e in range(6):
            _, _, _, _, bra, kind = hub_edges[e]
            delivered(e, kind, bra)

        @pl.when(corner_low)
        def _():
            delivered(EXTRA, NEXT, 2 * row - 1)
            swap(CORNER_SLOT).wait_send()
            sent_own(5).wait_send()

        @pl.when(corner_high)
        def _():
            delivered(EXTRA, NEXT, 4 * row - 1)
            swap(CORNER_SLOT).wait_send()

        for e in range(4):
            swap(e).wait_send()
        swap(BELOW_SLOT).wait_send()
        swap(ABOVE_SLOT).wait_send()
        sent_own(4).wait_send()

    @pl.when(is_outer)
    def _():
        for e, inverse, bra in ((0, 1, outer), (1, 0, inner)):
            offer(e, own, inverse, shift_of(bra, HALF))
        sent_own(0, CHUNKS - 1).wait_send()
        pl.semaphore_signal(go, inc=1, device_id={"ka": twin}, device_id_type=mesh)
        for e in range(2):
            take(e, own, e)
        pl.when(extra_site & ~lower_half)(extra_edge)

        def step(c, carry):
            arrived(first, first_sems, c)
            for e, inverse, bra in ((0, 1, outer), (1, 0, inner)):
                accumulate(e, c, first, own, e, inverse, shift_of(bra, HALF), inverse == 1)
            return carry

        lax.fori_loop(0, CHUNKS, step, 0)
        for e, inverse, bra in ((0, 1, outer), (1, 0, inner)):
            deliver(e, HALF, bra)
        pl.when(extra_site & lower_half)(extra_edge)
        for e, inverse, bra in ((0, 1, outer), (1, 0, inner)):
            delivered(e, HALF, bra)
            swap(e).wait_send()

    twin_inverse = jnp.where(column % 2 == 1, 0, 1)
    twin_bra = me - column % 2

    @pl.when(is_inner | is_far)
    def _():
        shift = shift_of(twin_bra, NEXT)
        offer(0, own, twin_inverse, shift)
        take(0, own, 0)

        def step(c, carry):
            arrived(first, first_sems, c)
            accumulate(0, c, first, own, 0, twin_inverse, shift)
            return carry

        lax.fori_loop(0, CHUNKS, step, 0)
        deliver(0, NEXT, twin_bra, twin_inverse)

        @pl.when(is_inner)
        def _():
            sent_own(0, CHUNKS - 1).wait_send()
            pl.semaphore_signal(go, inc=1, device_id={"ka": far}, device_id_type=mesh)

        @pl.when(gated_extra)
        def _():
            pl.semaphore_wait(go, 1)

        @pl.when(is_far)
        def _():
            pl.semaphore_wait(go, 2)
            send_own(third, 0, third_sems, hub)

        @pl.when(gated_extra)
        def _():
            send_own(extra, 3, extra_sems, extra_peer)

        pl.when(extra_site)(extra_edge)
        delivered(0, NEXT, twin_bra)
        swap(0).wait_send()
        pl.when(is_far)(sent_own(0).wait_send)

    @pl.when(extra_site)
    def _():
        delivered(EXTRA, NEXT, extra_bra)
        swap(OWN_EXTRA).wait_send()

    @pl.when(is_outer | is_inner)
    def _():
        sent_own(1, 1).wait_send()

    @pl.when(is_outer | is_hub)
    def _():
        sent_own(2).wait_send()

    @pl.when(extra_source)
    def _():
        sent_own(3).wait_send()

    for kind in range(ROLES):
        for g in range(2):
            slot = slots.at[kind, g]
            pltpu.make_async_copy(slot, slot, result_recv.at[kind * 2 + g]).wait()
    found = [slots[kind, 0] + slots[kind, 1] for kind in range(ROLES)]
    for b in range(ROLES):
        target = near_ref[0, b]
        chosen = jnp.where(target == (me + row) % points, found[ROW], found[HALF])
        chosen = jnp.where(target == (me + 1) % points, found[NEXT], chosen)
        out_ref[b, 0] = chosen[:, :bands]
        out_ref[b, 1] = chosen[:, bands:]


def meet(neighbour, shift_id, block_map, own, points, capacity):
    slab, bands, lanes = own.shape[0], own.shape[2], own.shape[3]
    block = own.shape[1:]
    shifts = block_map.shape[0]
    half = bands // 2
    dma = pltpu.SemaphoreType.DMA

    def blocks(count):
        return pltpu.VMEM((count,) + block, own.dtype)

    return pl.pallas_call(
        functools.partial(meet_kernel, points, slab, capacity),
        out_shape=pltpu.VMEM((ROLES, 2, half, bands), jnp.float32),
        in_specs=[pl.BlockSpec(memory_space=pl.ANY)] * 4,
        out_specs=pl.BlockSpec(memory_space=pltpu.VMEM),
        scratch_shapes=[
            pltpu.SMEM(neighbour.shape, jnp.int32),
            pltpu.SMEM(shift_id.shape, jnp.int32),
            pltpu.VMEM(block_map.shape, jnp.int32),
            blocks(slab + 5 * capacity),
            blocks(slab + capacity),
            blocks(slab + 2 * capacity),
            blocks(slab),
            blocks(slab + capacity),
            blocks(8 * capacity),
            blocks(8 * capacity),
            pltpu.VMEM((1, lanes), jnp.int32),
            pltpu.VMEM((points, 1, lanes), jnp.int32),
            pltpu.VMEM((4 * shifts, lanes), jnp.int32),
            pltpu.VMEM((7, 2 * bands, 2 * bands), jnp.float32),
            pltpu.VMEM((7, bands, 2 * bands), jnp.float32),
            pltpu.VMEM((ROLES, 2, half, 2 * bands), jnp.float32),
            pltpu.SMEM((points, 1, lanes), jnp.int32),
            pltpu.SMEM((4 * shifts, lanes), jnp.int32),
            dma((6,)), dma((2,)), dma((6,)),
            dma((CHUNKS,)), dma((CHUNKS,)), dma((CHUNKS,)), dma((CHUNKS,)),
            dma((8,)), dma((8,)), dma((14,)), dma((2 * ROLES,)),
            pltpu.SemaphoreType.REGULAR,
        ],
        compiler_params=pltpu.CompilerParams(
            collective_id=0, has_side_effects=True, vmem_limit_bytes=60 * 2**20
        ),
        name="meet",
    )(neighbour, shift_id, block_map, own)


def on_four_levels(coeffs, neighbour, shift_id, block_map):
    own = coeffs[0]
    points = lax.axis_size("ka")
    capacity = 2 * max(1, own.shape[0] // 12)
    return meet(neighbour, shift_id, block_map, own, points, capacity)[None]


def solution(mesh):
    in_specs = (P("ka", "ga", None, None, None), P("ka", None), P("ka", None), P())
    out_specs = P("ka", None, None, "ga", None)
    levels = mesh.shape["ka"] // 4
    square = mesh.shape["ga"] == 2 and mesh.shape["ka"] == 4 * levels and levels == 4

    def run(coeffs, neighbour, shift_id, block_map):
        one_each = coeffs.shape[0] == mesh.shape["ka"] and neighbour.shape[1] == ROLES
        per_slice = coeffs.shape[1] // mesh.shape["ga"]
        lanes = coeffs.shape[4]
        fits = per_slice % (2 * CHUNKS) == 0 and per_slice <= lanes and 2 * coeffs.shape[3] == lanes
        body = on_four_levels if square and one_each and fits else on_device
        return jax.shard_map(
            body, mesh=mesh, in_specs=in_specs, out_specs=out_specs, check_vma=False
        )(coeffs, neighbour, shift_id, block_map)

    return run
```

```python
import functools

import jax
import jax.numpy as jnp
from jax import lax
from jax.sharding import PartitionSpec as P
from jax.experimental import pallas as pl
from jax.experimental.pallas import tpu as pltpu

EARLY = 2
ROLES = 3


def shifted(block, axis, distance):
    devices = range(lax.axis_size(axis))
    route = [((i - distance) % len(devices), i) for i in devices]
    return lax.ppermute(block, axis, route)


def complex_intersection(bra_real, bra_imag, ket_real, ket_imag, form):
    real_part = jnp.einsum(form, bra_real, ket_real, preferred_element_type=jnp.float32)
    real_part = real_part + jnp.einsum(form, bra_imag, ket_imag, preferred_element_type=jnp.float32)
    imag_part = jnp.einsum(form, bra_real, ket_imag, preferred_element_type=jnp.float32)
    imag_part = imag_part - jnp.einsum(form, bra_imag, ket_real, preferred_element_type=jnp.float32)
    return jnp.stack([real_part, imag_part], axis=-3)


def slot_plan(
    home_slice, target_slice, sent_local, place_local, my_slice, slices, capacity, slab_blocks
):
    targets = jnp.arange(slices, dtype=jnp.int32)
    chosen = (home_slice == my_slice)[:, None, :] & (
        target_slice[:, None, :] == targets[None, :, None]
    )
    chosen = chosen & (targets != my_slice)[None, :, None]
    counted = jnp.cumsum(chosen.astype(jnp.int32), axis=2) - 1
    places = jnp.arange(capacity, dtype=jnp.int32)
    matched = (
        chosen[:, :, None, :] & (counted[:, :, None, :] == places[None, None, :, None])
    ).astype(jnp.int32)
    filled = jnp.sum(matched, axis=3)
    sent_block = jnp.sum(matched * sent_local[:, None, None, :], axis=3)
    where_to = jnp.sum(matched * place_local[:, None, None, :], axis=3) + (1 - filled) * slab_blocks
    pair_count = home_slice.shape[0]
    return (
        sent_block.reshape(pair_count, slices * capacity),
        where_to.reshape(pair_count, slices * capacity),
    )


def on_device(coeffs, neighbour, shift_id, block_map):
    k_local = coeffs.shape[0]
    slab_blocks = coeffs.shape[1]
    band_count = coeffs.shape[3]
    lane_width = coeffs.shape[4]
    vector_count = neighbour.shape[1]
    cycle_size = lax.axis_size("ka")
    slices = lax.axis_size("ga")
    my_cycle = lax.axis_index("ka")
    my_slice = lax.axis_index("ga")
    capacity = 2 * max(1, slab_blocks // 12)
    all_blocks = slab_blocks * slices
    pair_count = k_local * vector_count
    k_total = k_local * cycle_size
    row_points = min(16, k_total // 4)
    row_devices = row_points // k_local
    pad_spec = ((0, 0), (0, 1), (0, 0), (0, 0), (0, 0))
    row_point = shifted(coeffs, "ka", -1)
    row_source = jnp.mod(my_cycle + 1, cycle_size)
    plane_kets = shifted(coeffs, "ka", -row_devices)
    plane_source = jnp.mod(my_cycle + row_devices, cycle_size)
    opposite = shifted(coeffs, "ka", cycle_size // 2)
    targets_flat = neighbour.reshape(-1)
    shifts_flat = shift_id.reshape(-1)
    target_device = targets_flat // k_local
    target_lane = targets_flat - target_device * k_local
    ket_index = jnp.where(
        target_device == my_cycle,
        target_lane,
        jnp.where(
            target_device == row_source,
            k_local,
            jnp.where(
                target_device == plane_source,
                k_local + 1 + target_lane,
                2 * k_local + 1 + target_lane,
            ),
        ),
    )
    bra_index = jnp.arange(pair_count, dtype=jnp.int32) // vector_count
    picks = (
        shifts_flat[:, None] == jnp.arange(block_map.shape[0], dtype=jnp.int32)[None, :]
    ).astype(jnp.int32)
    relabel = jnp.sum(picks[:, :, None] * block_map[None, :, :], axis=1)
    dest_global = jnp.broadcast_to(jnp.arange(all_blocks, dtype=jnp.int32)[None, :], relabel.shape)
    source_slice = relabel // slab_blocks
    dest_slice = dest_global // slab_blocks
    source_local = relabel - source_slice * slab_blocks
    dest_local = dest_global - dest_slice * slab_blocks
    kets = jnp.pad(jnp.concatenate([coeffs, row_point, plane_kets, opposite], axis=0), pad_spec)
    own_source = lax.dynamic_slice_in_dim(relabel, my_slice * slab_blocks, slab_blocks, 1)
    self_place = jnp.where(
        own_source // slab_blocks == my_slice, own_source - my_slice * slab_blocks, slab_blocks
    )
    ket_self = kets[ket_index[:, None], self_place]
    ket_self = ket_self.reshape(k_local, vector_count, slab_blocks, 2, band_count, lane_width)
    local_terms = complex_intersection(
        coeffs[:, :, 0],
        coeffs[:, :, 1],
        ket_self[:, :, :, 0],
        ket_self[:, :, :, 1],
        "ksmw,kbsnw->kbmn",
    )
    sent_block, where_to = slot_plan(
        dest_slice, source_slice, dest_local, source_local, my_slice, slices, capacity, slab_blocks
    )
    payload = coeffs[bra_index[:, None], sent_block]
    owner = jnp.broadcast_to(ket_index[:, None], (pair_count, slices))
    blocks = lax.all_to_all(payload, "ga", split_axis=1, concat_axis=1, tiled=True)
    places_in = lax.all_to_all(where_to, "ga", split_axis=1, concat_axis=1, tiled=True)
    owners = lax.all_to_all(owner, "ga", split_axis=1, concat_axis=1, tiled=True)
    partner = kets[owners[:, 0][:, None], places_in]
    remote = complex_intersection(
        blocks[:, :, 0], blocks[:, :, 1], partner[:, :, 0], partner[:, :, 1], "ismw,isnw->imn"
    )
    summed_part = local_terms + remote.reshape(k_local, vector_count, 2, band_count, band_count)
    total = lax.psum(summed_part, "ga")
    row_count = band_count // slices
    return lax.dynamic_slice_in_dim(total, my_slice * row_count, row_count, 3)


def index_tables(block_map, my_slice, slab, capacity):
    shifts, blocks = block_map.shape
    exact = jnp.bfloat16
    base = (my_slice * slab).astype(jnp.float32)

    def lane_product(left, right, axis):
        return lax.dot_general(
            left.astype(exact), right.astype(exact), (((1,), (axis,)), ((), ())),
            preferred_element_type=jnp.float32,
        )

    def ones(mask):
        return jnp.where(mask, 1.0, 0.0)

    def place_rows(table):
        return lax.broadcasted_iota(jnp.int32, table.shape, 0)

    forward = block_map.astype(jnp.float32)
    counted = lax.broadcasted_iota(jnp.int32, (shifts, blocks), 1).astype(jnp.float32)
    block_rows = lax.broadcasted_iota(jnp.int32, (blocks, blocks), 0)
    inverse = jnp.zeros((shifts, blocks), jnp.float32)
    for r in range(shifts):
        row = lane_product(counted, ones(block_map[r : r + 1, :] == block_rows), 1)
        inverse = jnp.where(place_rows(row) == r, row, inverse)
    before = ones(
        lax.broadcasted_iota(jnp.int32, (slab, slab), 0)
        < lax.broadcasted_iota(jnp.int32, (slab, slab), 1)
    )
    padded = -(-capacity // 8) * 8
    slots = lax.broadcasted_iota(jnp.int32, (padded, slab), 0).astype(jnp.float32)
    indexes, sends = [], []
    for table in (forward, inverse):
        low, high = table[:, :slab], table[:, slab:]
        mine = jnp.where(my_slice == 0, low, high) - base
        other = jnp.where(my_slice == 0, high, low) - base
        inside = (mine >= 0) & (mine < slab)
        rank = jnp.minimum(lane_product(1.0 - ones(inside), before, 0), capacity - 1.0)
        at = jnp.where(inside, mine, slab + rank).astype(jnp.int32)
        indexes.append(jnp.clip(at, 0, slab + capacity - 1))
        wanted = ones((other >= 0) & (other < slab))
        rank = lane_product(wanted, before, 0)
        rank = jnp.where(wanted > 0, rank, -1.0)
        send = jnp.zeros((shifts, padded), jnp.float32)
        for r in range(shifts):
            row = lane_product(other, ones(rank[r : r + 1, :] == slots), 1)
            send = jnp.where(place_rows(row) == r, row, send)
        sends.append(jnp.clip(send.astype(jnp.int32), 0, slab - 1))
    return indexes, sends, padded


def pieces(slab):
    unit = slab // 20
    sizes = [unit, 3 * unit, 4 * unit, 4 * unit, 4 * unit, 2 * unit, unit, unit - 2, 2]
    starts = [sum(sizes[:n]) for n in range(len(sizes))]
    return list(zip(starts, sizes))


def meet_kernel(
    points, slab, capacity, near_hbm, shift_hbm, map_hbm, own_hbm, out_ref,
    near_ref, shift_ref, map_ref, own, first, second, third, extra, packs, landed,
    meta_out, meta_in, tables, sums, results, slots, meta, table_at,
    local_sems, meta_send, meta_recv, send_sems, first_sems, second_sems, third_sems, extra_sems,
    swap_send, swap_recv, result_send, result_recv, go, late_in,
):
    levels = 4
    row = points // levels
    me = lax.axis_index("ka")
    my_slice = lax.axis_index("ga")
    partner = 1 - my_slice
    z, column = me // row, me % row
    low = (column == 0) | (column == row - 1)
    role = jnp.where(low, z, levels - 1 - z)
    is_outer, is_hub, is_inner, is_far = role == 0, role == 1, role == 2, role == 3

    def member(r):
        return jnp.where(low, r, levels - 1 - r) * row + column

    outer, hub, inner, far = member(0), member(1), member(2), member(3)
    below, above = hub - row, hub + row
    twin = me + 1 - 2 * (column % 2)
    lower_half = z < 2
    bands, lanes = own.shape[2], own.shape[3]
    shifts = map_hbm.shape[0]
    parts = pieces(slab)
    count = len(parts)
    tail = parts[count - 2][0]

    barrier = pltpu.get_barrier_semaphore()
    mesh = pl.DeviceIdType.MESH
    is_last = z == levels - 1

    def greet(r, carry):
        peer = (me + r) % points

        @pl.when(~is_last | (peer // row == levels - 1))
        def _():
            for g in range(2):
                pl.semaphore_signal(barrier, inc=1, device_id={"ka": peer, "ga": g}, device_id_type=mesh)

        return carry

    lax.fori_loop(1, points, greet, 0)
    pl.semaphore_signal(barrier, inc=1, device_id={"ga": partner}, device_id_type=mesh)
    near_in = pltpu.make_async_copy(near_hbm, near_ref, local_sems.at[0])
    shift_in = pltpu.make_async_copy(shift_hbm, shift_ref, local_sems.at[1])
    map_in = pltpu.make_async_copy(map_hbm, map_ref, local_sems.at[2])
    keep = pltpu.make_async_copy(own_hbm, own.at[pl.ds(0, slab)], local_sems.at[3])
    for copy in (near_in, shift_in, map_in, keep):
        copy.start()
    pl.semaphore_wait(barrier, jnp.where(is_last, 2 * points - 1, 2 * (points - row) - 1))

    @pl.when(is_last)
    def _():
        def enter(peer, carry):
            for g in range(2):
                pl.semaphore_signal(late_in, inc=1, device_id={"ka": peer, "ga": g}, device_id_type=mesh)
            return carry

        lax.fori_loop(0, points - row, enter, 0)

    def remote(source, target, send, recv, peer):
        return pltpu.make_async_remote_copy(
            src_ref=source, dst_ref=target, send_sem=send, recv_sem=recv,
            device_id=peer, device_id_type=mesh,
        )

    def chunk(c):
        return pl.ds(*parts[c])

    def send_own(target, n, sems, peer, start=0, stop=count):
        for c in range(start, stop):
            remote(own_hbm.at[chunk(c)], target.at[chunk(c)], send_sems.at[n], sems.at[c], {"ka": peer}).start()

    def sent_own(n, size=slab):
        part = pl.ds(0, size)
        return remote(own_hbm.at[part], own.at[part], send_sems.at[n], first_sems.at[0], {"ka": twin})

    def arrived(buffer, sems, c):
        part = buffer.at[chunk(c)]
        remote(part, part, send_sems.at[0], sems.at[c], {"ka": twin}).wait_recv()

    def main_sends(pairs):
        @pl.when(me == below)
        def _():
            for n, start, stop in pairs:
                send_own(first, n, first_sems, hub, start, stop)

        @pl.when(me == above)
        def _():
            for n, start, stop in pairs:
                send_own(second, n, second_sems, hub, start, stop)

    main_sends(((0, 0, 1),))
    near_in.wait()
    shift_in.wait()

    def role_shift(step):
        target = (me + step) % points
        total = jnp.int32(0)
        for b in range(ROLES):
            total = total + jnp.where(near_ref[0, b] == target, shift_ref[0, b], 0)
        return total

    lane = lax.broadcasted_iota(jnp.int32, meta_out.shape, 1)
    facts = jnp.where(
        lane == 0, role_shift(1), jnp.where(lane == 1, role_shift(row), role_shift(points // 2))
    )
    meta_out[...] = facts
    meta_in[me] = facts

    @pl.when(~is_last)
    def _():
        pl.semaphore_wait(late_in, 2 * row)

    notices = (
        (~is_hub, hub),
        (is_inner, outer),
        (me == me, twin),
        ((z >= 2) & (column % 2 == 1) & (me != points - 1), me + 1),
        (me == 2 * row - 1, row),
    )
    heard = (
        (is_hub, 0, 3), (is_outer, 1, 1), (me == me, 2, 1),
        ((z >= 2) & (column % 2 == 0) & (me != 2 * row), 3, 1), (me == row, 4, 1),
    )

    def notice(n, peer):
        return remote(meta_out, meta_in.at[me], meta_send.at[n], meta_recv.at[n], {"ka": peer})

    for n, (sends, peer) in enumerate(notices):
        pl.when(sends)(notice(n, peer).start)

    main_sends(((0, 1, count - 2), (1, count - 2, count)))

    corner_low = me == row
    corner_high = me == 2 * row - 1
    extra_down = (me == 2) | (me == row + 2)
    extra_up = (me == 2 * row + 1) | (me == 2 * row + 3) | (me == 3 * row + 1)
    extra_source = extra_down | extra_up | corner_low | corner_high
    extra_site = (
        (me == row - 1) | (me == 1) | (me == row + 1)
        | (me == 2 * row + 2) | (me == 3 * row) | (me == 3 * row + 2)
    )
    extra_peer = jnp.where(corner_high, row, jnp.where(extra_up, me + 1, me - 1))

    @pl.when(extra_down | extra_up | corner_high)
    def _():
        send_own(extra, 3, extra_sems, extra_peer)

    @pl.when(corner_low)
    def _():
        send_own(extra, 3, extra_sems, extra_peer, 0, EARLY)

    @pl.when(is_outer | is_hub)
    def _():
        send_own(first, 2, first_sems, twin)

    map_in.wait()
    indexes, sends, padded = index_tables(map_ref[...], my_slice, slab, capacity)
    tables[...] = jnp.zeros_like(tables)
    for d in range(2):
        tables[pl.ds(d * shifts, shifts), pl.ds(0, slab)] = indexes[d]
        tables[pl.ds((2 + d) * shifts, shifts), pl.ds(0, padded)] = sends[d]
    tables_in = pltpu.make_async_copy(tables, table_at, local_sems.at[0])
    tables_in.start()

    def corner_copy(c):
        return remote(first.at[chunk(c)], extra.at[chunk(c)], send_sems.at[5], extra_sems.at[c], {"ka": 2 * row - 1})

    def relayed(source, c):
        return remote(source.at[chunk(c)], first.at[chunk(c)], send_sems.at[4], first_sems.at[c], {"ka": outer})

    def relay(c):
        arrived(second, second_sems, c)
        pl.when(low)(relayed(second, c).start)
        arrived(first, first_sems, c)
        pl.when(~low)(relayed(first, c).start)
        pl.when(corner_low)(corner_copy(c).start)

    @pl.when(is_hub)
    def _():
        relay(0)

    for hears, n, amount in heard:

        @pl.when(hears)
        def _():
            fact = meta_in.at[pl.ds(0, amount)]
            remote(fact, fact, meta_send.at[0], meta_recv.at[n], {"ka": twin}).wait_recv()

    meta_copy = pltpu.make_async_copy(meta_in, meta, local_sems.at[1])
    meta_copy.start()
    for n, (sends, peer) in enumerate(notices):
        pl.when(sends)(notice(n, peer).wait_send)
    meta_copy.wait()
    tables_in.wait()
    keep.wait()

    def shift_of(point, kind):
        return meta[point, 0, kind]

    NEXT, ROW, HALF = 0, 1, 2
    OWN_EXTRA, BELOW_SLOT, ABOVE_SLOT, CORNER_SLOT = 4, 5, 6, 7
    groups = (0, 0, 0, 0, 1, 2, 2, 3)

    def swap(n, many=1):
        part = pl.ds(n * capacity, many * capacity)
        group = groups[n]
        return remote(packs.at[part], landed.at[part], swap_send.at[group], swap_recv.at[group], {"ga": partner})

    def place_landed(n, target, place):
        def move(r, carry):
            target[slab + place * capacity + r] = landed[n * capacity + r]
            return carry

        lax.fori_loop(0, capacity, move, 0, unroll=4)

    def take(n, target, place):
        swap(n).wait_recv()
        place_landed(n, target, place)

    def offer(n, source, inverse, shift):
        line = (2 + inverse) * shifts + shift

        def gather(r, carry):
            packs[n * capacity + r] = source[table_at[line, r]]
            return carry

        lax.fori_loop(0, capacity, gather, 0, unroll=4)
        swap(n).start()

    def pick(ref, at):
        return ref[at].reshape(2 * bands, lanes)

    def accumulate(e, part, still, moving, place, inverse, shift, turn=False):
        start, size = part
        line = inverse * shifts + shift

        def at(n):
            value = table_at[line, n]
            return value + jnp.where(value >= slab, place * capacity, 0)

        def products(begin, many, total):
            for u in range(0, many, 2):
                n = begin + u
                left = jnp.concatenate([pick(still, n), pick(still, n + 1)], axis=1)
                right = jnp.concatenate([pick(moving, at(n)), pick(moving, at(n + 1))], axis=1)
                total = total + lax.dot_general(
                    right if turn else left,
                    left if turn else right,
                    (((1,), (1,)), ((), ())),
                    preferred_element_type=jnp.float32,
                )
            return total

        steps = [s for s in (12, 6, 4, 2) if size % s == 0][0]
        if steps == size:
            sums[e] = products(start, size, sums[e])
        else:
            sums[e] = lax.fori_loop(
                0, size // steps, lambda i, total: products(start + i * steps, steps, total), sums[e]
            )

    def result_copies(e, kind, bra, base):
        copies = []
        half = bands // 2
        for g in range(2):
            source = results.at[e, pl.ds(g * half, half)]
            target = slots.at[kind, my_slice]
            at_home = (bra == me) & (my_slice == g)
            near = pltpu.make_async_copy(source, target, result_recv.at[0])
            send = 0 if base is None else base + g
            away = remote(source, target, result_send.at[send], result_recv.at[0], {"ka": bra, "ga": g})
            copies.append((at_home, near, away))
        return copies

    def settle(e, inverse=None):
        total = sums[e]
        if inverse is not None:
            total = jnp.where(inverse == 1, total.T, total)
        upper, under = total[:bands], pltpu.roll(total[bands:], bands, 1)
        left = lax.broadcasted_iota(jnp.int32, upper.shape, 1) < bands
        results[e] = upper + jnp.where(left, under, -under)

    def dispatch(e, kind, bra, base):
        for at_home, near, away in result_copies(e, kind, bra, base):
            pl.when(at_home)(near.start)
            pl.when(~at_home)(away.start)

    def deliver(e, kind, bra, base, inverse=None):
        settle(e, inverse)
        dispatch(e, kind, bra, base)

    def delivered(e, kind, bra, base):
        for at_home, _, away in result_copies(e, kind, bra, base):
            pl.when(~at_home)(away.wait_send)

    sums[...] = jnp.zeros_like(sums)
    extra_inverse = jnp.where(lower_half, 1, 0)
    extra_bra = jnp.where(lower_half, me, me - 1)
    EXTRA, EXTRA_BASE = 6, 4

    hub_edges = (
        (first, own, 0, 0, below, ROW),
        (second, own, 1, 1, hub, ROW),
        (third, own, 2, 1, hub, HALF),
        (third, own, 3, 0, far, HALF),
        (third, first, 0, 0, far, ROW),
        (third, second, 0, 1, above, ROW),
    )

    @pl.when(extra_site)
    def _():
        offer(OWN_EXTRA, own, extra_inverse, shift_of(extra_bra, NEXT))

    def extra_edge():
        take(OWN_EXTRA, own, OWN_EXTRA)
        shift = shift_of(extra_bra, NEXT)
        for c in range(count):
            arrived(extra, extra_sems, c)
            accumulate(EXTRA, parts[c], extra, own, OWN_EXTRA, extra_inverse, shift)
        deliver(EXTRA, NEXT, extra_bra, EXTRA_BASE, extra_inverse)

    @pl.when(is_hub)
    def _():
        for e in range(4):
            _, _, _, inverse, bra, kind = hub_edges[e]
            offer(e, own, inverse, shift_of(bra, kind))

        for c in range(1, count):
            relay(c)

        @pl.when(corner_low)
        def _():
            send_own(extra, 3, extra_sems, extra_peer, EARLY, count)

        for n, e in ((BELOW_SLOT, 4), (ABOVE_SLOT, 5)):
            _, source, _, inverse, bra, kind = hub_edges[e]
            offer(n, source, inverse, shift_of(bra, kind))

        @pl.when(corner_low)
        def _():
            offer(CORNER_SLOT, second, 0, shift_of(2 * row - 1, NEXT))

        swap(0, 4).wait_recv()
        for e in range(4):
            place_landed(e, own, e)
        for e in range(2):
            still, moving, place, inverse, bra, kind = hub_edges[e]
            accumulate(e, (0, slab), still, moving, place, inverse, shift_of(bra, kind), inverse == 1)
            deliver(e, kind, bra, None)

        @pl.when(extra_site)
        def _():
            extra_edge()

        @pl.when(corner_high)
        def _():
            for c in range(count):
                arrived(extra, extra_sems, c)
            offer(CORNER_SLOT, extra, 0, shift_of(4 * row - 1, NEXT))

        swap(BELOW_SLOT, 2).wait_recv()
        place_landed(BELOW_SLOT, first, 0)
        place_landed(ABOVE_SLOT, second, 0)

        @pl.when(corner_low)
        def _():
            take(CORNER_SLOT, second, 1)

        @pl.when(corner_high)
        def _():
            take(CORNER_SLOT, extra, 0)

        for c in range(count):
            arrived(third, third_sems, c)

            @pl.when(corner_low)
            def _():
                arrived(extra, extra_sems, c)
                accumulate(EXTRA, parts[c], extra, second, 1, 0, shift_of(2 * row - 1, NEXT))
                if c == count - 1:
                    deliver(EXTRA, NEXT, 2 * row - 1, EXTRA_BASE)

            @pl.when(corner_high)
            def _():
                accumulate(EXTRA, parts[c], third, extra, 0, 0, shift_of(4 * row - 1, NEXT))
                if c == count - 1:
                    deliver(EXTRA, NEXT, 4 * row - 1, EXTRA_BASE)

            for e in (3, 4, 5, 2):
                still, moving, place, inverse, bra, kind = hub_edges[e]
                accumulate(e, parts[c], still, moving, place, inverse, shift_of(bra, kind), inverse == 1)

        for e in (3, 4, 5, 2):
            settle(e)
        for e in (3, 4, 5, 2):
            dispatch(e, hub_edges[e][5], hub_edges[e][4], None)

        sent = results.at[pl.ds(0, 5)]
        remote(sent, sent, result_send.at[0], result_recv.at[0], {"ka": twin}).wait_send()

        @pl.when(corner_low)
        def _():
            delivered(EXTRA, NEXT, 2 * row - 1, EXTRA_BASE)
            swap(CORNER_SLOT).wait_send()
            sent_own(5).wait_send()

        @pl.when(corner_high)
        def _():
            delivered(EXTRA, NEXT, 4 * row - 1, EXTRA_BASE)
            swap(CORNER_SLOT).wait_send()

        swap(0, 4).wait_send()
        swap(BELOW_SLOT, 2).wait_send()
        sent_own(4).wait_send()

    outer_edges = ((0, 1, outer), (1, 0, inner))

    @pl.when(is_outer)
    def _():
        for e, inverse, bra in outer_edges:
            offer(e, own, inverse, shift_of(bra, HALF))
        sent_own(0, tail).wait_send()
        pl.semaphore_signal(go, inc=1, device_id={"ka": twin}, device_id_type=mesh)
        swap(0, 2).wait_recv()
        for e in range(2):
            place_landed(e, own, e)
        pl.when(extra_site & ~lower_half)(extra_edge)
        for c in range(count):
            arrived(first, first_sems, c)
            for e, inverse, bra in outer_edges:
                accumulate(e, parts[c], first, own, e, inverse, shift_of(bra, HALF), inverse == 1)
        for e, inverse, bra in outer_edges:
            deliver(e, HALF, bra, 2 * e)
        pl.when(extra_site & lower_half)(extra_edge)
        for e, inverse, bra in outer_edges:
            delivered(e, HALF, bra, 2 * e)
        swap(0, 2).wait_send()

    twin_inverse = jnp.where(column % 2 == 1, 0, 1)
    twin_bra = me - column % 2

    @pl.when(is_inner | is_far)
    def _():
        shift = shift_of(twin_bra, NEXT)
        offer(0, own, twin_inverse, shift)
        take(0, own, 0)
        for c in range(count):
            arrived(first, first_sems, c)
        accumulate(0, (0, slab), first, own, 0, twin_inverse, shift)
        deliver(0, NEXT, twin_bra, 0, twin_inverse)

        @pl.when(is_inner)
        def _():
            sent_own(0, tail).wait_send()
            pl.semaphore_signal(go, inc=1, device_id={"ka": far}, device_id_type=mesh)

        @pl.when(is_far)
        def _():
            pl.semaphore_wait(go, 2)
            send_own(third, 0, third_sems, hub)

        pl.when(extra_site)(extra_edge)
        delivered(0, NEXT, twin_bra, 0)
        swap(0).wait_send()
        pl.when(is_far)(sent_own(0).wait_send)

    @pl.when(extra_site)
    def _():
        delivered(EXTRA, NEXT, extra_bra, EXTRA_BASE)
        swap(OWN_EXTRA).wait_send()

    @pl.when(is_outer | is_inner)
    def _():
        sent_own(1, slab - tail).wait_send()

    @pl.when(is_outer | is_hub)
    def _():
        sent_own(2).wait_send()

    @pl.when(extra_source)
    def _():
        sent_own(3).wait_send()

    pltpu.make_async_copy(slots, slots, result_recv.at[0]).wait()
    found = [slots[kind, 0] + slots[kind, 1] for kind in range(ROLES)]
    for b in range(ROLES):
        target = near_ref[0, b]
        chosen = jnp.where(target == (me + row) % points, found[ROW], found[HALF])
        chosen = jnp.where(target == (me + 1) % points, found[NEXT], chosen)
        out_ref[b, 0] = chosen[:, :bands]
        out_ref[b, 1] = chosen[:, bands:]


def meet(neighbour, shift_id, block_map, own, points, capacity):
    slab, bands, lanes = own.shape[0], own.shape[2], own.shape[3]
    block = own.shape[1:]
    shifts = block_map.shape[0]
    half = bands // 2
    dma = pltpu.SemaphoreType.DMA
    flows = len(pieces(slab))

    def blocks(count):
        return pltpu.VMEM((count,) + block, own.dtype)

    return pl.pallas_call(
        functools.partial(meet_kernel, points, slab, capacity),
        out_shape=pltpu.VMEM((ROLES, 2, half, bands), jnp.float32),
        in_specs=[pl.BlockSpec(memory_space=pl.ANY)] * 4,
        out_specs=pl.BlockSpec(memory_space=pltpu.VMEM),
        scratch_shapes=[
            pltpu.SMEM(neighbour.shape, jnp.int32),
            pltpu.SMEM(shift_id.shape, jnp.int32),
            pltpu.VMEM(block_map.shape, jnp.int32),
            blocks(slab + 5 * capacity),
            blocks(slab + capacity),
            blocks(slab + 2 * capacity),
            blocks(slab),
            blocks(slab + capacity),
            blocks(8 * capacity),
            blocks(8 * capacity),
            pltpu.VMEM((1, lanes), jnp.int32),
            pltpu.VMEM((points, 1, lanes), jnp.int32),
            pltpu.VMEM((4 * shifts, lanes), jnp.int32),
            pltpu.VMEM((7, 2 * bands, 2 * bands), jnp.float32),
            pltpu.VMEM((7, bands, 2 * bands), jnp.float32),
            pltpu.VMEM((ROLES, 2, half, 2 * bands), jnp.float32),
            pltpu.SMEM((points, 1, lanes), jnp.int32),
            pltpu.SMEM((4 * shifts, lanes), jnp.int32),
            dma((4,)), dma((5,)), dma((5,)), dma((6,)),
            dma((flows,)), dma((flows,)), dma((flows,)), dma((flows,)),
            dma((4,)), dma((4,)), dma((6,)), dma((1,)),
            pltpu.SemaphoreType.REGULAR,
            pltpu.SemaphoreType.REGULAR,
        ],
        compiler_params=pltpu.CompilerParams(
            collective_id=0, has_side_effects=True, vmem_limit_bytes=60 * 2**20
        ),
        name="meet",
    )(neighbour, shift_id, block_map, own)


def on_four_levels(coeffs, neighbour, shift_id, block_map):
    own = coeffs[0]
    points = lax.axis_size("ka")
    capacity = 2 * max(1, own.shape[0] // 12)
    return meet(neighbour, shift_id, block_map, own, points, capacity)[None]


def solution(mesh):
    in_specs = (P("ka", "ga", None, None, None), P("ka", None), P("ka", None), P())
    out_specs = P("ka", None, None, "ga", None)
    levels = mesh.shape["ka"] // 4
    square = mesh.shape["ga"] == 2 and mesh.shape["ka"] == 4 * levels and levels == 4

    def run(coeffs, neighbour, shift_id, block_map):
        one_each = coeffs.shape[0] == mesh.shape["ka"] and neighbour.shape[1] == ROLES
        per_slice = coeffs.shape[1] // mesh.shape["ga"]
        lanes = coeffs.shape[4]
        fits = per_slice % 40 == 0 and 80 <= per_slice <= lanes and 2 * coeffs.shape[3] == lanes
        body = on_four_levels if square and one_each and fits else on_device
        return jax.shard_map(
            body, mesh=mesh, in_specs=in_specs, out_specs=out_specs, check_vma=False
        )(coeffs, neighbour, shift_id, block_map)

    return run
```

```python
import functools

import jax
import jax.numpy as jnp
from jax import lax
from jax.sharding import PartitionSpec as P
from jax.experimental import pallas as pl
from jax.experimental.pallas import tpu as pltpu

EARLY = 2
MIDDLE = 4
ROLES = 3


def shifted(block, axis, distance):
    devices = range(lax.axis_size(axis))
    route = [((i - distance) % len(devices), i) for i in devices]
    return lax.ppermute(block, axis, route)


def complex_intersection(bra_real, bra_imag, ket_real, ket_imag, form):
    real_part = jnp.einsum(form, bra_real, ket_real, preferred_element_type=jnp.float32)
    real_part = real_part + jnp.einsum(form, bra_imag, ket_imag, preferred_element_type=jnp.float32)
    imag_part = jnp.einsum(form, bra_real, ket_imag, preferred_element_type=jnp.float32)
    imag_part = imag_part - jnp.einsum(form, bra_imag, ket_real, preferred_element_type=jnp.float32)
    return jnp.stack([real_part, imag_part], axis=-3)


def slot_plan(
    home_slice, target_slice, sent_local, place_local, my_slice, slices, capacity, slab_blocks
):
    targets = jnp.arange(slices, dtype=jnp.int32)
    chosen = (home_slice == my_slice)[:, None, :] & (
        target_slice[:, None, :] == targets[None, :, None]
    )
    chosen = chosen & (targets != my_slice)[None, :, None]
    counted = jnp.cumsum(chosen.astype(jnp.int32), axis=2) - 1
    places = jnp.arange(capacity, dtype=jnp.int32)
    matched = (
        chosen[:, :, None, :] & (counted[:, :, None, :] == places[None, None, :, None])
    ).astype(jnp.int32)
    filled = jnp.sum(matched, axis=3)
    sent_block = jnp.sum(matched * sent_local[:, None, None, :], axis=3)
    where_to = jnp.sum(matched * place_local[:, None, None, :], axis=3) + (1 - filled) * slab_blocks
    pair_count = home_slice.shape[0]
    return (
        sent_block.reshape(pair_count, slices * capacity),
        where_to.reshape(pair_count, slices * capacity),
    )


def on_device(coeffs, neighbour, shift_id, block_map):
    k_local = coeffs.shape[0]
    slab_blocks = coeffs.shape[1]
    band_count = coeffs.shape[3]
    lane_width = coeffs.shape[4]
    vector_count = neighbour.shape[1]
    cycle_size = lax.axis_size("ka")
    slices = lax.axis_size("ga")
    my_cycle = lax.axis_index("ka")
    my_slice = lax.axis_index("ga")
    capacity = 2 * max(1, slab_blocks // 12)
    all_blocks = slab_blocks * slices
    pair_count = k_local * vector_count
    k_total = k_local * cycle_size
    row_points = min(16, k_total // 4)
    row_devices = row_points // k_local
    pad_spec = ((0, 0), (0, 1), (0, 0), (0, 0), (0, 0))
    row_point = shifted(coeffs, "ka", -1)
    row_source = jnp.mod(my_cycle + 1, cycle_size)
    plane_kets = shifted(coeffs, "ka", -row_devices)
    plane_source = jnp.mod(my_cycle + row_devices, cycle_size)
    opposite = shifted(coeffs, "ka", cycle_size // 2)
    targets_flat = neighbour.reshape(-1)
    shifts_flat = shift_id.reshape(-1)
    target_device = targets_flat // k_local
    target_lane = targets_flat - target_device * k_local
    ket_index = jnp.where(
        target_device == my_cycle,
        target_lane,
        jnp.where(
            target_device == row_source,
            k_local,
            jnp.where(
                target_device == plane_source,
                k_local + 1 + target_lane,
                2 * k_local + 1 + target_lane,
            ),
        ),
    )
    bra_index = jnp.arange(pair_count, dtype=jnp.int32) // vector_count
    picks = (
        shifts_flat[:, None] == jnp.arange(block_map.shape[0], dtype=jnp.int32)[None, :]
    ).astype(jnp.int32)
    relabel = jnp.sum(picks[:, :, None] * block_map[None, :, :], axis=1)
    dest_global = jnp.broadcast_to(jnp.arange(all_blocks, dtype=jnp.int32)[None, :], relabel.shape)
    source_slice = relabel // slab_blocks
    dest_slice = dest_global // slab_blocks
    source_local = relabel - source_slice * slab_blocks
    dest_local = dest_global - dest_slice * slab_blocks
    kets = jnp.pad(jnp.concatenate([coeffs, row_point, plane_kets, opposite], axis=0), pad_spec)
    own_source = lax.dynamic_slice_in_dim(relabel, my_slice * slab_blocks, slab_blocks, 1)
    self_place = jnp.where(
        own_source // slab_blocks == my_slice, own_source - my_slice * slab_blocks, slab_blocks
    )
    ket_self = kets[ket_index[:, None], self_place]
    ket_self = ket_self.reshape(k_local, vector_count, slab_blocks, 2, band_count, lane_width)
    local_terms = complex_intersection(
        coeffs[:, :, 0],
        coeffs[:, :, 1],
        ket_self[:, :, :, 0],
        ket_self[:, :, :, 1],
        "ksmw,kbsnw->kbmn",
    )
    sent_block, where_to = slot_plan(
        dest_slice, source_slice, dest_local, source_local, my_slice, slices, capacity, slab_blocks
    )
    payload = coeffs[bra_index[:, None], sent_block]
    owner = jnp.broadcast_to(ket_index[:, None], (pair_count, slices))
    blocks = lax.all_to_all(payload, "ga", split_axis=1, concat_axis=1, tiled=True)
    places_in = lax.all_to_all(where_to, "ga", split_axis=1, concat_axis=1, tiled=True)
    owners = lax.all_to_all(owner, "ga", split_axis=1, concat_axis=1, tiled=True)
    partner = kets[owners[:, 0][:, None], places_in]
    remote = complex_intersection(
        blocks[:, :, 0], blocks[:, :, 1], partner[:, :, 0], partner[:, :, 1], "ismw,isnw->imn"
    )
    summed_part = local_terms + remote.reshape(k_local, vector_count, 2, band_count, band_count)
    total = lax.psum(summed_part, "ga")
    row_count = band_count // slices
    return lax.dynamic_slice_in_dim(total, my_slice * row_count, row_count, 3)


def index_tables(block_map, my_slice, slab, capacity):
    shifts, blocks = block_map.shape
    exact = jnp.bfloat16
    base = (my_slice * slab).astype(jnp.float32)

    def lane_product(left, right, axis):
        return lax.dot_general(
            left.astype(exact), right.astype(exact), (((1,), (axis,)), ((), ())),
            preferred_element_type=jnp.float32,
        )

    def ones(mask):
        return jnp.where(mask, 1.0, 0.0)

    def place_rows(table):
        return lax.broadcasted_iota(jnp.int32, table.shape, 0)

    forward = block_map.astype(jnp.float32)
    counted = lax.broadcasted_iota(jnp.int32, (shifts, blocks), 1).astype(jnp.float32)
    block_rows = lax.broadcasted_iota(jnp.int32, (blocks, blocks), 0)
    inverse = jnp.zeros((shifts, blocks), jnp.float32)
    for r in range(shifts):
        row = lane_product(counted, ones(block_map[r : r + 1, :] == block_rows), 1)
        inverse = jnp.where(place_rows(row) == r, row, inverse)
    before = ones(
        lax.broadcasted_iota(jnp.int32, (slab, slab), 0)
        < lax.broadcasted_iota(jnp.int32, (slab, slab), 1)
    )
    padded = -(-capacity // 8) * 8
    slots = lax.broadcasted_iota(jnp.int32, (padded, slab), 0).astype(jnp.float32)
    indexes, sends = [], []
    for table in (forward, inverse):
        low, high = table[:, :slab], table[:, slab:]
        mine = jnp.where(my_slice == 0, low, high) - base
        other = jnp.where(my_slice == 0, high, low) - base
        inside = (mine >= 0) & (mine < slab)
        rank = jnp.minimum(lane_product(1.0 - ones(inside), before, 0), capacity - 1.0)
        at = jnp.where(inside, mine, slab + rank).astype(jnp.int32)
        indexes.append(jnp.clip(at, 0, slab + capacity - 1))
        wanted = ones((other >= 0) & (other < slab))
        rank = lane_product(wanted, before, 0)
        rank = jnp.where(wanted > 0, rank, -1.0)
        send = jnp.zeros((shifts, padded), jnp.float32)
        for r in range(shifts):
            row = lane_product(other, ones(rank[r : r + 1, :] == slots), 1)
            send = jnp.where(place_rows(row) == r, row, send)
        sends.append(jnp.clip(send.astype(jnp.int32), 0, slab - 1))
    return indexes, sends, padded


def pieces(slab):
    unit = slab // 20
    sizes = [unit, 3 * unit, 4 * unit, 4 * unit, 4 * unit, 2 * unit, unit, unit - 2, 2]
    starts = [sum(sizes[:n]) for n in range(len(sizes))]
    return list(zip(starts, sizes))


def meet_kernel(
    points, slab, capacity, near_hbm, shift_hbm, map_hbm, own_hbm, out_ref,
    near_ref, shift_ref, map_ref, own, first, second, third, extra, packs, landed,
    meta_out, meta_in, tables, sums, results, slots, meta, table_at,
    local_sems, meta_send, meta_recv, send_sems, first_sems, second_sems, third_sems, extra_sems,
    swap_send, swap_recv, result_send, result_recv, go, late_in,
):
    levels = 4
    row = points // levels
    me = lax.axis_index("ka")
    my_slice = lax.axis_index("ga")
    partner = 1 - my_slice
    z, column = me // row, me % row
    low = (column == 0) | (column == row - 1)
    role = jnp.where(low, z, levels - 1 - z)
    is_outer, is_hub, is_inner, is_far = role == 0, role == 1, role == 2, role == 3

    def member(r):
        return jnp.where(low, r, levels - 1 - r) * row + column

    outer, hub, inner, far = member(0), member(1), member(2), member(3)
    below, above = hub - row, hub + row
    twin = me + 1 - 2 * (column % 2)
    lower_half = z < 2
    bands, lanes = own.shape[2], own.shape[3]
    shifts = map_hbm.shape[0]
    parts = pieces(slab)
    count = len(parts)
    tail = parts[count - 2][0]

    barrier = pltpu.get_barrier_semaphore()
    mesh = pl.DeviceIdType.MESH
    corner_low = me == row
    corner_high = me == 2 * row - 1
    high_source = me == 3 * row - 1
    high_site = me == 3 * row

    def signal(semaphore, peer):
        pl.semaphore_signal(semaphore, inc=1, device_id=peer, device_id_type=mesh)

    signal(barrier, {"ga": partner})
    signal(barrier, {"ka": twin})
    greetings = (
        (~is_hub, hub), (is_hub, outer), (is_hub, inner), (is_hub | is_inner, far),
        (column == 1, me + 1), (column == 2, me - 1), (me == row - 1, row), (corner_low, row - 1),
        (corner_low, 2 * row - 1), (corner_high, row), (high_source, 3 * row),
    )
    for greets, peer in greetings:

        @pl.when(greets)
        def _():
            signal(barrier, {"ka": peer})

    expected = (
        (is_hub, 3), (~is_hub, 1), (is_far, 1), ((column == 1) | (column == 2), 1),
        (me == row - 1, 1), (corner_low, 2), (corner_high, 1), (high_site, 1),
    )
    greeted = jnp.int32(2)
    for hears, amount in expected:
        greeted = greeted + jnp.where(hears, amount, 0)
    near_in = pltpu.make_async_copy(near_hbm, near_ref, local_sems.at[0])
    shift_in = pltpu.make_async_copy(shift_hbm, shift_ref, local_sems.at[1])
    map_in = pltpu.make_async_copy(map_hbm, map_ref, local_sems.at[2])
    keep = pltpu.make_async_copy(own_hbm, own.at[pl.ds(0, slab)], local_sems.at[3])
    for copy in (near_in, shift_in, map_in, keep):
        copy.start()
    pl.semaphore_wait(barrier, greeted)

    @pl.when(is_far)
    def _():
        signal(late_in, {"ka": inner})

    @pl.when(high_site)
    def _():
        signal(late_in, {"ka": me - 1})

    def remote(source, target, send, recv, peer):
        return pltpu.make_async_remote_copy(
            src_ref=source, dst_ref=target, send_sem=send, recv_sem=recv,
            device_id=peer, device_id_type=mesh,
        )

    def chunk(c):
        return pl.ds(*parts[c])

    def send_own(target, n, sems, peer, start=0, stop=count):
        for c in range(start, stop):
            remote(own_hbm.at[chunk(c)], target.at[chunk(c)], send_sems.at[n], sems.at[c], {"ka": peer}).start()

    def sent_own(n, size=slab):
        part = pl.ds(0, size)
        return remote(own_hbm.at[part], own.at[part], send_sems.at[n], first_sems.at[0], {"ka": twin})

    def arrived(buffer, sems, c):
        part = buffer.at[chunk(c)]
        remote(part, part, send_sems.at[0], sems.at[c], {"ka": twin}).wait_recv()

    def main_sends(pairs):
        @pl.when(me == below)
        def _():
            for n, start, stop in pairs:
                send_own(first, n, first_sems, hub, start, stop)

        @pl.when(me == above)
        def _():
            for n, start, stop in pairs:
                send_own(second, n, second_sems, hub, start, stop)

    main_sends(((0, 0, 1),))
    near_in.wait()
    shift_in.wait()

    def role_shift(step):
        target = (me + step) % points
        total = jnp.int32(0)
        for b in range(ROLES):
            total = total + jnp.where(near_ref[0, b] == target, shift_ref[0, b], 0)
        return total

    lane = lax.broadcasted_iota(jnp.int32, meta_out.shape, 1)
    facts = jnp.where(
        lane == 0, role_shift(1), jnp.where(lane == 1, role_shift(row), role_shift(points // 2))
    )
    meta_out[...] = facts
    meta_in[me] = facts

    steps_up = (z >= 2) & (column % 2 == 1) & (me != points - 1)
    notices = (
        (~is_hub, hub),
        (is_hub, outer),
        (me == me, twin),
        (steps_up, me + 1),
        (corner_high, row),
    )
    heard = (
        (is_hub, 0, 3), (is_outer, 1, 1), (me == me, 2, 1),
        ((z >= 2) & (column % 2 == 0) & (me != 2 * row), 3, 1), (corner_low, 4, 1),
    )

    def notice(n, peer):
        source = meta_out if n != 1 else meta_in.at[inner]
        target = meta_in.at[me] if n != 1 else meta_in.at[inner]
        return remote(source, target, meta_send.at[n], meta_recv.at[n], {"ka": peer})

    for n in (0, 2, 4):
        pl.when(notices[n][0])(notice(n, notices[n][1]).start)

    main_sends(((0, 1, count - 2), (1, count - 2, count)))

    @pl.when(high_source)
    def _():
        pl.semaphore_wait(late_in, 2)

    pl.when(steps_up)(notice(3, me + 1).start)
    extra_down = (me == 2) | (me == row + 2)
    extra_up = (me == 2 * row + 1) | (me == 2 * row + 3) | (me == 3 * row + 1)
    extra_source = extra_down | extra_up | corner_low | corner_high
    extra_site = (
        (me == row - 1) | (me == 1) | (me == row + 1)
        | (me == 2 * row + 2) | (me == 3 * row) | (me == 3 * row + 2)
    )
    extra_peer = jnp.where(corner_high, row, jnp.where(extra_up, me + 1, me - 1))

    @pl.when(extra_down | extra_up | corner_high)
    def _():
        send_own(extra, 3, extra_sems, extra_peer)

    @pl.when(corner_low)
    def _():
        send_own(extra, 3, extra_sems, extra_peer, 0, EARLY)

    @pl.when(is_outer | is_hub)
    def _():
        send_own(first, 2, first_sems, twin)

    map_in.wait()
    indexes, sends, padded = index_tables(map_ref[...], my_slice, slab, capacity)
    tables[...] = jnp.zeros_like(tables)
    for d in range(2):
        tables[pl.ds(d * shifts, shifts), pl.ds(0, slab)] = indexes[d]
        tables[pl.ds((2 + d) * shifts, shifts), pl.ds(0, padded)] = sends[d]
    tables_in = pltpu.make_async_copy(tables, table_at, local_sems.at[0])
    tables_in.start()

    def corner_copy(c):
        return remote(first.at[chunk(c)], extra.at[chunk(c)], send_sems.at[5], extra_sems.at[c], {"ka": 2 * row - 1})

    def relayed(source, c):
        return remote(source.at[chunk(c)], first.at[chunk(c)], send_sems.at[4], first_sems.at[c], {"ka": outer})

    def relay(c):
        arrived(second, second_sems, c)
        pl.when(low)(relayed(second, c).start)
        arrived(first, first_sems, c)
        pl.when(~low)(relayed(first, c).start)
        pl.when(corner_low)(corner_copy(c).start)

    @pl.when(is_hub)
    def _():
        relay(0)

    for hears, n, amount in heard:

        @pl.when(hears)
        def _():
            fact = meta_in.at[pl.ds(0, amount)]
            remote(fact, fact, meta_send.at[0], meta_recv.at[n], {"ka": twin}).wait_recv()
            if n == 0:
                notice(1, outer).start()

    meta_copy = pltpu.make_async_copy(meta_in, meta, local_sems.at[1])
    meta_copy.start()
    meta_copy.wait()
    tables_in.wait()
    keep.wait()

    def shift_of(point, kind):
        return meta[point, 0, kind]

    NEXT, ROW, HALF = 0, 1, 2
    OWN_EXTRA, BELOW_SLOT, ABOVE_SLOT, CORNER_SLOT = 4, 5, 6, 7
    groups = (0, 0, 0, 0, 1, 2, 2, 3)

    def swap(n, many=1):
        part = pl.ds(n * capacity, many * capacity)
        group = groups[n]
        return remote(packs.at[part], landed.at[part], swap_send.at[group], swap_recv.at[group], {"ga": partner})

    def place_landed(n, target, place):
        def move(r, carry):
            target[slab + place * capacity + r] = landed[n * capacity + r]
            return carry

        lax.fori_loop(0, capacity, move, 0, unroll=4)

    def take(n, target, place):
        swap(n).wait_recv()
        place_landed(n, target, place)

    def offer(n, source, inverse, shift):
        line = (2 + inverse) * shifts + shift

        def gather(r, carry):
            packs[n * capacity + r] = source[table_at[line, r]]
            return carry

        lax.fori_loop(0, capacity, gather, 0, unroll=4)
        swap(n).start()

    def pick(ref, at):
        return ref[at].reshape(2 * bands, lanes)

    def accumulate(e, part, still, moving, place, inverse, shift, turn=False):
        start, size = part
        line = inverse * shifts + shift

        def at(n):
            value = table_at[line, n]
            return value + jnp.where(value >= slab, place * capacity, 0)

        def products(begin, many, total):
            for u in range(0, many, 2):
                n = begin + u
                left = jnp.concatenate([pick(still, n), pick(still, n + 1)], axis=1)
                right = jnp.concatenate([pick(moving, at(n)), pick(moving, at(n + 1))], axis=1)
                total = total + lax.dot_general(
                    right if turn else left,
                    left if turn else right,
                    (((1,), (1,)), ((), ())),
                    preferred_element_type=jnp.float32,
                )
            return total

        steps = [s for s in (12, 6, 4, 2) if size % s == 0][0]
        if steps == size:
            sums[e] = products(start, size, sums[e])
        else:
            sums[e] = lax.fori_loop(
                0, size // steps, lambda i, total: products(start + i * steps, steps, total), sums[e]
            )

    def result_copies(e, kind, bra, base):
        copies = []
        half = bands // 2
        for n, g in enumerate((partner, my_slice)):
            source = results.at[e, pl.ds(g * half, half)]
            target = slots.at[kind, my_slice]
            at_home = bra == me
            near = pltpu.make_async_copy(source, target, result_recv.at[0])
            send = 0 if base is None else base + n
            away = remote(source, target, result_send.at[send], result_recv.at[0], {"ka": bra, "ga": g})
            copies.append((at_home, near, away))
        return copies

    def settle(e, inverse=None):
        total = sums[e]
        if inverse is not None:
            total = jnp.where(inverse == 1, total.T, total)
        upper, under = total[:bands], pltpu.roll(total[bands:], bands, 1)
        left = lax.broadcasted_iota(jnp.int32, upper.shape, 1) < bands
        results[e] = upper + jnp.where(left, under, -under)

    def dispatch(edges, base):
        for n in range(2):
            for e, kind, bra in edges:
                at_home, near, away = result_copies(e, kind, bra, base)[n]
                if n == 0:
                    away.start()
                else:
                    pl.when(at_home)(near.start)
                    pl.when(~at_home)(away.start)

    def deliver(e, kind, bra, base, inverse=None):
        settle(e, inverse)
        dispatch(((e, kind, bra),), base)

    def delivered(e, kind, bra, base):
        first_copy, second_copy = result_copies(e, kind, bra, base)
        first_copy[2].wait_send()
        pl.when(~second_copy[0])(second_copy[2].wait_send)

    sums[...] = jnp.zeros_like(sums)
    extra_inverse = jnp.where(lower_half, 1, 0)
    extra_bra = jnp.where(lower_half, me, me - 1)
    EXTRA, EXTRA_BASE = 6, 4

    hub_edges = (
        (first, own, 0, 0, below, ROW),
        (second, own, 1, 1, hub, ROW),
        (third, own, 2, 1, hub, HALF),
        (third, own, 3, 0, far, HALF),
        (third, first, 0, 0, far, ROW),
        (third, second, 0, 1, above, ROW),
    )

    @pl.when(extra_site)
    def _():
        offer(OWN_EXTRA, own, extra_inverse, shift_of(extra_bra, NEXT))

    def extra_edge():
        take(OWN_EXTRA, own, OWN_EXTRA)
        shift = shift_of(extra_bra, NEXT)
        for c in range(count):
            arrived(extra, extra_sems, c)
            accumulate(EXTRA, parts[c], extra, own, OWN_EXTRA, extra_inverse, shift)
        deliver(EXTRA, NEXT, extra_bra, EXTRA_BASE, extra_inverse)

    @pl.when(is_hub)
    def _():
        for e in range(4):
            _, _, _, inverse, bra, kind = hub_edges[e]
            offer(e, own, inverse, shift_of(bra, kind))

        for c in range(1, count):
            relay(c)

        @pl.when(corner_low)
        def _():
            send_own(extra, 3, extra_sems, extra_peer, EARLY, MIDDLE)

        for n, e in ((BELOW_SLOT, 4), (ABOVE_SLOT, 5)):
            _, source, _, inverse, bra, kind = hub_edges[e]
            offer(n, source, inverse, shift_of(bra, kind))

        @pl.when(corner_low)
        def _():
            offer(CORNER_SLOT, second, 0, shift_of(2 * row - 1, NEXT))

        swap(0, 4).wait_recv()
        for e in range(4):
            place_landed(e, own, e)
        for e in range(2):
            still, moving, place, inverse, bra, kind = hub_edges[e]
            accumulate(e, (0, slab), still, moving, place, inverse, shift_of(bra, kind), inverse == 1)
            deliver(e, kind, bra, None)

        @pl.when(corner_low)
        def _():
            send_own(extra, 3, extra_sems, extra_peer, MIDDLE, count)

        @pl.when(extra_site)
        def _():
            extra_edge()

        @pl.when(corner_high)
        def _():
            for c in range(count):
                arrived(extra, extra_sems, c)
            offer(CORNER_SLOT, extra, 0, shift_of(4 * row - 1, NEXT))

        swap(BELOW_SLOT, 2).wait_recv()
        place_landed(BELOW_SLOT, first, 0)
        place_landed(ABOVE_SLOT, second, 0)

        @pl.when(corner_low)
        def _():
            take(CORNER_SLOT, second, 1)

        @pl.when(corner_high)
        def _():
            take(CORNER_SLOT, extra, 0)

        for c in range(count):
            arrived(third, third_sems, c)

            @pl.when(corner_low)
            def _():
                arrived(extra, extra_sems, c)
                accumulate(EXTRA, parts[c], extra, second, 1, 0, shift_of(2 * row - 1, NEXT))
                if c == count - 1:
                    deliver(EXTRA, NEXT, 2 * row - 1, EXTRA_BASE)

            @pl.when(corner_high)
            def _():
                accumulate(EXTRA, parts[c], third, extra, 0, 0, shift_of(4 * row - 1, NEXT))
                if c == count - 1:
                    deliver(EXTRA, NEXT, 4 * row - 1, EXTRA_BASE)

            for e in (3, 4, 5, 2):
                still, moving, place, inverse, bra, kind = hub_edges[e]
                accumulate(e, parts[c], still, moving, place, inverse, shift_of(bra, kind), inverse == 1)

        for e in (3, 4, 5, 2):
            settle(e)
        dispatch([(e, hub_edges[e][5], hub_edges[e][4]) for e in (3, 4, 5, 2)], None)

        sent = results.at[pl.ds(0, 5)]
        remote(sent, sent, result_send.at[0], result_recv.at[0], {"ka": twin}).wait_send()

        @pl.when(corner_low)
        def _():
            delivered(EXTRA, NEXT, 2 * row - 1, EXTRA_BASE)
            swap(CORNER_SLOT).wait_send()
            sent_own(5).wait_send()

        @pl.when(corner_high)
        def _():
            delivered(EXTRA, NEXT, 4 * row - 1, EXTRA_BASE)
            swap(CORNER_SLOT).wait_send()

        swap(0, 4).wait_send()
        swap(BELOW_SLOT, 2).wait_send()
        sent_own(4).wait_send()

    outer_edges = ((0, 1, outer), (1, 0, inner))

    @pl.when(is_outer)
    def _():
        for e, inverse, bra in outer_edges:
            offer(e, own, inverse, shift_of(bra, HALF))
        swap(0, 2).wait_recv()
        for e in range(2):
            place_landed(e, own, e)
        pl.when(extra_site & ~lower_half)(extra_edge)
        for c in range(count):
            arrived(first, first_sems, c)
            for e, inverse, bra in outer_edges:
                accumulate(e, parts[c], first, own, e, inverse, shift_of(bra, HALF), inverse == 1)
        for e, inverse, bra in outer_edges:
            deliver(e, HALF, bra, 2 * e)
        pl.when(extra_site & lower_half)(extra_edge)
        for e, inverse, bra in outer_edges:
            delivered(e, HALF, bra, 2 * e)
        swap(0, 2).wait_send()
        sent_own(0, tail).wait_send()

    twin_inverse = jnp.where(column % 2 == 1, 0, 1)
    twin_bra = me - column % 2

    @pl.when(is_inner | is_far)
    def _():
        shift = shift_of(twin_bra, NEXT)
        offer(0, own, twin_inverse, shift)
        take(0, own, 0)
        for c in range(count):
            arrived(first, first_sems, c)
        accumulate(0, (0, slab), first, own, 0, twin_inverse, shift)
        deliver(0, NEXT, twin_bra, 0, twin_inverse)

        @pl.when(is_inner)
        def _():
            @pl.when(~high_source)
            def _():
                pl.semaphore_wait(late_in, 1)

            sent_own(0, tail).wait_send()
            signal(go, {"ka": far})

        @pl.when(is_far)
        def _():
            pl.semaphore_wait(go, 1)
            send_own(third, 0, third_sems, hub)

        pl.when(extra_site)(extra_edge)
        delivered(0, NEXT, twin_bra, 0)
        swap(0).wait_send()
        pl.when(is_far)(sent_own(0).wait_send)

    @pl.when(extra_site)
    def _():
        delivered(EXTRA, NEXT, extra_bra, EXTRA_BASE)
        swap(OWN_EXTRA).wait_send()

    @pl.when(is_outer | is_inner)
    def _():
        sent_own(1, slab - tail).wait_send()

    @pl.when(is_outer | is_hub)
    def _():
        sent_own(2).wait_send()

    @pl.when(extra_source)
    def _():
        sent_own(3).wait_send()

    for n, (sends, peer) in enumerate(notices):
        pl.when(sends)(notice(n, peer).wait_send)

    pltpu.make_async_copy(slots, slots, result_recv.at[0]).wait()
    found = [slots[kind, 0] + slots[kind, 1] for kind in range(ROLES)]
    for b in range(ROLES):
        target = near_ref[0, b]
        chosen = jnp.where(target == (me + row) % points, found[ROW], found[HALF])
        chosen = jnp.where(target == (me + 1) % points, found[NEXT], chosen)
        out_ref[b, 0] = chosen[:, :bands]
        out_ref[b, 1] = chosen[:, bands:]


def meet(neighbour, shift_id, block_map, own, points, capacity):
    slab, bands, lanes = own.shape[0], own.shape[2], own.shape[3]
    block = own.shape[1:]
    shifts = block_map.shape[0]
    half = bands // 2
    dma = pltpu.SemaphoreType.DMA
    flows = len(pieces(slab))

    def blocks(count):
        return pltpu.VMEM((count,) + block, own.dtype)

    return pl.pallas_call(
        functools.partial(meet_kernel, points, slab, capacity),
        out_shape=pltpu.VMEM((ROLES, 2, half, bands), jnp.float32),
        in_specs=[pl.BlockSpec(memory_space=pl.ANY)] * 4,
        out_specs=pl.BlockSpec(memory_space=pltpu.VMEM),
        scratch_shapes=[
            pltpu.SMEM(neighbour.shape, jnp.int32),
            pltpu.SMEM(shift_id.shape, jnp.int32),
            pltpu.VMEM(block_map.shape, jnp.int32),
            blocks(slab + 5 * capacity),
            blocks(slab + capacity),
            blocks(slab + 2 * capacity),
            blocks(slab),
            blocks(slab + capacity),
            blocks(8 * capacity),
            blocks(8 * capacity),
            pltpu.VMEM((1, lanes), jnp.int32),
            pltpu.VMEM((points, 1, lanes), jnp.int32),
            pltpu.VMEM((4 * shifts, lanes), jnp.int32),
            pltpu.VMEM((7, 2 * bands, 2 * bands), jnp.float32),
            pltpu.VMEM((7, bands, 2 * bands), jnp.float32),
            pltpu.VMEM((ROLES, 2, half, 2 * bands), jnp.float32),
            pltpu.SMEM((points, 1, lanes), jnp.int32),
            pltpu.SMEM((4 * shifts, lanes), jnp.int32),
            dma((4,)), dma((5,)), dma((5,)), dma((6,)),
            dma((flows,)), dma((flows,)), dma((flows,)), dma((flows,)),
            dma((4,)), dma((4,)), dma((6,)), dma((1,)),
            pltpu.SemaphoreType.REGULAR,
            pltpu.SemaphoreType.REGULAR,
        ],
        compiler_params=pltpu.CompilerParams(
            collective_id=0, has_side_effects=True, vmem_limit_bytes=60 * 2**20
        ),
        name="meet",
    )(neighbour, shift_id, block_map, own)


def on_four_levels(coeffs, neighbour, shift_id, block_map):
    own = coeffs[0]
    points = lax.axis_size("ka")
    capacity = 2 * max(1, own.shape[0] // 12)
    return meet(neighbour, shift_id, block_map, own, points, capacity)[None]


def solution(mesh):
    in_specs = (P("ka", "ga", None, None, None), P("ka", None), P("ka", None), P())
    out_specs = P("ka", None, None, "ga", None)
    levels = mesh.shape["ka"] // 4
    square = mesh.shape["ga"] == 2 and mesh.shape["ka"] == 4 * levels and levels == 4

    def run(coeffs, neighbour, shift_id, block_map):
        one_each = coeffs.shape[0] == mesh.shape["ka"] and neighbour.shape[1] == ROLES
        per_slice = coeffs.shape[1] // mesh.shape["ga"]
        lanes = coeffs.shape[4]
        fits = per_slice % 40 == 0 and 80 <= per_slice <= lanes and 2 * coeffs.shape[3] == lanes
        body = on_four_levels if square and one_each and fits else on_device
        return jax.shard_map(
            body, mesh=mesh, in_specs=in_specs, out_specs=out_specs, check_vma=False
        )(coeffs, neighbour, shift_id, block_map)

    return run
```

```python
import functools

import jax
import jax.numpy as jnp
from jax import lax
from jax.sharding import PartitionSpec as P
from jax.experimental import pallas as pl
from jax.experimental.pallas import tpu as pltpu

ROLES = 3


def shifted(block, axis, distance):
    devices = range(lax.axis_size(axis))
    route = [((i - distance) % len(devices), i) for i in devices]
    return lax.ppermute(block, axis, route)


def complex_intersection(bra_real, bra_imag, ket_real, ket_imag, form):
    real_part = jnp.einsum(form, bra_real, ket_real, preferred_element_type=jnp.float32)
    real_part = real_part + jnp.einsum(form, bra_imag, ket_imag, preferred_element_type=jnp.float32)
    imag_part = jnp.einsum(form, bra_real, ket_imag, preferred_element_type=jnp.float32)
    imag_part = imag_part - jnp.einsum(form, bra_imag, ket_real, preferred_element_type=jnp.float32)
    return jnp.stack([real_part, imag_part], axis=-3)


def slot_plan(
    home_slice, target_slice, sent_local, place_local, my_slice, slices, capacity, slab_blocks
):
    targets = jnp.arange(slices, dtype=jnp.int32)
    chosen = (home_slice == my_slice)[:, None, :] & (
        target_slice[:, None, :] == targets[None, :, None]
    )
    chosen = chosen & (targets != my_slice)[None, :, None]
    counted = jnp.cumsum(chosen.astype(jnp.int32), axis=2) - 1
    places = jnp.arange(capacity, dtype=jnp.int32)
    matched = (
        chosen[:, :, None, :] & (counted[:, :, None, :] == places[None, None, :, None])
    ).astype(jnp.int32)
    filled = jnp.sum(matched, axis=3)
    sent_block = jnp.sum(matched * sent_local[:, None, None, :], axis=3)
    where_to = jnp.sum(matched * place_local[:, None, None, :], axis=3) + (1 - filled) * slab_blocks
    pair_count = home_slice.shape[0]
    return (
        sent_block.reshape(pair_count, slices * capacity),
        where_to.reshape(pair_count, slices * capacity),
    )


def on_device(coeffs, neighbour, shift_id, block_map):
    k_local = coeffs.shape[0]
    slab_blocks = coeffs.shape[1]
    band_count = coeffs.shape[3]
    lane_width = coeffs.shape[4]
    vector_count = neighbour.shape[1]
    cycle_size = lax.axis_size("ka")
    slices = lax.axis_size("ga")
    my_cycle = lax.axis_index("ka")
    my_slice = lax.axis_index("ga")
    capacity = 2 * max(1, slab_blocks // 12)
    all_blocks = slab_blocks * slices
    pair_count = k_local * vector_count
    k_total = k_local * cycle_size
    row_points = min(16, k_total // 4)
    row_devices = row_points // k_local
    pad_spec = ((0, 0), (0, 1), (0, 0), (0, 0), (0, 0))
    row_point = shifted(coeffs, "ka", -1)
    row_source = jnp.mod(my_cycle + 1, cycle_size)
    plane_kets = shifted(coeffs, "ka", -row_devices)
    plane_source = jnp.mod(my_cycle + row_devices, cycle_size)
    opposite = shifted(coeffs, "ka", cycle_size // 2)
    targets_flat = neighbour.reshape(-1)
    shifts_flat = shift_id.reshape(-1)
    target_device = targets_flat // k_local
    target_lane = targets_flat - target_device * k_local
    ket_index = jnp.where(
        target_device == my_cycle,
        target_lane,
        jnp.where(
            target_device == row_source,
            k_local,
            jnp.where(
                target_device == plane_source,
                k_local + 1 + target_lane,
                2 * k_local + 1 + target_lane,
            ),
        ),
    )
    bra_index = jnp.arange(pair_count, dtype=jnp.int32) // vector_count
    picks = (
        shifts_flat[:, None] == jnp.arange(block_map.shape[0], dtype=jnp.int32)[None, :]
    ).astype(jnp.int32)
    relabel = jnp.sum(picks[:, :, None] * block_map[None, :, :], axis=1)
    dest_global = jnp.broadcast_to(jnp.arange(all_blocks, dtype=jnp.int32)[None, :], relabel.shape)
    source_slice = relabel // slab_blocks
    dest_slice = dest_global // slab_blocks
    source_local = relabel - source_slice * slab_blocks
    dest_local = dest_global - dest_slice * slab_blocks
    kets = jnp.pad(jnp.concatenate([coeffs, row_point, plane_kets, opposite], axis=0), pad_spec)
    own_source = lax.dynamic_slice_in_dim(relabel, my_slice * slab_blocks, slab_blocks, 1)
    self_place = jnp.where(
        own_source // slab_blocks == my_slice, own_source - my_slice * slab_blocks, slab_blocks
    )
    ket_self = kets[ket_index[:, None], self_place]
    ket_self = ket_self.reshape(k_local, vector_count, slab_blocks, 2, band_count, lane_width)
    local_terms = complex_intersection(
        coeffs[:, :, 0],
        coeffs[:, :, 1],
        ket_self[:, :, :, 0],
        ket_self[:, :, :, 1],
        "ksmw,kbsnw->kbmn",
    )
    sent_block, where_to = slot_plan(
        dest_slice, source_slice, dest_local, source_local, my_slice, slices, capacity, slab_blocks
    )
    payload = coeffs[bra_index[:, None], sent_block]
    owner = jnp.broadcast_to(ket_index[:, None], (pair_count, slices))
    blocks = lax.all_to_all(payload, "ga", split_axis=1, concat_axis=1, tiled=True)
    places_in = lax.all_to_all(where_to, "ga", split_axis=1, concat_axis=1, tiled=True)
    owners = lax.all_to_all(owner, "ga", split_axis=1, concat_axis=1, tiled=True)
    partner = kets[owners[:, 0][:, None], places_in]
    remote = complex_intersection(
        blocks[:, :, 0], blocks[:, :, 1], partner[:, :, 0], partner[:, :, 1], "ismw,isnw->imn"
    )
    summed_part = local_terms + remote.reshape(k_local, vector_count, 2, band_count, band_count)
    total = lax.psum(summed_part, "ga")
    row_count = band_count // slices
    return lax.dynamic_slice_in_dim(total, my_slice * row_count, row_count, 3)


def index_tables(block_map, my_slice, slab, capacity):
    shifts, blocks = block_map.shape
    exact = jnp.bfloat16
    base = (my_slice * slab).astype(jnp.float32)

    def lane_product(left, right, axis):
        return lax.dot_general(
            left.astype(exact), right.astype(exact), (((1,), (axis,)), ((), ())),
            preferred_element_type=jnp.float32,
        )

    def ones(mask):
        return jnp.where(mask, 1.0, 0.0)

    def place_rows(table):
        return lax.broadcasted_iota(jnp.int32, table.shape, 0)

    forward = block_map.astype(jnp.float32)
    counted = lax.broadcasted_iota(jnp.int32, (shifts, blocks), 1).astype(jnp.float32)
    block_rows = lax.broadcasted_iota(jnp.int32, (blocks, blocks), 0)
    inverse = jnp.zeros((shifts, blocks), jnp.float32)
    for r in range(shifts):
        row = lane_product(counted, ones(block_map[r : r + 1, :] == block_rows), 1)
        inverse = jnp.where(place_rows(row) == r, row, inverse)
    before = ones(
        lax.broadcasted_iota(jnp.int32, (slab, slab), 0)
        < lax.broadcasted_iota(jnp.int32, (slab, slab), 1)
    )
    padded = -(-capacity // 8) * 8
    slots = lax.broadcasted_iota(jnp.int32, (padded, slab), 0).astype(jnp.float32)
    indexes, sends = [], []
    for table in (forward, inverse):
        low, high = table[:, :slab], table[:, slab:]
        mine = jnp.where(my_slice == 0, low, high) - base
        other = jnp.where(my_slice == 0, high, low) - base
        inside = (mine >= 0) & (mine < slab)
        rank = jnp.minimum(lane_product(1.0 - ones(inside), before, 0), capacity - 1.0)
        at = jnp.where(inside, mine, slab + rank).astype(jnp.int32)
        indexes.append(jnp.clip(at, 0, slab + capacity - 1))
        wanted = ones((other >= 0) & (other < slab))
        rank = lane_product(wanted, before, 0)
        rank = jnp.where(wanted > 0, rank, -1.0)
        send = jnp.zeros((shifts, padded), jnp.float32)
        for r in range(shifts):
            row = lane_product(other, ones(rank[r : r + 1, :] == slots), 1)
            send = jnp.where(place_rows(row) == r, row, send)
        sends.append(jnp.clip(send.astype(jnp.int32), 0, slab - 1))
    return indexes, sends, padded


def cut(slab, twentieths):
    unit = slab // 20
    sizes = [unit * n for n in twentieths]
    return [(sum(sizes[:n]), sizes[n]) for n in range(len(sizes))]


def main_pieces(slab):
    return cut(slab, (1, 3, 5, 5, 4, 1, 1))


def late_pieces(slab):
    *most, (start, size) = cut(slab, (9, 6, 3, 1, 1))
    return [*most, (start, size - 2), (start + size - 2, 2)]


def extra_pieces(slab):
    return cut(slab, (10, 6, 3, 1))


def meet_kernel(
    points, slab, capacity, near_hbm, shift_hbm, map_hbm, own_hbm, out_ref,
    near_ref, shift_ref, map_ref, own, first, second, third, extra, packs, landed,
    meta_out, meta_in, tables, sums, results, slots, meta, table_at,
    local_sems, meta_sems, send_sems, first_sems, second_sems, third_sems, extra_sems,
    swap_send, swap_recv, result_sems, go, late_in,
):
    levels = 4
    row = points // levels
    me = lax.axis_index("ka")
    my_slice = lax.axis_index("ga")
    partner = 1 - my_slice
    z, column = me // row, me % row
    low = (column == 0) | (column == row - 1)
    role = jnp.where(low, z, levels - 1 - z)
    is_outer, is_hub, is_inner, is_far = role == 0, role == 1, role == 2, role == 3

    def member(r):
        return jnp.where(low, r, levels - 1 - r) * row + column

    outer, hub, inner, far = member(0), member(1), member(2), member(3)
    below, above = hub - row, hub + row
    twin = me + 1 - 2 * (column % 2)
    lower_half = z < 2
    bands, lanes = own.shape[2], own.shape[3]
    shifts = map_hbm.shape[0]
    parts, late_parts, extra_parts = main_pieces(slab), late_pieces(slab), extra_pieces(slab)
    count = len(parts)
    tail = parts[count - 1][0]

    barrier = pltpu.get_barrier_semaphore()
    mesh = pl.DeviceIdType.MESH
    corner_low = me == row
    corner_high = me == 2 * row - 1
    high_source = me == 3 * row - 1
    high_site = me == 3 * row

    def signal(semaphore, peer):
        pl.semaphore_signal(semaphore, inc=1, device_id=peer, device_id_type=mesh)

    signal(barrier, {"ga": partner})
    signal(barrier, {"ka": twin})
    greetings = (
        (~is_hub, hub), (is_hub, outer), (is_hub, inner), (is_hub | is_inner, far),
        (column == 1, me + 1), (column == 2, me - 1), (me == row - 1, row), (corner_low, row - 1),
        (corner_low, 2 * row - 1), (corner_high, row), (high_source, 3 * row),
    )
    for greets, peer in greetings:

        @pl.when(greets)
        def _():
            signal(barrier, {"ka": peer})

    expected = (
        (is_hub, 3), (~is_hub, 1), (is_far, 1), ((column == 1) | (column == 2), 1),
        (me == row - 1, 1), (corner_low, 2), (corner_high, 1), (high_site, 1),
    )
    greeted = jnp.int32(2)
    for hears, amount in expected:
        greeted = greeted + jnp.where(hears, amount, 0)
    near_in = pltpu.make_async_copy(near_hbm, near_ref, local_sems.at[0])
    shift_in = pltpu.make_async_copy(shift_hbm, shift_ref, local_sems.at[1])
    map_in = pltpu.make_async_copy(map_hbm, map_ref, local_sems.at[2])
    keep = pltpu.make_async_copy(own_hbm, own.at[pl.ds(0, slab)], local_sems.at[3])
    for copy in (near_in, shift_in, map_in, keep):
        copy.start()
    pl.semaphore_wait(barrier, greeted)

    @pl.when(is_far)
    def _():
        signal(late_in, {"ka": inner})

    @pl.when(high_site)
    def _():
        signal(late_in, {"ka": me - 1})

    def remote(source, target, send, recv, peer):
        return pltpu.make_async_remote_copy(
            src_ref=source, dst_ref=target, send_sem=send, recv_sem=recv,
            device_id=peer, device_id_type=mesh,
        )

    def send_own(target, n, sems, peer, cuts):
        for c, (start, size) in cuts:
            part = pl.ds(start, size)
            remote(own_hbm.at[part], target.at[part], send_sems.at[n], sems.at[c], {"ka": peer}).start()

    def sent_own(n, size=slab):
        part = pl.ds(0, size)
        return remote(own_hbm.at[part], own.at[part], send_sems.at[n], first_sems.at[0], {"ka": twin})

    def arrived(buffer, sems, c, cuts):
        part = buffer.at[pl.ds(*cuts[c])]
        remote(part, part, send_sems.at[0], sems.at[c], {"ka": twin}).wait_recv()

    def main_sends(pairs):
        @pl.when(me == below)
        def _():
            for n, start, stop in pairs:
                send_own(first, n, first_sems, hub, list(enumerate(parts))[start:stop])

        @pl.when(me == above)
        def _():
            for n, start, stop in pairs:
                send_own(second, n, second_sems, hub, list(enumerate(parts))[start:stop])

    main_sends(((0, 0, 1),))
    near_in.wait()
    shift_in.wait()

    def role_shift(step):
        target = (me + step) % points
        total = jnp.int32(0)
        for b in range(ROLES):
            total = total + jnp.where(near_ref[0, b] == target, shift_ref[0, b], 0)
        return total

    lane = lax.broadcasted_iota(jnp.int32, meta_out.shape, 1)
    facts = jnp.where(
        lane == 0, role_shift(1), jnp.where(lane == 1, role_shift(row), role_shift(points // 2))
    )
    meta_out[...] = facts
    meta_in[me] = facts

    steps_up = (z >= 2) & (column % 2 == 1) & (me != points - 1)
    notices = (
        (~is_hub, hub),
        (is_hub, outer),
        (me == me, twin),
        (steps_up, me + 1),
        (corner_high, row),
    )
    steps_in = (z >= 2) & (column % 2 == 0) & (me != 2 * row)
    heard = jnp.where(is_hub, 4, jnp.where(is_outer, 2, 1)) + jnp.where(steps_in | corner_low, 1, 0)
    told = 2 + jnp.where(steps_up | corner_high, 1, 0)

    def notice(n, peer):
        source = meta_out if n != 1 else meta_in.at[inner]
        target = meta_in.at[me] if n != 1 else meta_in.at[inner]
        return remote(source, target, meta_sems.at[0], meta_sems.at[1], {"ka": peer})

    def facts_of(amount):
        fact = meta_in.at[pl.ds(0, amount)]
        return remote(fact, fact, meta_sems.at[0], meta_sems.at[1], {"ka": twin})

    for n in (0, 2, 4):
        pl.when(notices[n][0])(notice(n, notices[n][1]).start)

    main_sends(((0, 1, count - 1), (1, count - 1, count)))

    @pl.when(high_source)
    def _():
        pl.semaphore_wait(late_in, 2)

    pl.when(steps_up)(notice(3, me + 1).start)
    extra_cuts = list(enumerate(extra_parts))
    extra_down = (me == 2) | (me == row + 2)
    extra_up = (me == 2 * row + 1) | (me == 2 * row + 3) | (me == 3 * row + 1)
    extra_source = extra_down | extra_up | corner_low | corner_high
    extra_site = (
        (me == row - 1) | (me == 1) | (me == row + 1)
        | (me == 2 * row + 2) | (me == 3 * row) | (me == 3 * row + 2)
    )
    extra_peer = jnp.where(corner_high, row, jnp.where(extra_up, me + 1, me - 1))

    @pl.when(extra_down | extra_up | corner_high)
    def _():
        send_own(extra, 3, extra_sems, extra_peer, extra_cuts)

    @pl.when(corner_low)
    def _():
        send_own(extra, 3, extra_sems, extra_peer, extra_cuts[:1])

    @pl.when(is_outer | is_hub)
    def _():
        send_own(first, 2, first_sems, twin, list(enumerate(parts)))

    map_in.wait()
    indexes, sends, padded = index_tables(map_ref[...], my_slice, slab, capacity)
    tables[...] = jnp.zeros_like(tables)
    for d in range(2):
        tables[pl.ds(d * shifts, shifts), pl.ds(0, slab)] = indexes[d]
        tables[pl.ds((2 + d) * shifts, shifts), pl.ds(0, padded)] = sends[d]
    tables_in = pltpu.make_async_copy(tables, table_at, local_sems.at[0])
    tables_in.start()

    def corner_copy(c):
        part = pl.ds(*parts[c])
        return remote(first.at[part], extra.at[part], send_sems.at[5], extra_sems.at[0], {"ka": 2 * row - 1})

    def relayed(source, c):
        part = pl.ds(*parts[c])
        return remote(source.at[part], first.at[part], send_sems.at[4], first_sems.at[c], {"ka": outer})

    def relay(c):
        arrived(second, second_sems, c, parts)
        pl.when(low)(relayed(second, c).start)
        arrived(first, first_sems, c, parts)
        pl.when(~low)(relayed(first, c).start)
        pl.when(corner_low)(corner_copy(c).start)

    @pl.when(is_hub)
    def _():
        relay(0)

    for amount in range(1, 6):
        pl.when(heard == amount)(facts_of(amount).wait_recv)

    pl.when(is_hub)(notice(1, outer).start)
    meta_copy = pltpu.make_async_copy(meta_in, meta, local_sems.at[1])
    meta_copy.start()
    meta_copy.wait()
    tables_in.wait()
    keep.wait()

    def shift_of(point, kind):
        return meta[point, 0, kind]

    NEXT, ROW, HALF = 0, 1, 2
    OWN_EXTRA, BELOW_SLOT, ABOVE_SLOT, CORNER_SLOT = 4, 5, 6, 7
    groups = (0, 0, 0, 0, 1, 2, 2, 3)

    def swap(n, many=1):
        part = pl.ds(n * capacity, many * capacity)
        group = groups[n]
        return remote(packs.at[part], landed.at[part], swap_send.at[0], swap_recv.at[group], {"ga": partner})

    def place_landed(n, target, place):
        def move(r, carry):
            target[slab + place * capacity + r] = landed[n * capacity + r]
            return carry

        lax.fori_loop(0, capacity, move, 0, unroll=4)

    def take(n, target, place):
        swap(n).wait_recv()
        place_landed(n, target, place)

    def offer(n, source, inverse, shift):
        line = (2 + inverse) * shifts + shift

        def gather(r, carry):
            packs[n * capacity + r] = source[table_at[line, r]]
            return carry

        lax.fori_loop(0, capacity, gather, 0, unroll=4)
        swap(n).start()

    def pick(ref, at):
        return ref[at].reshape(2 * bands, lanes)

    def accumulate(e, part, still, moving, place, inverse, shift, turn=False):
        start, size = part
        line = inverse * shifts + shift

        def at(n):
            value = table_at[line, n]
            return value + jnp.where(value >= slab, place * capacity, 0)

        def products(begin, many, total):
            for u in range(0, many, 2):
                n = begin + u
                left = jnp.concatenate([pick(still, n), pick(still, n + 1)], axis=1)
                right = jnp.concatenate([pick(moving, at(n)), pick(moving, at(n + 1))], axis=1)
                total = total + lax.dot_general(
                    right if turn else left,
                    left if turn else right,
                    (((1,), (1,)), ((), ())),
                    preferred_element_type=jnp.float32,
                )
            return total

        steps = [s for s in (12, 10, 18, 6, 4, 2) if size % s == 0][0]
        if steps == size:
            sums[e] = products(start, size, sums[e])
        else:
            sums[e] = lax.fori_loop(
                0, size // steps, lambda i, total: products(start + i * steps, steps, total), sums[e]
            )

    def result_copies(e, kind, bra):
        copies = []
        half = bands // 2
        for g in (partner, my_slice):
            source = results.at[e, pl.ds(g * half, half)]
            target = slots.at[kind, my_slice]
            near = pltpu.make_async_copy(source, target, result_sems.at[1])
            away = remote(source, target, result_sems.at[0], result_sems.at[1], {"ka": bra, "ga": g})
            copies.append((bra == me, near, away))
        return copies

    def settle(e, inverse=None):
        total = sums[e]
        if inverse is not None:
            total = jnp.where(inverse == 1, total.T, total)
        upper, under = total[:bands], pltpu.roll(total[bands:], bands, 1)
        left = lax.broadcasted_iota(jnp.int32, upper.shape, 1) < bands
        results[e] = upper + jnp.where(left, under, -under)

    def dispatch(edges):
        for n in range(2):
            for e, kind, bra in edges:
                at_home, near, away = result_copies(e, kind, bra)[n]
                if n == 0:
                    away.start()
                else:
                    pl.when(at_home)(near.start)
                    pl.when(~at_home)(away.start)

    def deliver(e, kind, bra, inverse=None):
        settle(e, inverse)
        dispatch(((e, kind, bra),))

    sums[...] = jnp.zeros_like(sums)
    extra_inverse = jnp.where(lower_half, 1, 0)
    extra_bra = jnp.where(lower_half, me, me - 1)
    EXTRA = 6

    hub_edges = (
        (first, own, 0, 0, below, ROW),
        (second, own, 1, 1, hub, ROW),
        (third, own, 2, 1, hub, HALF),
        (third, own, 3, 0, far, HALF),
        (third, first, 0, 0, far, ROW),
        (third, second, 0, 1, above, ROW),
    )

    @pl.when(extra_site)
    def _():
        offer(OWN_EXTRA, own, extra_inverse, shift_of(extra_bra, NEXT))

    def extra_edge():
        take(OWN_EXTRA, own, OWN_EXTRA)
        shift = shift_of(extra_bra, NEXT)
        for c, part in extra_cuts:
            arrived(extra, extra_sems, c, extra_parts)
            accumulate(EXTRA, part, extra, own, OWN_EXTRA, extra_inverse, shift)
        deliver(EXTRA, NEXT, extra_bra, extra_inverse)

    @pl.when(is_hub)
    def _():
        for e in range(4):
            _, _, _, inverse, bra, kind = hub_edges[e]
            offer(e, own, inverse, shift_of(bra, kind))

        for c in range(1, count):
            relay(c)

        for n, e in ((BELOW_SLOT, 4), (ABOVE_SLOT, 5)):
            _, source, _, inverse, bra, kind = hub_edges[e]
            offer(n, source, inverse, shift_of(bra, kind))

        @pl.when(corner_low)
        def _():
            offer(CORNER_SLOT, second, 0, shift_of(2 * row - 1, NEXT))

        swap(0, 4).wait_recv()
        for e in range(4):
            place_landed(e, own, e)
        for e in range(2):
            still, moving, place, inverse, bra, kind = hub_edges[e]
            accumulate(e, (0, slab), still, moving, place, inverse, shift_of(bra, kind), inverse == 1)
            deliver(e, kind, bra)

        @pl.when(corner_low)
        def _():
            send_own(extra, 3, extra_sems, extra_peer, extra_cuts[1:])

        @pl.when(extra_site)
        def _():
            extra_edge()

        @pl.when(corner_high)
        def _():
            arrived(extra, extra_sems, 0, [(0, slab)])
            offer(CORNER_SLOT, extra, 0, shift_of(4 * row - 1, NEXT))

        swap(BELOW_SLOT, 2).wait_recv()
        place_landed(BELOW_SLOT, first, 0)
        place_landed(ABOVE_SLOT, second, 0)

        @pl.when(corner_low)
        def _():
            take(CORNER_SLOT, second, 1)

        @pl.when(corner_high)
        def _():
            take(CORNER_SLOT, extra, 0)

        def late_edge(e, part):
            still, moving, place, inverse, bra, kind = hub_edges[e]
            accumulate(e, part, still, moving, place, inverse, shift_of(bra, kind), inverse == 1)

        for c, part in enumerate(late_parts):
            arrived(third, third_sems, c, late_parts)
            ends = c == len(late_parts) - 1
            for pair in ((3, 4), (5, 2)):
                for e in pair:
                    late_edge(e, part)
                if ends:
                    for e in pair:
                        settle(e)
                    dispatch([(e, hub_edges[e][5], hub_edges[e][4]) for e in pair])

            @pl.when(corner_high)
            def _():
                accumulate(EXTRA, part, third, extra, 0, 0, shift_of(4 * row - 1, NEXT))
                if ends:
                    deliver(EXTRA, NEXT, 4 * row - 1)

            if c < len(extra_parts):

                @pl.when(corner_low)
                def _():
                    arrived(extra, extra_sems, c, extra_parts)
                    accumulate(EXTRA, extra_parts[c], extra, second, 1, 0, shift_of(2 * row - 1, NEXT))
                    if c == len(extra_parts) - 1:
                        deliver(EXTRA, NEXT, 2 * row - 1)

        pl.when(corner_low)(sent_own(5).wait_send)
        sent_own(4).wait_send()

    outer_edges = ((0, 1, outer), (1, 0, inner))

    @pl.when(is_outer)
    def _():
        for e, inverse, bra in outer_edges:
            offer(e, own, inverse, shift_of(bra, HALF))
        swap(0, 2).wait_recv()
        for e in range(2):
            place_landed(e, own, e)
        pl.when(extra_site & ~lower_half)(extra_edge)
        for c, part in enumerate(parts):
            arrived(first, first_sems, c, parts)
            for e, inverse, bra in outer_edges:
                accumulate(e, part, first, own, e, inverse, shift_of(bra, HALF), inverse == 1)
        for e, inverse, bra in outer_edges:
            deliver(e, HALF, bra)
        pl.when(extra_site & lower_half)(extra_edge)
        sent_own(0, tail).wait_send()

    twin_inverse = jnp.where(column % 2 == 1, 0, 1)
    twin_bra = me - column % 2

    @pl.when(is_inner | is_far)
    def _():
        shift = shift_of(twin_bra, NEXT)
        offer(0, own, twin_inverse, shift)
        take(0, own, 0)
        for c in range(count):
            arrived(first, first_sems, c, parts)
        accumulate(0, (0, slab), first, own, 0, twin_inverse, shift)
        deliver(0, NEXT, twin_bra, twin_inverse)

        @pl.when(is_inner)
        def _():
            @pl.when(~high_source)
            def _():
                pl.semaphore_wait(late_in, 1)

            sent_own(0, tail).wait_send()
            signal(go, {"ka": far})

        @pl.when(is_far)
        def _():
            pl.semaphore_wait(go, 1)
            send_own(third, 0, third_sems, hub, list(enumerate(late_parts)))

        pl.when(extra_site)(extra_edge)
        pl.when(is_far)(sent_own(0).wait_send)

    @pl.when(is_outer | is_inner)
    def _():
        sent_own(1, slab - tail).wait_send()

    @pl.when(is_outer | is_hub)
    def _():
        sent_own(2).wait_send()

    @pl.when(extra_source)
    def _():
        sent_own(3).wait_send()

    for amount in (2, 3):
        pl.when(told == amount)(facts_of(amount).wait_send)

    packed = jnp.where(is_hub, 6, jnp.where(is_outer, 2, 1)) + jnp.where(extra_site | corner_low | corner_high, 1, 0)
    for amount in (1, 2, 3, 6, 7):
        pl.when(packed == amount)(swap(0, amount).wait_send)

    own_twin = jnp.where(column % 2 == 0, 1, 2)
    sent_results = jnp.where(is_hub, 10, jnp.where(is_outer, 3, own_twin))
    sent_results = sent_results + jnp.where(corner_low | corner_high, 2, 0)
    sent_results = sent_results + jnp.where(extra_site, jnp.where(lower_half, 1, 2), 0)
    for amount in (1, 2, 3, 4, 5, 10, 12):
        halves = results.at[pl.ds(0, amount), pl.ds(0, bands // 2)] if amount < 8 else results.at[pl.ds(0, amount // 2)]
        done = remote(halves, halves, result_sems.at[0], result_sems.at[1], {"ka": twin})
        pl.when(sent_results == amount)(done.wait_send)

    pltpu.make_async_copy(slots, slots, result_sems.at[1]).wait()
    found = [slots[kind, 0] + slots[kind, 1] for kind in range(ROLES)]
    for b in range(ROLES):
        target = near_ref[0, b]
        chosen = jnp.where(target == (me + row) % points, found[ROW], found[HALF])
        chosen = jnp.where(target == (me + 1) % points, found[NEXT], chosen)
        out_ref[b, 0] = chosen[:, :bands]
        out_ref[b, 1] = chosen[:, bands:]


def meet(neighbour, shift_id, block_map, own, points, capacity):
    slab, bands, lanes = own.shape[0], own.shape[2], own.shape[3]
    block = own.shape[1:]
    shifts = block_map.shape[0]
    half = bands // 2
    dma = pltpu.SemaphoreType.DMA
    mains, lates, extras = (len(f(slab)) for f in (main_pieces, late_pieces, extra_pieces))

    def blocks(count):
        return pltpu.VMEM((count,) + block, own.dtype)

    return pl.pallas_call(
        functools.partial(meet_kernel, points, slab, capacity),
        out_shape=pltpu.VMEM((ROLES, 2, half, bands), jnp.float32),
        in_specs=[pl.BlockSpec(memory_space=pl.ANY)] * 4,
        out_specs=pl.BlockSpec(memory_space=pltpu.VMEM),
        scratch_shapes=[
            pltpu.SMEM(neighbour.shape, jnp.int32),
            pltpu.SMEM(shift_id.shape, jnp.int32),
            pltpu.VMEM(block_map.shape, jnp.int32),
            blocks(slab + 5 * capacity),
            blocks(slab + capacity),
            blocks(slab + 2 * capacity),
            blocks(slab),
            blocks(slab + capacity),
            blocks(8 * capacity),
            blocks(8 * capacity),
            pltpu.VMEM((1, lanes), jnp.int32),
            pltpu.VMEM((points, 1, lanes), jnp.int32),
            pltpu.VMEM((4 * shifts, lanes), jnp.int32),
            pltpu.VMEM((7, 2 * bands, 2 * bands), jnp.float32),
            pltpu.VMEM((7, bands, 2 * bands), jnp.float32),
            pltpu.VMEM((ROLES, 2, half, 2 * bands), jnp.float32),
            pltpu.SMEM((points, 1, lanes), jnp.int32),
            pltpu.SMEM((4 * shifts, lanes), jnp.int32),
            dma((4,)), dma((2,)), dma((6,)),
            dma((mains,)), dma((mains,)), dma((lates,)), dma((extras,)),
            dma((1,)), dma((4,)), dma((2,)),
            pltpu.SemaphoreType.REGULAR,
            pltpu.SemaphoreType.REGULAR,
        ],
        compiler_params=pltpu.CompilerParams(
            collective_id=0, has_side_effects=True, vmem_limit_bytes=60 * 2**20
        ),
        name="meet",
    )(neighbour, shift_id, block_map, own)


def on_four_levels(coeffs, neighbour, shift_id, block_map):
    own = coeffs[0]
    points = lax.axis_size("ka")
    capacity = 2 * max(1, own.shape[0] // 12)
    return meet(neighbour, shift_id, block_map, own, points, capacity)[None]


def solution(mesh):
    in_specs = (P("ka", "ga", None, None, None), P("ka", None), P("ka", None), P())
    out_specs = P("ka", None, None, "ga", None)
    levels = mesh.shape["ka"] // 4
    square = mesh.shape["ga"] == 2 and mesh.shape["ka"] == 4 * levels and levels == 4

    def run(coeffs, neighbour, shift_id, block_map):
        one_each = coeffs.shape[0] == mesh.shape["ka"] and neighbour.shape[1] == ROLES
        per_slice = coeffs.shape[1] // mesh.shape["ga"]
        lanes = coeffs.shape[4]
        fits = per_slice % 40 == 0 and 80 <= per_slice <= lanes and 2 * coeffs.shape[3] == lanes
        body = on_four_levels if square and one_each and fits else on_device
        return jax.shard_map(
            body, mesh=mesh, in_specs=in_specs, out_specs=out_specs, check_vma=False
        )(coeffs, neighbour, shift_id, block_map)

    return run
```

```python
import functools

import jax
import jax.numpy as jnp
from jax import lax
from jax.sharding import PartitionSpec as P
from jax.experimental import pallas as pl
from jax.experimental.pallas import tpu as pltpu

ROLES = 3


def shifted(block, axis, distance):
    devices = range(lax.axis_size(axis))
    route = [((i - distance) % len(devices), i) for i in devices]
    return lax.ppermute(block, axis, route)


def complex_intersection(bra_real, bra_imag, ket_real, ket_imag, form):
    real_part = jnp.einsum(form, bra_real, ket_real, preferred_element_type=jnp.float32)
    real_part = real_part + jnp.einsum(form, bra_imag, ket_imag, preferred_element_type=jnp.float32)
    imag_part = jnp.einsum(form, bra_real, ket_imag, preferred_element_type=jnp.float32)
    imag_part = imag_part - jnp.einsum(form, bra_imag, ket_real, preferred_element_type=jnp.float32)
    return jnp.stack([real_part, imag_part], axis=-3)


def slot_plan(
    home_slice, target_slice, sent_local, place_local, my_slice, slices, capacity, slab_blocks
):
    targets = jnp.arange(slices, dtype=jnp.int32)
    chosen = (home_slice == my_slice)[:, None, :] & (
        target_slice[:, None, :] == targets[None, :, None]
    )
    chosen = chosen & (targets != my_slice)[None, :, None]
    counted = jnp.cumsum(chosen.astype(jnp.int32), axis=2) - 1
    places = jnp.arange(capacity, dtype=jnp.int32)
    matched = (
        chosen[:, :, None, :] & (counted[:, :, None, :] == places[None, None, :, None])
    ).astype(jnp.int32)
    filled = jnp.sum(matched, axis=3)
    sent_block = jnp.sum(matched * sent_local[:, None, None, :], axis=3)
    where_to = jnp.sum(matched * place_local[:, None, None, :], axis=3) + (1 - filled) * slab_blocks
    pair_count = home_slice.shape[0]
    return (
        sent_block.reshape(pair_count, slices * capacity),
        where_to.reshape(pair_count, slices * capacity),
    )


def on_device(coeffs, neighbour, shift_id, block_map):
    k_local = coeffs.shape[0]
    slab_blocks = coeffs.shape[1]
    band_count = coeffs.shape[3]
    lane_width = coeffs.shape[4]
    vector_count = neighbour.shape[1]
    cycle_size = lax.axis_size("ka")
    slices = lax.axis_size("ga")
    my_cycle = lax.axis_index("ka")
    my_slice = lax.axis_index("ga")
    capacity = 2 * max(1, slab_blocks // 12)
    all_blocks = slab_blocks * slices
    pair_count = k_local * vector_count
    k_total = k_local * cycle_size
    row_points = min(16, k_total // 4)
    row_devices = row_points // k_local
    pad_spec = ((0, 0), (0, 1), (0, 0), (0, 0), (0, 0))
    row_point = shifted(coeffs, "ka", -1)
    row_source = jnp.mod(my_cycle + 1, cycle_size)
    plane_kets = shifted(coeffs, "ka", -row_devices)
    plane_source = jnp.mod(my_cycle + row_devices, cycle_size)
    opposite = shifted(coeffs, "ka", cycle_size // 2)
    targets_flat = neighbour.reshape(-1)
    shifts_flat = shift_id.reshape(-1)
    target_device = targets_flat // k_local
    target_lane = targets_flat - target_device * k_local
    ket_index = jnp.where(
        target_device == my_cycle,
        target_lane,
        jnp.where(
            target_device == row_source,
            k_local,
            jnp.where(
                target_device == plane_source,
                k_local + 1 + target_lane,
                2 * k_local + 1 + target_lane,
            ),
        ),
    )
    bra_index = jnp.arange(pair_count, dtype=jnp.int32) // vector_count
    picks = (
        shifts_flat[:, None] == jnp.arange(block_map.shape[0], dtype=jnp.int32)[None, :]
    ).astype(jnp.int32)
    relabel = jnp.sum(picks[:, :, None] * block_map[None, :, :], axis=1)
    dest_global = jnp.broadcast_to(jnp.arange(all_blocks, dtype=jnp.int32)[None, :], relabel.shape)
    source_slice = relabel // slab_blocks
    dest_slice = dest_global // slab_blocks
    source_local = relabel - source_slice * slab_blocks
    dest_local = dest_global - dest_slice * slab_blocks
    kets = jnp.pad(jnp.concatenate([coeffs, row_point, plane_kets, opposite], axis=0), pad_spec)
    own_source = lax.dynamic_slice_in_dim(relabel, my_slice * slab_blocks, slab_blocks, 1)
    self_place = jnp.where(
        own_source // slab_blocks == my_slice, own_source - my_slice * slab_blocks, slab_blocks
    )
    ket_self = kets[ket_index[:, None], self_place]
    ket_self = ket_self.reshape(k_local, vector_count, slab_blocks, 2, band_count, lane_width)
    local_terms = complex_intersection(
        coeffs[:, :, 0],
        coeffs[:, :, 1],
        ket_self[:, :, :, 0],
        ket_self[:, :, :, 1],
        "ksmw,kbsnw->kbmn",
    )
    sent_block, where_to = slot_plan(
        dest_slice, source_slice, dest_local, source_local, my_slice, slices, capacity, slab_blocks
    )
    payload = coeffs[bra_index[:, None], sent_block]
    owner = jnp.broadcast_to(ket_index[:, None], (pair_count, slices))
    blocks = lax.all_to_all(payload, "ga", split_axis=1, concat_axis=1, tiled=True)
    places_in = lax.all_to_all(where_to, "ga", split_axis=1, concat_axis=1, tiled=True)
    owners = lax.all_to_all(owner, "ga", split_axis=1, concat_axis=1, tiled=True)
    partner = kets[owners[:, 0][:, None], places_in]
    remote = complex_intersection(
        blocks[:, :, 0], blocks[:, :, 1], partner[:, :, 0], partner[:, :, 1], "ismw,isnw->imn"
    )
    summed_part = local_terms + remote.reshape(k_local, vector_count, 2, band_count, band_count)
    total = lax.psum(summed_part, "ga")
    row_count = band_count // slices
    return lax.dynamic_slice_in_dim(total, my_slice * row_count, row_count, 3)


def index_tables(block_map, my_slice, slab, capacity):
    shifts, blocks = block_map.shape
    exact = jnp.bfloat16
    base = (my_slice * slab).astype(jnp.float32)

    def lane_product(left, right, axis):
        return lax.dot_general(
            left.astype(exact), right.astype(exact), (((1,), (axis,)), ((), ())),
            preferred_element_type=jnp.float32,
        )

    def ones(mask):
        return jnp.where(mask, 1.0, 0.0)

    def place_rows(table):
        return lax.broadcasted_iota(jnp.int32, table.shape, 0)

    forward = block_map.astype(jnp.float32)
    counted = lax.broadcasted_iota(jnp.int32, (shifts, blocks), 1).astype(jnp.float32)
    block_rows = lax.broadcasted_iota(jnp.int32, (blocks, blocks), 0)
    inverse = jnp.zeros((shifts, blocks), jnp.float32)
    for r in range(shifts):
        row = lane_product(counted, ones(block_map[r : r + 1, :] == block_rows), 1)
        inverse = jnp.where(place_rows(row) == r, row, inverse)
    before = ones(
        lax.broadcasted_iota(jnp.int32, (slab, slab), 0)
        < lax.broadcasted_iota(jnp.int32, (slab, slab), 1)
    )
    padded = -(-capacity // 8) * 8
    slots = lax.broadcasted_iota(jnp.int32, (padded, slab), 0).astype(jnp.float32)
    indexes, sends = [], []
    for table in (forward, inverse):
        low, high = table[:, :slab], table[:, slab:]
        mine = jnp.where(my_slice == 0, low, high) - base
        other = jnp.where(my_slice == 0, high, low) - base
        inside = (mine >= 0) & (mine < slab)
        rank = jnp.minimum(lane_product(1.0 - ones(inside), before, 0), capacity - 1.0)
        at = jnp.where(inside, mine, slab + rank).astype(jnp.int32)
        indexes.append(jnp.clip(at, 0, slab + capacity - 1))
        wanted = ones((other >= 0) & (other < slab))
        rank = lane_product(wanted, before, 0)
        rank = jnp.where(wanted > 0, rank, -1.0)
        send = jnp.zeros((shifts, padded), jnp.float32)
        for r in range(shifts):
            row = lane_product(other, ones(rank[r : r + 1, :] == slots), 1)
            send = jnp.where(place_rows(row) == r, row, send)
        sends.append(jnp.clip(send.astype(jnp.int32), 0, slab - 1))
    return indexes, sends, padded


def cut(slab, twentieths):
    unit = slab // 20
    sizes = [unit * n for n in twentieths]
    return [(sum(sizes[:n]), sizes[n]) for n in range(len(sizes))]


def main_pieces(slab):
    return cut(slab, (1, 8, 8, 2, 1))


def late_pieces(slab):
    *most, (start, size) = cut(slab, (10, 6, 3, 1))
    return [*most, (start, size - 2), (start + size - 2, 2)]


def extra_pieces(slab):
    return cut(slab, (10, 9, 1))


def meet_kernel(
    points, slab, capacity, near_hbm, shift_hbm, map_hbm, own_hbm, out_ref,
    near_ref, shift_ref, map_ref, own, first, second, third, extra, packs, landed,
    meta_out, meta_in, tables, sums, results, slots, meta, table_at,
    local_sems, meta_sems, send_sems, first_sems, second_sems, third_sems, extra_sems,
    swap_send, swap_recv, result_sems, go, late_in,
):
    levels = 4
    row = points // levels
    me = lax.axis_index("ka")
    my_slice = lax.axis_index("ga")
    partner = 1 - my_slice
    z, column = me // row, me % row
    low = (column == 0) | (column == row - 1)
    role = jnp.where(low, z, levels - 1 - z)
    is_outer, is_hub, is_inner, is_far = role == 0, role == 1, role == 2, role == 3

    def member(r):
        return jnp.where(low, r, levels - 1 - r) * row + column

    outer, hub, inner, far = member(0), member(1), member(2), member(3)
    below, above = hub - row, hub + row
    twin = me + 1 - 2 * (column % 2)
    lower_half = z < 2
    bands, lanes = own.shape[2], own.shape[3]
    shifts = map_hbm.shape[0]
    parts, late_parts, extra_parts = main_pieces(slab), late_pieces(slab), extra_pieces(slab)
    count = len(parts)
    tail = parts[count - 1][0]

    barrier = pltpu.get_barrier_semaphore()
    mesh = pl.DeviceIdType.MESH
    corner_low = me == row
    corner_high = me == 2 * row - 1
    high_source = me == 3 * row - 1
    high_site = me == 3 * row

    def signal(semaphore, peer):
        pl.semaphore_signal(semaphore, inc=1, device_id=peer, device_id_type=mesh)

    signal(barrier, {"ga": partner})
    signal(barrier, {"ka": twin})
    greetings = (
        (~is_hub, hub), (is_hub, outer), (is_hub, inner), (is_hub | is_inner, far),
        (column == 1, me + 1), (column == 2, me - 1), (me == row - 1, row), (corner_low, row - 1),
        (corner_low, 2 * row - 1), (corner_high, row), (high_source, 3 * row),
    )
    for greets, peer in greetings:

        @pl.when(greets)
        def _():
            signal(barrier, {"ka": peer})

    expected = (
        (is_hub, 3), (~is_hub, 1), (is_far, 1), ((column == 1) | (column == 2), 1),
        (me == row - 1, 1), (corner_low, 2), (corner_high, 1), (high_site, 1),
    )
    greeted = jnp.int32(2)
    for hears, amount in expected:
        greeted = greeted + jnp.where(hears, amount, 0)
    near_in = pltpu.make_async_copy(near_hbm, near_ref, local_sems.at[0])
    shift_in = pltpu.make_async_copy(shift_hbm, shift_ref, local_sems.at[1])
    map_in = pltpu.make_async_copy(map_hbm, map_ref, local_sems.at[2])
    keep = pltpu.make_async_copy(own_hbm, own.at[pl.ds(0, slab)], local_sems.at[3])
    for copy in (near_in, shift_in, map_in, keep):
        copy.start()
    pl.semaphore_wait(barrier, greeted)

    @pl.when(is_far)
    def _():
        signal(late_in, {"ka": inner})

    @pl.when(high_site)
    def _():
        signal(late_in, {"ka": me - 1})

    def remote(source, target, send, recv, peer):
        return pltpu.make_async_remote_copy(
            src_ref=source, dst_ref=target, send_sem=send, recv_sem=recv,
            device_id=peer, device_id_type=mesh,
        )

    def send_own(target, n, sems, peer, cuts):
        for c, (start, size) in cuts:
            part = pl.ds(start, size)
            remote(own_hbm.at[part], target.at[part], send_sems.at[n], sems.at[c], {"ka": peer}).start()

    def sent_own(n, size=slab):
        part = pl.ds(0, size)
        return remote(own_hbm.at[part], own.at[part], send_sems.at[n], first_sems.at[0], {"ka": twin})

    def arrived(buffer, sems, c, cuts):
        part = buffer.at[pl.ds(*cuts[c])]
        remote(part, part, send_sems.at[0], sems.at[c], {"ka": twin}).wait_recv()

    def main_sends(pairs):
        @pl.when(me == below)
        def _():
            for n, start, stop in pairs:
                send_own(first, n, first_sems, hub, list(enumerate(parts))[start:stop])

        @pl.when(me == above)
        def _():
            for n, start, stop in pairs:
                send_own(second, n, second_sems, hub, list(enumerate(parts))[start:stop])

    main_sends(((0, 0, 1),))
    near_in.wait()
    shift_in.wait()

    def role_shift(step):
        target = (me + step) % points
        total = jnp.int32(0)
        for b in range(ROLES):
            total = total + jnp.where(near_ref[0, b] == target, shift_ref[0, b], 0)
        return total

    lane = lax.broadcasted_iota(jnp.int32, meta_out.shape, 1)
    facts = jnp.where(
        lane == 0, role_shift(1), jnp.where(lane == 1, role_shift(row), role_shift(points // 2))
    )
    meta_out[...] = facts
    meta_in[me] = facts

    steps_up = (z >= 2) & (column % 2 == 1) & (me != points - 1)
    notices = (
        (~is_hub, hub),
        (is_hub, outer),
        (me == me, twin),
        (steps_up, me + 1),
        (corner_high, row),
    )
    steps_in = (z >= 2) & (column % 2 == 0) & (me != 2 * row)
    heard = jnp.where(is_hub, 4, jnp.where(is_outer, 2, 1)) + jnp.where(steps_in | corner_low, 1, 0)
    told = 2 + jnp.where(steps_up | corner_high, 1, 0)

    def notice(n, peer):
        source = meta_out if n != 1 else meta_in.at[inner]
        target = meta_in.at[me] if n != 1 else meta_in.at[inner]
        return remote(source, target, meta_sems.at[0], meta_sems.at[1], {"ka": peer})

    def facts_of(amount):
        fact = meta_in.at[pl.ds(0, amount)]
        return remote(fact, fact, meta_sems.at[0], meta_sems.at[1], {"ka": twin})

    for n in (0, 2, 4):
        pl.when(notices[n][0])(notice(n, notices[n][1]).start)

    main_sends(((0, 1, count - 1), (1, count - 1, count)))

    @pl.when(high_source)
    def _():
        pl.semaphore_wait(late_in, 2)

    pl.when(steps_up)(notice(3, me + 1).start)
    extra_cuts = list(enumerate(extra_parts))
    extra_down = (me == 2) | (me == row + 2)
    extra_up = (me == 2 * row + 1) | (me == 2 * row + 3) | (me == 3 * row + 1)
    extra_source = extra_down | extra_up | corner_low | corner_high
    extra_site = (
        (me == row - 1) | (me == 1) | (me == row + 1)
        | (me == 2 * row + 2) | (me == 3 * row) | (me == 3 * row + 2)
    )
    extra_peer = jnp.where(corner_high, row, jnp.where(extra_up, me + 1, me - 1))

    @pl.when(extra_down | extra_up | corner_high)
    def _():
        send_own(extra, 3, extra_sems, extra_peer, extra_cuts)

    @pl.when(corner_low)
    def _():
        send_own(extra, 3, extra_sems, extra_peer, extra_cuts[:1])

    @pl.when(is_outer | is_hub)
    def _():
        send_own(first, 2, first_sems, twin, list(enumerate(parts)))

    map_in.wait()
    indexes, sends, padded = index_tables(map_ref[...], my_slice, slab, capacity)
    tables[...] = jnp.zeros_like(tables)
    for d in range(2):
        tables[pl.ds(d * shifts, shifts), pl.ds(0, slab)] = indexes[d]
        tables[pl.ds((2 + d) * shifts, shifts), pl.ds(0, padded)] = sends[d]
    tables_in = pltpu.make_async_copy(tables, table_at, local_sems.at[0])
    tables_in.start()

    def corner_copy(c):
        part = pl.ds(*parts[c])
        return remote(first.at[part], extra.at[part], send_sems.at[5], extra_sems.at[0], {"ka": 2 * row - 1})

    def relayed(source, c):
        part = pl.ds(*parts[c])
        return remote(source.at[part], first.at[part], send_sems.at[4], first_sems.at[c], {"ka": outer})

    def relay(c):
        arrived(second, second_sems, c, parts)
        pl.when(low)(relayed(second, c).start)
        arrived(first, first_sems, c, parts)
        pl.when(~low)(relayed(first, c).start)
        pl.when(corner_low)(corner_copy(c).start)

    @pl.when(is_hub)
    def _():
        relay(0)

    for amount in range(1, 6):
        pl.when(heard == amount)(facts_of(amount).wait_recv)

    pl.when(is_hub)(notice(1, outer).start)
    meta_copy = pltpu.make_async_copy(meta_in, meta, local_sems.at[1])
    meta_copy.start()
    meta_copy.wait()
    tables_in.wait()
    keep.wait()

    def shift_of(point, kind):
        return meta[point, 0, kind]

    NEXT, ROW, HALF = 0, 1, 2
    OWN_EXTRA, BELOW_SLOT, ABOVE_SLOT, CORNER_SLOT = 4, 5, 6, 7
    groups = (0, 0, 0, 0, 1, 2, 2, 3)

    def swap(n, many=1):
        part = pl.ds(n * capacity, many * capacity)
        group = groups[n]
        return remote(packs.at[part], landed.at[part], swap_send.at[0], swap_recv.at[group], {"ga": partner})

    def place_landed(n, target, place):
        def move(r, carry):
            target[slab + place * capacity + r] = landed[n * capacity + r]
            return carry

        lax.fori_loop(0, capacity, move, 0, unroll=4)

    def take(n, target, place):
        swap(n).wait_recv()
        place_landed(n, target, place)

    def offer(n, source, inverse, shift):
        line = (2 + inverse) * shifts + shift

        def gather(r, carry):
            packs[n * capacity + r] = source[table_at[line, r]]
            return carry

        lax.fori_loop(0, capacity, gather, 0, unroll=4)
        swap(n).start()

    def pick(ref, at):
        return ref[at].reshape(2 * bands, lanes)

    def accumulate(e, part, still, moving, place, inverse, shift, turn=False):
        start, size = part
        line = inverse * shifts + shift

        def at(n):
            value = table_at[line, n]
            return value + jnp.where(value >= slab, place * capacity, 0)

        def products(begin, many, total):
            for u in range(0, many, 2):
                n = begin + u
                left = jnp.concatenate([pick(still, n), pick(still, n + 1)], axis=1)
                right = jnp.concatenate([pick(moving, at(n)), pick(moving, at(n + 1))], axis=1)
                total = total + lax.dot_general(
                    right if turn else left,
                    left if turn else right,
                    (((1,), (1,)), ((), ())),
                    preferred_element_type=jnp.float32,
                )
            return total

        steps = [s for s in (12, 10, 18, 6, 4, 2) if size % s == 0][0]
        if steps == size:
            sums[e] = products(start, size, sums[e])
        else:
            sums[e] = lax.fori_loop(
                0, size // steps, lambda i, total: products(start + i * steps, steps, total), sums[e]
            )

    def result_copies(e, kind, bra):
        copies = []
        half = bands // 2
        for g in (partner, my_slice):
            source = results.at[e, pl.ds(g * half, half)]
            target = slots.at[kind, my_slice]
            near = pltpu.make_async_copy(source, target, result_sems.at[1])
            away = remote(source, target, result_sems.at[0], result_sems.at[1], {"ka": bra, "ga": g})
            copies.append((bra == me, near, away))
        return copies

    def settle(e, inverse=None):
        total = sums[e]
        if inverse is not None:
            total = jnp.where(inverse == 1, total.T, total)
        upper, under = total[:bands], pltpu.roll(total[bands:], bands, 1)
        left = lax.broadcasted_iota(jnp.int32, upper.shape, 1) < bands
        results[e] = upper + jnp.where(left, under, -under)

    def dispatch(edges):
        for n in range(2):
            for e, kind, bra in edges:
                at_home, near, away = result_copies(e, kind, bra)[n]
                if n == 0:
                    away.start()
                else:
                    pl.when(at_home)(near.start)
                    pl.when(~at_home)(away.start)

    def deliver(e, kind, bra, inverse=None):
        settle(e, inverse)
        dispatch(((e, kind, bra),))

    sums[...] = jnp.zeros_like(sums)
    extra_inverse = jnp.where(lower_half, 1, 0)
    extra_bra = jnp.where(lower_half, me, me - 1)
    EXTRA = 6

    hub_edges = (
        (first, own, 0, 0, below, ROW),
        (second, own, 1, 1, hub, ROW),
        (third, own, 2, 1, hub, HALF),
        (third, own, 3, 0, far, HALF),
        (third, first, 0, 0, far, ROW),
        (third, second, 0, 1, above, ROW),
    )

    @pl.when(extra_site)
    def _():
        offer(OWN_EXTRA, own, extra_inverse, shift_of(extra_bra, NEXT))

    def extra_edge():
        take(OWN_EXTRA, own, OWN_EXTRA)
        shift = shift_of(extra_bra, NEXT)
        for c, part in extra_cuts:
            arrived(extra, extra_sems, c, extra_parts)
            accumulate(EXTRA, part, extra, own, OWN_EXTRA, extra_inverse, shift)
        deliver(EXTRA, NEXT, extra_bra, extra_inverse)

    @pl.when(is_hub)
    def _():
        for e in range(4):
            _, _, _, inverse, bra, kind = hub_edges[e]
            offer(e, own, inverse, shift_of(bra, kind))

        for c in range(1, count):
            relay(c)

        for n, e in ((BELOW_SLOT, 4), (ABOVE_SLOT, 5)):
            _, source, _, inverse, bra, kind = hub_edges[e]
            offer(n, source, inverse, shift_of(bra, kind))

        @pl.when(corner_low)
        def _():
            offer(CORNER_SLOT, second, 0, shift_of(2 * row - 1, NEXT))

        swap(0, 4).wait_recv()
        for e in range(4):
            place_landed(e, own, e)
        for e in range(2):
            still, moving, place, inverse, bra, kind = hub_edges[e]
            accumulate(e, (0, slab), still, moving, place, inverse, shift_of(bra, kind), inverse == 1)
            deliver(e, kind, bra)

        @pl.when(corner_low)
        def _():
            send_own(extra, 3, extra_sems, extra_peer, extra_cuts[1:])

        @pl.when(extra_site)
        def _():
            extra_edge()

        @pl.when(corner_high)
        def _():
            arrived(extra, extra_sems, 0, [(0, slab)])
            offer(CORNER_SLOT, extra, 0, shift_of(4 * row - 1, NEXT))

        swap(BELOW_SLOT, 2).wait_recv()
        place_landed(BELOW_SLOT, first, 0)
        place_landed(ABOVE_SLOT, second, 0)

        @pl.when(corner_low)
        def _():
            take(CORNER_SLOT, second, 1)

        @pl.when(corner_high)
        def _():
            take(CORNER_SLOT, extra, 0)

        def late_edge(e, part):
            still, moving, place, inverse, bra, kind = hub_edges[e]
            accumulate(e, part, still, moving, place, inverse, shift_of(bra, kind), inverse == 1)

        for c, part in enumerate(late_parts):
            arrived(third, third_sems, c, late_parts)
            ends = c == len(late_parts) - 1
            for pair in ((3, 4), (5, 2)):
                for e in pair:
                    late_edge(e, part)
                if ends:
                    for e in pair:
                        settle(e)
                    dispatch([(e, hub_edges[e][5], hub_edges[e][4]) for e in pair])

            @pl.when(corner_high)
            def _():
                accumulate(EXTRA, part, third, extra, 0, 0, shift_of(4 * row - 1, NEXT))
                if ends:
                    deliver(EXTRA, NEXT, 4 * row - 1)

            if c < len(extra_parts):

                @pl.when(corner_low)
                def _():
                    arrived(extra, extra_sems, c, extra_parts)
                    accumulate(EXTRA, extra_parts[c], extra, second, 1, 0, shift_of(2 * row - 1, NEXT))
                    if c == len(extra_parts) - 1:
                        deliver(EXTRA, NEXT, 2 * row - 1)

        pl.when(corner_low)(sent_own(5).wait_send)
        sent_own(4).wait_send()

    outer_edges = ((0, 1, outer), (1, 0, inner))

    @pl.when(is_outer)
    def _():
        for e, inverse, bra in outer_edges:
            offer(e, own, inverse, shift_of(bra, HALF))
        swap(0, 2).wait_recv()
        for e in range(2):
            place_landed(e, own, e)
        pl.when(extra_site & ~lower_half)(extra_edge)
        for c, part in enumerate(parts):
            arrived(first, first_sems, c, parts)
            for e, inverse, bra in outer_edges:
                accumulate(e, part, first, own, e, inverse, shift_of(bra, HALF), inverse == 1)
        for e, inverse, bra in outer_edges:
            deliver(e, HALF, bra)
        pl.when(extra_site & lower_half)(extra_edge)
        sent_own(0, tail).wait_send()

    twin_inverse = jnp.where(column % 2 == 1, 0, 1)
    twin_bra = me - column % 2

    @pl.when(is_inner | is_far)
    def _():
        shift = shift_of(twin_bra, NEXT)
        offer(0, own, twin_inverse, shift)
        take(0, own, 0)
        for c in range(count):
            arrived(first, first_sems, c, parts)
        accumulate(0, (0, slab), first, own, 0, twin_inverse, shift)
        deliver(0, NEXT, twin_bra, twin_inverse)

        @pl.when(is_inner)
        def _():
            @pl.when(~high_source)
            def _():
                pl.semaphore_wait(late_in, 1)

            sent_own(0, tail).wait_send()
            signal(go, {"ka": far})

        @pl.when(is_far)
        def _():
            pl.semaphore_wait(go, 1)
            send_own(third, 0, third_sems, hub, list(enumerate(late_parts)))

        pl.when(extra_site)(extra_edge)
        pl.when(is_far)(sent_own(0).wait_send)

    @pl.when(is_outer | is_inner)
    def _():
        sent_own(1, slab - tail).wait_send()

    @pl.when(is_outer | is_hub)
    def _():
        sent_own(2).wait_send()

    @pl.when(extra_source)
    def _():
        sent_own(3).wait_send()

    for amount in (2, 3):
        pl.when(told == amount)(facts_of(amount).wait_send)

    packed = jnp.where(is_hub, 6, jnp.where(is_outer, 2, 1)) + jnp.where(extra_site | corner_low | corner_high, 1, 0)
    for amount in (1, 2, 3, 6, 7):
        pl.when(packed == amount)(swap(0, amount).wait_send)

    own_twin = jnp.where(column % 2 == 0, 1, 2)
    sent_results = jnp.where(is_hub, 10, jnp.where(is_outer, 3, own_twin))
    sent_results = sent_results + jnp.where(corner_low | corner_high, 2, 0)
    sent_results = sent_results + jnp.where(extra_site, jnp.where(lower_half, 1, 2), 0)
    for amount in (1, 2, 3, 4, 5, 10, 12):
        halves = results.at[pl.ds(0, amount), pl.ds(0, bands // 2)] if amount < 8 else results.at[pl.ds(0, amount // 2)]
        done = remote(halves, halves, result_sems.at[0], result_sems.at[1], {"ka": twin})
        pl.when(sent_results == amount)(done.wait_send)

    pltpu.make_async_copy(slots, slots, result_sems.at[1]).wait()
    found = [slots[kind, 0] + slots[kind, 1] for kind in range(ROLES)]
    for b in range(ROLES):
        target = near_ref[0, b]
        chosen = jnp.where(target == (me + row) % points, found[ROW], found[HALF])
        chosen = jnp.where(target == (me + 1) % points, found[NEXT], chosen)
        out_ref[b, 0] = chosen[:, :bands]
        out_ref[b, 1] = chosen[:, bands:]


def meet(neighbour, shift_id, block_map, own, points, capacity):
    slab, bands, lanes = own.shape[0], own.shape[2], own.shape[3]
    block = own.shape[1:]
    shifts = block_map.shape[0]
    half = bands // 2
    dma = pltpu.SemaphoreType.DMA
    mains, lates, extras = (len(f(slab)) for f in (main_pieces, late_pieces, extra_pieces))

    def blocks(count):
        return pltpu.VMEM((count,) + block, own.dtype)

    return pl.pallas_call(
        functools.partial(meet_kernel, points, slab, capacity),
        out_shape=pltpu.VMEM((ROLES, 2, half, bands), jnp.float32),
        in_specs=[pl.BlockSpec(memory_space=pl.ANY)] * 4,
        out_specs=pl.BlockSpec(memory_space=pltpu.VMEM),
        scratch_shapes=[
            pltpu.SMEM(neighbour.shape, jnp.int32),
            pltpu.SMEM(shift_id.shape, jnp.int32),
            pltpu.VMEM(block_map.shape, jnp.int32),
            blocks(slab + 5 * capacity),
            blocks(slab + capacity),
            blocks(slab + 2 * capacity),
            blocks(slab),
            blocks(slab + capacity),
            blocks(8 * capacity),
            blocks(8 * capacity),
            pltpu.VMEM((1, lanes), jnp.int32),
            pltpu.VMEM((points, 1, lanes), jnp.int32),
            pltpu.VMEM((4 * shifts, lanes), jnp.int32),
            pltpu.VMEM((7, 2 * bands, 2 * bands), jnp.float32),
            pltpu.VMEM((7, bands, 2 * bands), jnp.float32),
            pltpu.VMEM((ROLES, 2, half, 2 * bands), jnp.float32),
            pltpu.SMEM((points, 1, lanes), jnp.int32),
            pltpu.SMEM((4 * shifts, lanes), jnp.int32),
            dma((4,)), dma((2,)), dma((6,)),
            dma((mains,)), dma((mains,)), dma((lates,)), dma((extras,)),
            dma((1,)), dma((4,)), dma((2,)),
            pltpu.SemaphoreType.REGULAR,
            pltpu.SemaphoreType.REGULAR,
        ],
        compiler_params=pltpu.CompilerParams(
            collective_id=0, has_side_effects=True, vmem_limit_bytes=60 * 2**20
        ),
        name="meet",
    )(neighbour, shift_id, block_map, own)


def on_four_levels(coeffs, neighbour, shift_id, block_map):
    own = coeffs[0]
    points = lax.axis_size("ka")
    capacity = 2 * max(1, own.shape[0] // 12)
    return meet(neighbour, shift_id, block_map, own, points, capacity)[None]


def solution(mesh):
    in_specs = (P("ka", "ga", None, None, None), P("ka", None), P("ka", None), P())
    out_specs = P("ka", None, None, "ga", None)
    levels = mesh.shape["ka"] // 4
    square = mesh.shape["ga"] == 2 and mesh.shape["ka"] == 4 * levels and levels == 4

    def run(coeffs, neighbour, shift_id, block_map):
        one_each = coeffs.shape[0] == mesh.shape["ka"] and neighbour.shape[1] == ROLES
        per_slice = coeffs.shape[1] // mesh.shape["ga"]
        lanes = coeffs.shape[4]
        fits = per_slice % 40 == 0 and 80 <= per_slice <= lanes and 2 * coeffs.shape[3] == lanes
        body = on_four_levels if square and one_each and fits else on_device
        return jax.shard_map(
            body, mesh=mesh, in_specs=in_specs, out_specs=out_specs, check_vma=False
        )(coeffs, neighbour, shift_id, block_map)

    return run
```
